32 devices in a mesh: gx: 4 (over z), gy: 4 (over y, core), gz: 2 (over x).
Axes of the slice: x: 2, y: 2, z: 4, core: 2. Of those that a mesh axis runs over, the one named last changes fastest.
Arguments:
- volume: bfloat16 [32, 64, 32, 128], P('gx', 'gy', 'gz'), may hold values from -6 to 6
- w_full: bfloat16 [3, 3, 3, 128, 128], replicated, may hold values from -0.15625 to 0.15625
- w_half: bfloat16 [3, 3, 3, 128, 256], replicated, may hold values from -0.15625 to 0.15625
- w_bottom_in: bfloat16 [3, 3, 3, 256, 512], P(None, None, None, None, 'gx'), may hold values from -0.109375 to 0.109375
- w_bottom_out: bfloat16 [3, 3, 3, 512, 512], P(None, None, None, None, 'gx'), may hold values from -0.078125 to 0.078125
- w_up: bfloat16 [3, 3, 3, 768, 256], replicated, may hold values from -0.0625 to 0.0625
Outputs:
- decoded: bfloat16 [16, 32, 16, 256], P('gx', 'gy', 'gz')
The draws below stay inside these ranges and needn't reach their ends.
All inputs are finite; a program needn't handle non-finite values.
Results may differ from the reference program's by a relative error of at most 0.009.
Values may be sent and summed in bfloat16 or wider, within the bound.
A program may use at most 64 MiB of HBM per device.

```python
import jax
import jax.numpy as jnp
from jax import lax

C0 = 128
C1 = 256
C2 = 512
NX = 32
NY = 64
NZ = 32


def block_levels(own_key, shape, cuts, least, top_value):
    def one(dim, blocks):
        draws = jax.random.uniform(jax.random.fold_in(jax.random.fold_in(own_key, 6), dim), (blocks,), jnp.float32, least / len(cuts), top_value / len(cuts))
        return jnp.repeat(jnp.exp(draws), shape[dim] // blocks).reshape((-1,) + (1,) * (len(shape) - dim - 1))

    gain = one(*cuts[0])
    for cut in cuts[1:]:
        gain = gain * one(*cut)
    return gain


def normal_values(own_key, dims, scale, reach, cuts=(), held_as=jnp.bfloat16):
    array = scale * jax.random.normal(own_key, dims, jnp.float32)
    if cuts:
        array = array * block_levels(own_key, dims, cuts, -0.22, 0.18)
    return jnp.clip(array, -reach, reach).astype(held_as)


def setup_inputs(seed: int = 0) -> dict:
    keys = jax.random.split(jax.random.key(seed), 7)
    return {
        "volume": normal_values(keys[0], (NX, NY, NZ, C0), 1.0, 6.0, ((0, 4), (1, 4), (2, 2))),
        "w_full": normal_values(keys[1], (3, 3, 3, C0, C0), (27 * C0 // 2) ** -0.5, 0.15625),
        "w_half": normal_values(keys[2], (3, 3, 3, C0, C1), (27 * C0 // 2) ** -0.5, 0.15625),
        "w_bottom_in": normal_values(keys[3], (3, 3, 3, C1, C2), (27 * C1 // 2) ** -0.5, 0.109375, ((4, 4),)),
        "w_bottom_out": normal_values(keys[4], (3, 3, 3, C2, C2), (27 * C2 // 2) ** -0.5, 0.078125, ((4, 4),)),
        "w_up": normal_values(keys[5], (3, 3, 3, C2 + C1, C1), (27 * (C2 + C1) // 2) ** -0.5, 0.0625),
    }


def convolve(field, kernel):
    result = lax.conv_general_dilated(field[None], kernel, (1, 1, 1), "SAME", dimension_numbers=("NDHWC", "DHWIO", "NDHWC"), preferred_element_type=jnp.float32)
    return result[0]


def rectify(total):
    return jnp.maximum(total, 0.0).astype(jnp.bfloat16)


def shrink(field):
    size_x, size_y, size_z, channels = field.shape
    blocks = field.reshape(size_x // 2, 2, size_y // 2, 2, size_z // 2, 2, channels)
    return jnp.max(blocks, axis=(1, 3, 5))


def enlarge(field):
    size_x, size_y, size_z, channels = field.shape
    spread = jnp.broadcast_to(field[:, None, :, None, :, None, :], (size_x, 2, size_y, 2, size_z, 2, channels))
    return spread.reshape(2 * size_x, 2 * size_y, 2 * size_z, channels)


def reference(volume, w_full, w_half, w_bottom_in, w_bottom_out, w_up):
    full_level = rectify(convolve(volume, w_full))
    pooled = shrink(full_level)
    skip_level = rectify(convolve(pooled, w_half))
    coarse = shrink(skip_level)
    bottom_first = rectify(convolve(coarse, w_bottom_in))
    bottom_second = rectify(convolve(bottom_first, w_bottom_out))
    joined = jnp.concatenate([enlarge(bottom_second), skip_level], axis=3)
    return convolve(joined, w_up).astype(jnp.bfloat16)
```

```python
import functools

import jax
import jax.numpy as jnp
from jax import lax
from jax.experimental import pallas as pl
from jax.experimental.pallas import tpu as pltpu
from jax.sharding import PartitionSpec as P

F32 = jnp.float32
BF16 = jnp.bfloat16
STEPS = [(dx, dy) for dx in (-1, 0, 1) for dy in (-1, 0, 1)]


def span(d, n, pad):
    if d == 0:
        return pl.ds(pad, n), pl.ds(1, n)
    if d < 0:
        return pl.ds(pad, 1), pl.ds(n + 1, 1)
    return pl.ds(pad + n - 1, 1), pl.ds(0, 1)


def kernel(
    dims,
    v, wf_h, wh_h, w1_h, w2_h, wu_h,
    out,
    wf, wh, w1, w2, wu, wsem, wt,
    p1, f1, g1, e1, t1,
    p2, f2, g2, e2,
    p3, f3, g3, e3, acc,
    pk2, l2, sel2, q2, pk3, l3, q3, pk4, l4, vup,
    s1, r1, s2, r2, s3, r3, s4, r4, s5, r5, s6, r6,
):
    gxn, gyn = dims
    gx, gy, gz = lax.axis_index("gx"), lax.axis_index("gy"), lax.axis_index("gz")
    oz = 1 - gz

    loads = [
        pltpu.make_async_copy(src, dst, wsem.at[i])
        for i, (src, dst) in enumerate(((wf_h, wf), (wh_h, wh), (w1_h, w1), (w2_h, w2), (wu_h, wu)))
    ]
    for load in loads:
        load.start()

    def on(cond, fn):
        if cond is True:
            fn()
        else:
            pl.when(cond)(fn)

    def exists(dx, dy):
        conds = []
        if dx < 0:
            conds.append(gx > 0)
        if dx > 0:
            conds.append(gx < gxn - 1)
        if dy < 0:
            conds.append(gy > 0)
        if dy > 0:
            conds.append(gy < gyn - 1)
        if not conds:
            return True
        return functools.reduce(jnp.logical_and, conds)

    for ref in (p1, g1, p2, g2, p3, g3, l2, l3, l4):
        ref[...] = jnp.zeros(ref.shape, ref.dtype)

    barrier = pltpu.get_barrier_semaphore()
    for s in range(gxn):
        there = lax.rem(gx + s, gxn)
        for dy in (-1, 0, 1):
            for z in (0, 1):
                if s == 0 and dy == 0 and z == 0:
                    continue

                def signal(there=there, dy=dy, z=z):
                    pl.semaphore_signal(
                        barrier, inc=1,
                        device_id={"gx": there, "gy": gy + dy, "gz": oz if z else gz},
                        device_id_type=pl.DeviceIdType.MESH,
                    )

                on(exists(0, dy), signal)
    lines = 1 + (gy > 0).astype(jnp.int32) + (gy < gyn - 1).astype(jnp.int32)
    pl.semaphore_wait(barrier, 2 * gxn * lines - 1)

    def send(src, dst, ss, rs, x, y, z):
        return pltpu.make_async_remote_copy(
            src_ref=src, dst_ref=dst, send_sem=ss, recv_sem=rs,
            device_id={"gx": x, "gy": y, "gz": z}, device_id_type=pl.DeviceIdType.MESH,
        )

    many_x = jnp.logical_and(gx > 0, gx < gxn - 1)
    many_y = jnp.logical_and(gy > 0, gy < gyn - 1)

    def by_y(fn):
        for b in (1, 2):
            pl.when(many_y if b == 2 else jnp.logical_not(many_y))(functools.partial(fn, b))

    def by_xy(fn):
        for a in (1, 2):
            for b in (1, 2):
                cx_ = many_x if a == 2 else jnp.logical_not(many_x)
                cy_ = many_y if b == 2 else jnp.logical_not(many_y)
                pl.when(jnp.logical_and(cx_, cy_))(functools.partial(fn, a, b))

    def drain(ref, sem):
        pltpu.make_async_copy(ref, ref, sem).wait()

    late = []

    def neighbours(src, pad, face, rim, side, nx, ny, ss, rs):
        for dx, dy in STEPS:
            sx, tx = span(dx, nx, pad)
            sy, ty = span(dy, ny, pad)
            fx, _ = span(dx, nx, 0)
            fy, _ = span(dy, ny, 0)
            copies = [send(face.at[fx, fy], side.at[tx, ty], ss.at[0], rs.at[0], gx + dx, gy + dy, oz)]
            if (dx, dy) != (0, 0):
                k = 1 if dx else 2
                copies.append(send(src.at[sx, sy], rim.at[tx, ty], ss.at[k], rs.at[k], gx + dx, gy + dy, gz))
            for copy in copies:
                on(exists(dx, dy), copy.start)

        def finish(sems):
            def both(a, b):
                drain(side.at[0 : nx + a, 0 : ny + b], sems.at[0])
                drain(rim.at[0:a, 0 : ny + b], sems.at[1])
                drain(rim.at[0:nx, 0:b], sems.at[2])

            by_xy(both)

        late.append(lambda: finish(ss))
        return lambda: finish(rs)

    def edge(block):
        size = block.shape[-2]
        rows = lax.broadcasted_iota(jnp.int32, block.shape, block.ndim - 2)
        return jnp.sum(jnp.where(rows == (size - 1) * oz, block, 0.0), axis=block.ndim - 2, keepdims=True)

    def shifted(block, fill):
        size = block.shape[-2]
        axis = block.ndim - 2
        rows = lax.broadcasted_iota(jnp.int32, block.shape, axis)
        below = jnp.where(rows == 0, 0.0, pltpu.roll(block, 1, axis))
        above = jnp.where(rows == size - 1, 0.0, pltpu.roll(block, size - 1, axis))
        if fill is not None:
            fill = jnp.broadcast_to(fill, block.shape)
            below = jnp.where(rows == jnp.where(gz == 1, 0, -1), fill, below)
            above = jnp.where(rows == jnp.where(gz == 0, size - 1, -1), fill, above)
        return below, above

    def rounded(x):
        return x.astype(BF16).astype(F32)

    nx, ny, nz, c0 = v.shape
    for x in range(nx):
        f1[x] = edge(v[x].astype(F32))
    arrived = neighbours(v, 0, f1, p1, g1, nx, ny, s1, r1)
    p1[1 : nx + 1, 1 : ny + 1] = v[...]

    loads[0].wait()
    k0 = 3 * c0
    for oy in range(3):
        for plane in range(4):
            at = pl.ds(plane * k0, k0)
            wt[oy, at, :c0] = wf[plane * 3 + oy] if plane < 3 else jnp.zeros((k0, c0), BF16)
            wt[oy, at, c0:] = wf[(plane - 1) * 3 + oy] if plane > 0 else jnp.zeros((k0, c0), BF16)
    arrived()

    @pl.loop(0, nx + 2)
    def _(x):
        block = p1[x].astype(F32)
        below, above = shifted(block, g1[x])
        e1[x, :, :, 0:c0] = below.astype(BF16)
        e1[x, :, :, c0 : 2 * c0] = p1[x]
        e1[x, :, :, 2 * c0 :] = above.astype(BF16)

    def full_rows(x):
        total = jnp.zeros((ny * nz, 2 * c0), F32)
        for oy in range(3):
            for half in range(2):
                lhs = [e1[x + 2 * half + i, oy : oy + ny].reshape(ny * nz, k0) for i in range(2)]
                rhs = wt[oy, 2 * half * k0 : 2 * (half + 1) * k0]
                total = total + jnp.dot(jnp.concatenate(lhs, axis=1), rhs, preferred_element_type=F32)
        return jnp.maximum(jnp.maximum(total[:, :c0], total[:, c0:]), 0.0)

    hx, hy, hz = nx // 2, ny // 2, nz // 2

    @pl.loop(0, hx)
    def _(x):
        both = full_rows(2 * x).reshape(hy, 2, nz, c0)
        t1[...] = jnp.max(both, axis=1)
        small = jnp.maximum(t1[:, pl.ds(0, hz, stride=2), :], t1[:, pl.ds(1, hz, stride=2), :])
        small = rounded(small)
        p2[x + 1, 1 : hy + 1] = small
        f2[x] = edge(small)

    arrived = neighbours(p2, 1, f2, p2, g2, hx, hy, s2, r2)
    arrived()
    for x in range(hx + 2):
        block = p2[x]
        below, above = shifted(block, g2[x])
        e2[0, x], e2[1, x], e2[2, x] = below, block, above
    loads[1].wait()
    rows = hx * hy * hz
    c1 = wh.shape[2]
    total = jnp.zeros((rows, c1), F32)
    for ox in range(3):
        for oy in range(3):
            for k in range(3):
                lhs = e2[k, ox : ox + hx, oy : oy + hy].reshape(rows, c0).astype(BF16)
                total = total + jnp.dot(lhs, wh[(ox * 3 + oy) * 3 + k], preferred_element_type=F32)
    skip = rounded(jnp.maximum(total, 0.0)).reshape(hx, hy, hz, c1)
    p3[1 : hx + 1, 1 : hy + 1] = skip
    f3[...] = edge(skip)

    cx, cy, cz = hx // 2, hy // 2, hz // 2
    ax = gxn * cx
    group = cz * cx
    m = jnp.max(skip.reshape(cx, 2, cy, 2, hz, c1), axis=(1, 3))
    m = m.reshape(cx * cy * hz, c1)
    m = jnp.maximum(m, pltpu.roll(m, m.shape[0] - 1, 0)).astype(BF16)

    blocks = []
    lane = lax.broadcasted_iota(jnp.int32, (group, cx * cy * hz), 1)
    sub = lax.broadcasted_iota(jnp.int32, (group, cx * cy * hz), 0)
    shift_x = cx.bit_length() - 1
    sub_x = sub & (cx - 1)
    sub_o = sub >> shift_x
    for y in range(cy):
        blocks.append(jnp.where(lane == (sub_x * cy + y) * hz + 2 * sub_o, 1.0, 0.0))
    blocks.append(jnp.where(lane == (sub_x * cy + sub_o) * hz + 2 * (cz - 1) * oz, 1.0, 0.0))
    pick = jnp.concatenate(blocks, axis=0).astype(BF16)
    packets = jnp.dot(pick, m, preferred_element_type=F32).reshape(cy + 1, group, c1).astype(BF16)
    pk2[...] = packets
    l2[gx, 0:cy] = packets[0:cy]

    slots = cy + 5

    def coarse_copy(k, dy, z):
        def make(src_gx, tgt_gx):
            if z == 0:
                src = {0: pl.ds(0, cy), -1: pl.ds(0, 1), 1: pl.ds(cy - 1, 1)}[dy]
                dst = {0: pl.ds(0, cy), 1: pl.ds(cy, 1), -1: pl.ds(cy + 1, 1)}[dy]
            else:
                src = pl.ds(cy, 1)
                dst = {0: pl.ds(cy + 2, 1), 1: pl.ds(cy + 3, 1), -1: pl.ds(cy + 4, 1)}[dy]
            return send(pk2.at[src], l2.at[src_gx, dst], s4.at[k], r4.at[k], tgt_gx, gy + dy, oz if z else gz)

        return make

    def deep_copy(pk, land, ss, rs):
        def choose(k, dy, z):
            def make(src_gx, tgt_gx):
                sy, ty = span(dy, cy, 0)
                sender = gz if src_gx is gx else (oz if z else gz)
                if z == 0:
                    src = pk.at[sy]
                    dst = land.at[src_gx, ty, pl.ds(1, cz)]
                else:
                    src = pk.at[sy, pl.ds((cz - 1) * (1 - sender), 1)]
                    dst = land.at[src_gx, ty, pl.ds((cz + 1) * sender, 1)]
                return send(src, dst, ss.at[k], rs.at[k], tgt_gx, gy + dy, oz if z else gz)

            return make

        return choose

    def narrow_copy(k, dy, z):
        def make(src_gx, tgt_gx):
            sy, ty = span(dy, cy, 0)
            sender = gz if src_gx is gx else (oz if z else gz)
            if z == 0:
                src = pk4.at[tgt_gx, sy]
                dst = l4.at[src_gx, ty, pl.ds(1, cz // 2)]
            else:
                src = pk4.at[tgt_gx, sy, pl.ds((cz // 2 - 1) * (1 - sender), 1)]
                dst = l4.at[src_gx, ty, pl.ds((cz // 2 + 1) * sender, 1)]
            return send(src, dst, s6.at[k], r6.at[k], tgt_gx, gy + dy, oz if z else gz)

        return make

    def column_exchange(choose, away, home):
        for s in list(range(1, gxn)) + [0]:
            there = lax.rem(gx + s, gxn)
            for k, (dy, z) in enumerate(((0, 0), (-1, 0), (1, 0), (0, 1), (-1, 1), (1, 1))):
                if s == 0 and k == 0:
                    continue
                on(exists(0, dy), choose(0 if s else 1 + z, dy, z)(gx, there).start)

        def finish(which):
            def both(b):
                drain(*away(b, which))
                for k in (0, 1):
                    drain(*home(b, k, which))

            by_y(both)

        late.append(lambda: finish(0))
        return lambda: finish(1)

    def blocks_of(land, sems):
        wz = land.shape[2] - 2

        def away(b, which):
            return land.at[0 : gxn - 1, 0 : cy + b, 0 : wz + 1], sems[which].at[0]

        def home(b, k, which):
            return land.at[0, 0 : (cy if k else 0) + b, 0 : 1 if k else wz], sems[which].at[1 + k]

        return away, home

    arrived = column_exchange(
        coarse_copy,
        lambda b, which: (l2.at[0 : gxn - 1, 0 : cy + 1 + 2 * b], (s4, r4)[which].at[0]),
        lambda b, k, which: (l2.at[0, 0 : b + k], (s4, r4)[which].at[1 + k]),
    )

    span_g = slots * group
    width = gxn * span_g
    lane = lax.broadcasted_iota(jnp.int32, (ax, width), 1)
    xs = lax.broadcasted_iota(jnp.int32, (ax, width), 0)
    base = lane - ((xs >> shift_x) * span_g + (xs & (cx - 1)))
    for y in range(-1, cy + 1):
        for z in range(-1, cz + 1):
            if 0 <= z < cz:
                slot = y if 0 <= y < cy else (cy if y < 0 else cy + 1)
                at = slot * group + z * cx
            else:
                slot = cy + 2 if 0 <= y < cy else (cy + 3 if y < 0 else cy + 4)
                line = y if 0 <= y < cy else (cy - 1 if y < 0 else 0)
                mine = (gz == 1) if z < 0 else (gz == 0)
                at = jnp.where(mine, slot * group + line * cx, -width * 4)
            sel2[y + 1, z + 1] = jnp.where(base == at, 1.0, 0.0)

    rim = (cy + 2) * (cz + 2) * ax
    select = sel2[...].reshape(rim, width).astype(BF16)
    arrived()
    skip_arrived = neighbours(p3, 1, f3, p3, g3, hx, hy, s3, r3)
    landed = l2[...].astype(F32).reshape(width, c1).astype(BF16)
    block = jnp.dot(select, landed, preferred_element_type=F32).reshape(cy + 2, cz + 2, ax, c1)

    def spread(q, block):
        below, above = shifted(block, None)
        q[0], q[1], q[2] = below, block, above

    deep = cy * cz * ax
    fo = w1.shape[2]

    def bottom(q, w):
        total = jnp.zeros((deep, fo), F32)
        for ox in range(3):
            for oy in range(3):
                for k in range(3):
                    lhs = q[ox, oy : oy + cy, k : k + cz].reshape(deep, q.shape[-1]).astype(BF16)
                    total = total + jnp.dot(lhs, w[(ox * 3 + oy) * 3 + k], preferred_element_type=F32)
        return jnp.maximum(total, 0.0).reshape(cy, cz, ax, fo).astype(BF16)

    spread(q2, block)
    loads[2].wait()
    first = bottom(q2, w1)
    pk3[...] = first
    l3[gx, 1 : cy + 1, 1 : cz + 1] = first
    arrived = column_exchange(deep_copy(pk3, l3, s5, r5), *blocks_of(l3, (s5, r5)))

    skip_arrived()
    for x in range(hx + 2):
        block = p3[x]
        below, above = shifted(block, g3[x])
        e3[0, x], e3[1, x], e3[2, x] = below, block, above
    loads[4].wait()
    c2 = w2.shape[1]
    total = jnp.zeros((rows, c1), F32)
    for ox in range(3):
        for oy in range(3):
            for k in range(3):
                lhs = e3[k, ox : ox + hx, oy : oy + hy].reshape(rows, c1).astype(BF16)
                total = total + jnp.dot(lhs, wu[(ox * 3 + oy) * 3 + k, c2:, :], preferred_element_type=F32)
    acc[...] = total.reshape(hx, hy, hz, c1)

    near = cx + 2
    wide = gxn * cz * near
    lane = lax.broadcasted_iota(jnp.int32, (wide, cz * ax), 1)
    row = lax.broadcasted_iota(jnp.int32, (wide, cz * ax), 0)
    shift_n = near.bit_length() - 1
    shift_z = cz.bit_length() - 1
    at = (row >> (shift_n + shift_z)) * cx + (row & (near - 1)) - 1
    at = jnp.where(jnp.logical_and(at >= 0, at < ax), at, -(cz + 1) * ax)
    share = jnp.where(lane == ((row >> shift_n) & (cz - 1)) * ax + at, 1.0, 0.0).astype(BF16)

    lane = lax.broadcasted_iota(jnp.int32, (hz, (cz + 4) * near), 1)
    zs = lax.broadcasted_iota(jnp.int32, (hz, (cz + 4) * near), 0)
    blocks = []
    for k in range(3):
        for x in range(-1, hx + 1):
            blocks.append(jnp.where(lane == (((zs + (k - 1)) >> 1) + 2) * near + (x >> 1) + 1, 1.0, 0.0))
    pick = jnp.concatenate(blocks, axis=0).astype(BF16)

    arrived()
    spread(q3, jnp.concatenate([l3[g].astype(F32) for g in range(gxn)], axis=-1))
    loads[3].wait()
    second = bottom(q3, w2)
    for y in range(cy):
        line = second[y].astype(F32).reshape(cz * ax, fo).astype(BF16)
        line = jnp.dot(share, line, preferred_element_type=F32)
        pk4[:, y] = line.reshape(gxn, cz // 2, 2 * near, fo).astype(BF16)
    l4[gx, 1 : cy + 1, 1 : cz // 2 + 1] = pk4[gx]
    arrived = column_exchange(narrow_copy, *blocks_of(l4, (s6, r6)))
    arrived()
    for y in range(cy + 2):
        field = jnp.concatenate([l4[g, y].astype(F32) for g in range(gxn)], axis=-1)
        field = field.reshape((cz + 4) * near, c2).astype(BF16)
        vup[:, y] = jnp.dot(pick, field, preferred_element_type=F32).reshape(3, hx + 2, hz, c2)

    parts = []
    for oy in range(3):
        low, high = (oy + 1) // 2, (hy - 1 + oy + 1) // 2 + 1
        count = high - low
        total = jnp.zeros((count * hx * hz, c1), F32)
        for ox in range(3):
            for k in range(3):
                lhs = vup[k, low:high, ox : ox + hx].reshape(count * hx * hz, c2).astype(BF16)
                total = total + jnp.dot(lhs, wu[(ox * 3 + oy) * 3 + k, :c2, :], preferred_element_type=F32)
        parts.append((low, total.reshape(count, hx, hz, c1)))
    for y in range(hy):
        line = acc[:, y]
        for oy in range(3):
            low, part = parts[oy]
            line = line + part[(y + oy + 1) // 2 - low]
        out[:, y] = line.astype(BF16)

    for fn in late:
        fn()


def on_device(dims, volume, w_full, w_half, w_bottom_in, w_bottom_out, w_up):
    gxn, gyn = dims
    nx, ny, nz, c0 = volume.shape
    c1 = w_half.shape[4]
    c2, fo = w_bottom_out.shape[3:]
    hx, hy, hz = nx // 2, ny // 2, nz // 2
    cx, cy, cz = hx // 2, hy // 2, hz // 2
    ax = gxn * cx
    weights = [
        w_full.reshape(9, 3 * c0, c0),
        w_half.reshape(27, c0, c1),
        w_bottom_in.reshape(27, c1, fo),
        w_bottom_out.reshape(27, c2, fo),
        w_up.reshape(27, c2 + c1, c1),
    ]
    vm = pltpu.VMEM
    dma = pltpu.SemaphoreType.DMA
    scratch = [vm(w.shape, BF16) for w in weights] + [dma((5,)), vm((3, 12 * c0, 2 * c0), BF16)]
    scratch += [
        vm((nx + 2, ny + 2, nz, c0), BF16), vm((nx, ny, 1, c0), F32), vm((nx + 2, ny + 2, 1, c0), F32),
        vm((nx + 2, ny + 2, nz, 3 * c0), BF16), vm((hy, nz, c0), F32),
        vm((hx + 2, hy + 2, hz, c0), F32), vm((hx, hy, 1, c0), F32), vm((hx + 2, hy + 2, 1, c0), F32),
        vm((3, hx + 2, hy + 2, hz, c0), F32),
        vm((hx + 2, hy + 2, hz, c1), F32), vm((hx, hy, 1, c1), F32), vm((hx + 2, hy + 2, 1, c1), F32),
        vm((3, hx + 2, hy + 2, hz, c1), F32), vm((hx, hy, hz, c1), F32),
        vm((cy + 1, cz * cx, c1), BF16), vm((gxn, cy + 5, cz * cx, c1), BF16),
        vm((cy + 2, cz + 2, ax, gxn * (cy + 5) * cz * cx), F32), vm((3, cy + 2, cz + 2, ax, c1), F32),
        vm((cy, cz, ax, fo), BF16), vm((gxn, cy + 2, cz + 2, ax, fo), BF16), vm((3, cy + 2, cz + 2, ax, c2), F32),
        vm((gxn, cy, cz // 2, 2 * (cx + 2), fo), BF16), vm((gxn, cy + 2, cz // 2 + 2, 2 * (cx + 2), fo), BF16),
        vm((3, cy + 2, hx + 2, hz, c2), F32),
    ]
    scratch += [dma((3,))] * 12
    return pl.pallas_call(
        functools.partial(kernel, dims),
        out_shape=jax.ShapeDtypeStruct((hx, hy, hz, c1), BF16),
        in_specs=[pl.BlockSpec(memory_space=pltpu.VMEM)] + [pl.BlockSpec(memory_space=pl.ANY)] * 5,
        out_specs=pl.BlockSpec(memory_space=pltpu.VMEM),
        scratch_shapes=scratch,
        compiler_params=pltpu.CompilerParams(
            collective_id=0, has_side_effects=True, vmem_limit_bytes=60 * 1024 * 1024
        ),
    )(volume, *weights)


def solution(mesh):
    dims = (mesh.shape["gx"], mesh.shape["gy"])
    assert mesh.shape["gz"] == 2
    return jax.shard_map(
        functools.partial(on_device, dims),
        mesh=mesh,
        in_specs=(
            P("gx", "gy", "gz", None),
            P(),
            P(),
            P(None, None, None, None, "gx"),
            P(None, None, None, None, "gx"),
            P(),
        ),
        out_specs=P("gx", "gy", "gz", None),
        check_vma=False,
    )
```

```python
import functools

import jax
import jax.numpy as jnp
from jax import lax
from jax.experimental import pallas as pl
from jax.experimental.pallas import tpu as pltpu
from jax.sharding import PartitionSpec as P

F32 = jnp.float32
BF16 = jnp.bfloat16
STEPS = [(dx, dy) for dx in (-1, 0, 1) for dy in (-1, 0, 1)]


def span(d, n, pad):
    if d == 0:
        return pl.ds(pad, n), pl.ds(1, n)
    if d < 0:
        return pl.ds(pad, 1), pl.ds(n + 1, 1)
    return pl.ds(pad + n - 1, 1), pl.ds(0, 1)


def kernel(
    dims,
    v_h, wf_h, wh_h, w1_h, w2_h, wu_h,
    out,
    wf, wh, w1, w2, wu, wsem, vsem, wt,
    p1, f1, g1, e1, t1,
    p2, f2, g2, e2,
    p3, f3, g3, e3, acc,
    pk2, l2, sel2, q2, pk3, l3, q3, pk4, l4, vup,
    s1, r1, s2, r2, s3, r3, s4, r4, s5, r5, s6, r6,
):
    gxn, gyn = dims
    gx, gy, gz = lax.axis_index("gx"), lax.axis_index("gy"), lax.axis_index("gz")
    oz = 1 - gz

    nx, ny, nz, c0 = v_h.shape
    fetch = pltpu.make_async_copy(v_h, p1.at[1 : nx + 1, 1 : ny + 1], vsem)
    fetch.start()
    loads = [
        pltpu.make_async_copy(src, dst, wsem.at[i])
        for i, (src, dst) in enumerate(((wf_h, wf), (wh_h, wh), (w1_h, w1), (w2_h, w2), (wu_h, wu)))
    ]
    for load in loads:
        load.start()

    def on(cond, fn):
        if cond is True:
            fn()
        else:
            pl.when(cond)(fn)

    def exists(dx, dy):
        conds = []
        if dx < 0:
            conds.append(gx > 0)
        if dx > 0:
            conds.append(gx < gxn - 1)
        if dy < 0:
            conds.append(gy > 0)
        if dy > 0:
            conds.append(gy < gyn - 1)
        if not conds:
            return True
        return functools.reduce(jnp.logical_and, conds)

    for x in (0, nx + 1):
        p1[x] = jnp.zeros(p1.shape[1:], BF16)
    for y in (0, ny + 1):
        p1[1 : nx + 1, y] = jnp.zeros((nx, nz, c0), BF16)
    for ref in (g1, p2, g2, p3, g3, l2, l3, l4):
        ref[...] = jnp.zeros(ref.shape, ref.dtype)

    fetch.wait()
    barrier = pltpu.get_barrier_semaphore()
    for s in range(gxn):
        there = lax.rem(gx + s, gxn)
        for dy in (-1, 0, 1):
            for z in (0, 1):
                if s == 0 and dy == 0 and z == 0:
                    continue

                def signal(there=there, dy=dy, z=z):
                    pl.semaphore_signal(
                        barrier, inc=1,
                        device_id={"gx": there, "gy": gy + dy, "gz": oz if z else gz},
                        device_id_type=pl.DeviceIdType.MESH,
                    )

                on(exists(0, dy), signal)
    lines = 1 + (gy > 0).astype(jnp.int32) + (gy < gyn - 1).astype(jnp.int32)
    pl.semaphore_wait(barrier, 2 * gxn * lines - 1)

    def send(src, dst, ss, rs, x, y, z):
        return pltpu.make_async_remote_copy(
            src_ref=src, dst_ref=dst, send_sem=ss, recv_sem=rs,
            device_id={"gx": x, "gy": y, "gz": z}, device_id_type=pl.DeviceIdType.MESH,
        )

    many_x = jnp.logical_and(gx > 0, gx < gxn - 1)
    many_y = jnp.logical_and(gy > 0, gy < gyn - 1)

    def by_y(fn):
        for b in (1, 2):
            pl.when(many_y if b == 2 else jnp.logical_not(many_y))(functools.partial(fn, b))

    def by_xy(fn):
        for a in (1, 2):
            for b in (1, 2):
                cx_ = many_x if a == 2 else jnp.logical_not(many_x)
                cy_ = many_y if b == 2 else jnp.logical_not(many_y)
                pl.when(jnp.logical_and(cx_, cy_))(functools.partial(fn, a, b))

    def drain(ref, sem):
        pltpu.make_async_copy(ref, ref, sem).wait()

    late = []

    def neighbours(src, pad, face, rim, side, nx, ny, ss, rs):
        for dx, dy in STEPS:
            sx, tx = span(dx, nx, pad)
            sy, ty = span(dy, ny, pad)
            fx, _ = span(dx, nx, 0)
            fy, _ = span(dy, ny, 0)
            copies = [send(face.at[fx, fy], side.at[tx, ty], ss.at[0], rs.at[0], gx + dx, gy + dy, oz)]
            if (dx, dy) != (0, 0):
                k = 1 if dx else 2
                copies.append(send(src.at[sx, sy], rim.at[tx, ty], ss.at[k], rs.at[k], gx + dx, gy + dy, gz))
            for copy in copies:
                on(exists(dx, dy), copy.start)

        def finish(sems):
            def both(a, b):
                drain(side.at[0 : nx + a, 0 : ny + b], sems.at[0])
                drain(rim.at[0:a, 0 : ny + b], sems.at[1])
                drain(rim.at[0:nx, 0:b], sems.at[2])

            by_xy(both)

        late.append(lambda: finish(ss))
        return lambda: finish(rs)

    def edge(block):
        size = block.shape[-2]
        rows = lax.broadcasted_iota(jnp.int32, block.shape, block.ndim - 2)
        return jnp.sum(jnp.where(rows == (size - 1) * oz, block, 0.0), axis=block.ndim - 2, keepdims=True)

    def shifted(block, fill):
        size = block.shape[-2]
        axis = block.ndim - 2
        rows = lax.broadcasted_iota(jnp.int32, block.shape, axis)
        below = jnp.where(rows == 0, 0.0, pltpu.roll(block, 1, axis))
        above = jnp.where(rows == size - 1, 0.0, pltpu.roll(block, size - 1, axis))
        if fill is not None:
            fill = jnp.broadcast_to(fill, block.shape)
            below = jnp.where(rows == jnp.where(gz == 1, 0, -1), fill, below)
            above = jnp.where(rows == jnp.where(gz == 0, size - 1, -1), fill, above)
        return below, above

    def rounded(x):
        return x.astype(BF16).astype(F32)

    for x in range(nx):
        f1[x] = edge(p1[x + 1, 1 : ny + 1].astype(F32))
    arrived = neighbours(p1, 1, f1, p1, g1, nx, ny, s1, r1)

    loads[0].wait()
    k0 = 3 * c0
    for oy in range(3):
        for plane in range(4):
            at = pl.ds(plane * k0, k0)
            wt[oy, at, :c0] = wf[plane * 3 + oy] if plane < 3 else jnp.zeros((k0, c0), BF16)
            wt[oy, at, c0:] = wf[(plane - 1) * 3 + oy] if plane > 0 else jnp.zeros((k0, c0), BF16)
    arrived()

    @pl.loop(0, nx + 2)
    def _(x):
        block = p1[x].astype(F32)
        below, above = shifted(block, g1[x])
        e1[x, :, :, 0:c0] = below.astype(BF16)
        e1[x, :, :, c0 : 2 * c0] = p1[x]
        e1[x, :, :, 2 * c0 :] = above.astype(BF16)

    def full_rows(x):
        total = jnp.zeros((ny * nz, 2 * c0), F32)
        for oy in range(3):
            for half in range(2):
                lhs = [e1[x + 2 * half + i, oy : oy + ny].reshape(ny * nz, k0) for i in range(2)]
                rhs = wt[oy, 2 * half * k0 : 2 * (half + 1) * k0]
                total = total + jnp.dot(jnp.concatenate(lhs, axis=1), rhs, preferred_element_type=F32)
        return jnp.maximum(jnp.maximum(total[:, :c0], total[:, c0:]), 0.0)

    hx, hy, hz = nx // 2, ny // 2, nz // 2

    @pl.loop(0, hx)
    def _(x):
        both = full_rows(2 * x).reshape(hy, 2, nz, c0)
        t1[...] = jnp.max(both, axis=1)
        small = jnp.maximum(t1[:, pl.ds(0, hz, stride=2), :], t1[:, pl.ds(1, hz, stride=2), :])
        small = rounded(small)
        p2[x + 1, 1 : hy + 1] = small
        f2[x] = edge(small)

    arrived = neighbours(p2, 1, f2, p2, g2, hx, hy, s2, r2)
    arrived()
    for x in range(hx + 2):
        block = p2[x]
        below, above = shifted(block, g2[x])
        e2[0, x], e2[1, x], e2[2, x] = below, block, above
    loads[1].wait()
    rows = hx * hy * hz
    c1 = wh.shape[2]
    total = jnp.zeros((rows, c1), F32)
    for ox in range(3):
        for oy in range(3):
            for k in range(3):
                lhs = e2[k, ox : ox + hx, oy : oy + hy].reshape(rows, c0).astype(BF16)
                total = total + jnp.dot(lhs, wh[(ox * 3 + oy) * 3 + k], preferred_element_type=F32)
    skip = rounded(jnp.maximum(total, 0.0)).reshape(hx, hy, hz, c1)
    p3[1 : hx + 1, 1 : hy + 1] = skip
    f3[...] = edge(skip)

    cx, cy, cz = hx // 2, hy // 2, hz // 2
    ax = gxn * cx
    group = cz * cx
    m = jnp.max(skip.reshape(cx, 2, cy, 2, hz, c1), axis=(1, 3))
    m = m.reshape(cx * cy * hz, c1)
    m = jnp.maximum(m, pltpu.roll(m, m.shape[0] - 1, 0)).astype(BF16)

    blocks = []
    lane = lax.broadcasted_iota(jnp.int32, (group, cx * cy * hz), 1)
    sub = lax.broadcasted_iota(jnp.int32, (group, cx * cy * hz), 0)
    shift_x = cx.bit_length() - 1
    sub_x = sub & (cx - 1)
    sub_o = sub >> shift_x
    for y in range(cy):
        blocks.append(jnp.where(lane == (sub_x * cy + y) * hz + 2 * sub_o, 1.0, 0.0))
    blocks.append(jnp.where(lane == (sub_x * cy + sub_o) * hz + 2 * (cz - 1) * oz, 1.0, 0.0))
    pick = jnp.concatenate(blocks, axis=0).astype(BF16)
    packets = jnp.dot(pick, m, preferred_element_type=F32).reshape(cy + 1, group, c1).astype(BF16)
    pk2[...] = packets
    l2[gx, 0:cy] = packets[0:cy]

    slots = cy + 5

    def coarse_copy(k, dy, z):
        def make(src_gx, tgt_gx):
            if z == 0:
                src = {0: pl.ds(0, cy), -1: pl.ds(0, 1), 1: pl.ds(cy - 1, 1)}[dy]
                dst = {0: pl.ds(0, cy), 1: pl.ds(cy, 1), -1: pl.ds(cy + 1, 1)}[dy]
            else:
                src = pl.ds(cy, 1)
                dst = {0: pl.ds(cy + 2, 1), 1: pl.ds(cy + 3, 1), -1: pl.ds(cy + 4, 1)}[dy]
            return send(pk2.at[src], l2.at[src_gx, dst], s4.at[k], r4.at[k], tgt_gx, gy + dy, oz if z else gz)

        return make

    def deep_copy(pk, land, ss, rs):
        def choose(k, dy, z):
            def make(src_gx, tgt_gx):
                sy, ty = span(dy, cy, 0)
                sender = gz if src_gx is gx else (oz if z else gz)
                if z == 0:
                    src = pk.at[sy]
                    dst = land.at[src_gx, ty, pl.ds(1, cz)]
                else:
                    src = pk.at[sy, pl.ds((cz - 1) * (1 - sender), 1)]
                    dst = land.at[src_gx, ty, pl.ds((cz + 1) * sender, 1)]
                return send(src, dst, ss.at[k], rs.at[k], tgt_gx, gy + dy, oz if z else gz)

            return make

        return choose

    def narrow_copy(k, dy, z):
        def make(src_gx, tgt_gx):
            sy, ty = span(dy, cy, 0)
            sender = gz if src_gx is gx else (oz if z else gz)
            if z == 0:
                src = pk4.at[tgt_gx, sy]
                dst = l4.at[src_gx, ty, pl.ds(1, cz // 2)]
            else:
                src = pk4.at[tgt_gx, sy, pl.ds((cz // 2 - 1) * (1 - sender), 1)]
                dst = l4.at[src_gx, ty, pl.ds((cz // 2 + 1) * sender, 1)]
            return send(src, dst, s6.at[k], r6.at[k], tgt_gx, gy + dy, oz if z else gz)

        return make

    def column_exchange(choose, away, home):
        for s in list(range(1, gxn)) + [0]:
            there = lax.rem(gx + s, gxn)
            for k, (dy, z) in enumerate(((0, 0), (-1, 0), (1, 0), (0, 1), (-1, 1), (1, 1))):
                if s == 0 and k == 0:
                    continue
                on(exists(0, dy), choose(0 if s else 1 + z, dy, z)(gx, there).start)

        def finish(which):
            def both(b):
                drain(*away(b, which))
                for k in (0, 1):
                    drain(*home(b, k, which))

            by_y(both)

        late.append(lambda: finish(0))
        return lambda: finish(1)

    def blocks_of(land, sems):
        wz = land.shape[2] - 2

        def away(b, which):
            return land.at[0 : gxn - 1, 0 : cy + b, 0 : wz + 1], sems[which].at[0]

        def home(b, k, which):
            return land.at[0, 0 : (cy if k else 0) + b, 0 : 1 if k else wz], sems[which].at[1 + k]

        return away, home

    arrived = column_exchange(
        coarse_copy,
        lambda b, which: (l2.at[0 : gxn - 1, 0 : cy + 1 + 2 * b], (s4, r4)[which].at[0]),
        lambda b, k, which: (l2.at[0, 0 : b + k], (s4, r4)[which].at[1 + k]),
    )

    span_g = slots * group
    width = gxn * span_g
    lane = lax.broadcasted_iota(jnp.int32, (ax, width), 1)
    xs = lax.broadcasted_iota(jnp.int32, (ax, width), 0)
    base = lane - ((xs >> shift_x) * span_g + (xs & (cx - 1)))
    for y in range(-1, cy + 1):
        for z in range(-1, cz + 1):
            if 0 <= z < cz:
                slot = y if 0 <= y < cy else (cy if y < 0 else cy + 1)
                at = slot * group + z * cx
            else:
                slot = cy + 2 if 0 <= y < cy else (cy + 3 if y < 0 else cy + 4)
                line = y if 0 <= y < cy else (cy - 1 if y < 0 else 0)
                mine = (gz == 1) if z < 0 else (gz == 0)
                at = jnp.where(mine, slot * group + line * cx, -width * 4)
            sel2[y + 1, z + 1] = jnp.where(base == at, 1.0, 0.0)

    rim = (cy + 2) * (cz + 2) * ax
    select = sel2[...].reshape(rim, width).astype(BF16)
    arrived()
    skip_arrived = neighbours(p3, 1, f3, p3, g3, hx, hy, s3, r3)
    landed = l2[...].astype(F32).reshape(width, c1).astype(BF16)
    block = jnp.dot(select, landed, preferred_element_type=F32).reshape(cy + 2, cz + 2, ax, c1)

    def spread(q, block):
        below, above = shifted(block, None)
        q[0], q[1], q[2] = below, block, above

    deep = cy * cz * ax
    fo = w1.shape[2]

    def bottom(q, w):
        total = jnp.zeros((deep, fo), F32)
        for ox in range(3):
            for oy in range(3):
                for k in range(3):
                    lhs = q[ox, oy : oy + cy, k : k + cz].reshape(deep, q.shape[-1]).astype(BF16)
                    total = total + jnp.dot(lhs, w[(ox * 3 + oy) * 3 + k], preferred_element_type=F32)
        return jnp.maximum(total, 0.0).reshape(cy, cz, ax, fo).astype(BF16)

    spread(q2, block)
    loads[2].wait()
    first = bottom(q2, w1)
    pk3[...] = first
    l3[gx, 1 : cy + 1, 1 : cz + 1] = first
    arrived = column_exchange(deep_copy(pk3, l3, s5, r5), *blocks_of(l3, (s5, r5)))

    skip_arrived()
    for x in range(hx + 2):
        block = p3[x]
        below, above = shifted(block, g3[x])
        e3[0, x], e3[1, x], e3[2, x] = below, block, above
    loads[4].wait()
    c2 = w2.shape[1]
    total = jnp.zeros((rows, c1), F32)
    for ox in range(3):
        for oy in range(3):
            for k in range(3):
                lhs = e3[k, ox : ox + hx, oy : oy + hy].reshape(rows, c1).astype(BF16)
                total = total + jnp.dot(lhs, wu[(ox * 3 + oy) * 3 + k, c2:, :], preferred_element_type=F32)
    acc[...] = total.reshape(hx, hy, hz, c1)

    near = cx + 2
    wide = gxn * cz * near
    lane = lax.broadcasted_iota(jnp.int32, (wide, cz * ax), 1)
    row = lax.broadcasted_iota(jnp.int32, (wide, cz * ax), 0)
    shift_n = near.bit_length() - 1
    shift_z = cz.bit_length() - 1
    at = (row >> (shift_n + shift_z)) * cx + (row & (near - 1)) - 1
    at = jnp.where(jnp.logical_and(at >= 0, at < ax), at, -(cz + 1) * ax)
    share = jnp.where(lane == ((row >> shift_n) & (cz - 1)) * ax + at, 1.0, 0.0).astype(BF16)

    lane = lax.broadcasted_iota(jnp.int32, (hz, (cz + 4) * near), 1)
    zs = lax.broadcasted_iota(jnp.int32, (hz, (cz + 4) * near), 0)
    blocks = []
    for k in range(3):
        for x in range(-1, hx + 1):
            blocks.append(jnp.where(lane == (((zs + (k - 1)) >> 1) + 2) * near + (x >> 1) + 1, 1.0, 0.0))
    pick = jnp.concatenate(blocks, axis=0).astype(BF16)

    arrived()
    spread(q3, jnp.concatenate([l3[g].astype(F32) for g in range(gxn)], axis=-1))
    loads[3].wait()
    second = bottom(q3, w2)
    for y in range(cy):
        line = second[y].astype(F32).reshape(cz * ax, fo).astype(BF16)
        line = jnp.dot(share, line, preferred_element_type=F32)
        pk4[:, y] = line.reshape(gxn, cz // 2, 2 * near, fo).astype(BF16)
    l4[gx, 1 : cy + 1, 1 : cz // 2 + 1] = pk4[gx]
    arrived = column_exchange(narrow_copy, *blocks_of(l4, (s6, r6)))
    arrived()
    for y in range(cy + 2):
        field = jnp.concatenate([l4[g, y].astype(F32) for g in range(gxn)], axis=-1)
        field = field.reshape((cz + 4) * near, c2).astype(BF16)
        vup[:, y] = jnp.dot(pick, field, preferred_element_type=F32).reshape(3, hx + 2, hz, c2)

    parts = []
    for oy in range(3):
        low, high = (oy + 1) // 2, (hy - 1 + oy + 1) // 2 + 1
        count = high - low
        total = jnp.zeros((count * hx * hz, c1), F32)
        for ox in range(3):
            for k in range(3):
                lhs = vup[k, low:high, ox : ox + hx].reshape(count * hx * hz, c2).astype(BF16)
                total = total + jnp.dot(lhs, wu[(ox * 3 + oy) * 3 + k, :c2, :], preferred_element_type=F32)
        parts.append((low, total.reshape(count, hx, hz, c1)))
    for y in range(hy):
        line = acc[:, y]
        for oy in range(3):
            low, part = parts[oy]
            line = line + part[(y + oy + 1) // 2 - low]
        out[:, y] = line.astype(BF16)

    for fn in late:
        fn()


def on_device(dims, volume, w_full, w_half, w_bottom_in, w_bottom_out, w_up):
    gxn, gyn = dims
    nx, ny, nz, c0 = volume.shape
    c1 = w_half.shape[4]
    c2, fo = w_bottom_out.shape[3:]
    hx, hy, hz = nx // 2, ny // 2, nz // 2
    cx, cy, cz = hx // 2, hy // 2, hz // 2
    ax = gxn * cx
    weights = [
        w_full.reshape(9, 3 * c0, c0),
        w_half.reshape(27, c0, c1),
        w_bottom_in.reshape(27, c1, fo),
        w_bottom_out.reshape(27, c2, fo),
        w_up.reshape(27, c2 + c1, c1),
    ]
    vm = pltpu.VMEM
    dma = pltpu.SemaphoreType.DMA
    scratch = [vm(w.shape, BF16) for w in weights] + [dma((5,)), dma(()), vm((3, 12 * c0, 2 * c0), BF16)]
    scratch += [
        vm((nx + 2, ny + 2, nz, c0), BF16), vm((nx, ny, 1, c0), F32), vm((nx + 2, ny + 2, 1, c0), F32),
        vm((nx + 2, ny + 2, nz, 3 * c0), BF16), vm((hy, nz, c0), F32),
        vm((hx + 2, hy + 2, hz, c0), F32), vm((hx, hy, 1, c0), F32), vm((hx + 2, hy + 2, 1, c0), F32),
        vm((3, hx + 2, hy + 2, hz, c0), F32),
        vm((hx + 2, hy + 2, hz, c1), F32), vm((hx, hy, 1, c1), F32), vm((hx + 2, hy + 2, 1, c1), F32),
        vm((3, hx + 2, hy + 2, hz, c1), F32), vm((hx, hy, hz, c1), F32),
        vm((cy + 1, cz * cx, c1), BF16), vm((gxn, cy + 5, cz * cx, c1), BF16),
        vm((cy + 2, cz + 2, ax, gxn * (cy + 5) * cz * cx), F32), vm((3, cy + 2, cz + 2, ax, c1), F32),
        vm((cy, cz, ax, fo), BF16), vm((gxn, cy + 2, cz + 2, ax, fo), BF16), vm((3, cy + 2, cz + 2, ax, c2), F32),
        vm((gxn, cy, cz // 2, 2 * (cx + 2), fo), BF16), vm((gxn, cy + 2, cz // 2 + 2, 2 * (cx + 2), fo), BF16),
        vm((3, cy + 2, hx + 2, hz, c2), F32),
    ]
    scratch += [dma((3,))] * 12
    return pl.pallas_call(
        functools.partial(kernel, dims),
        out_shape=jax.ShapeDtypeStruct((hx, hy, hz, c1), BF16),
        in_specs=[pl.BlockSpec(memory_space=pltpu.HBM)] * 6,
        out_specs=pl.BlockSpec(memory_space=pltpu.VMEM),
        scratch_shapes=scratch,
        compiler_params=pltpu.CompilerParams(
            collective_id=0, has_side_effects=True, vmem_limit_bytes=52 * 1024 * 1024
        ),
    )(*[pltpu.with_memory_space_constraint(a, pltpu.HBM) for a in (volume, *weights)])


def solution(mesh):
    dims = (mesh.shape["gx"], mesh.shape["gy"])
    assert mesh.shape["gz"] == 2
    return jax.shard_map(
        functools.partial(on_device, dims),
        mesh=mesh,
        in_specs=(
            P("gx", "gy", "gz", None),
            P(),
            P(),
            P(None, None, None, None, "gx"),
            P(None, None, None, None, "gx"),
            P(),
        ),
        out_specs=P("gx", "gy", "gz", None),
        check_vma=False,
    )
```

```python
import functools

import jax
import jax.numpy as jnp
from jax import lax
from jax.experimental import pallas as pl
from jax.experimental.pallas import tpu as pltpu
from jax.sharding import PartitionSpec as P

F32 = jnp.float32
BF16 = jnp.bfloat16
STEPS = [(dx, dy) for dx in (-1, 0, 1) for dy in (-1, 0, 1)]


def span(d, n, pad):
    if d == 0:
        return pl.ds(pad, n), pl.ds(1, n)
    if d < 0:
        return pl.ds(pad, 1), pl.ds(n + 1, 1)
    return pl.ds(pad + n - 1, 1), pl.ds(0, 1)


def kernel(
    dims,
    v_h, wf_h, wh_h, w1_h, w2_h, wu_h,
    out,
    wf, wh, w1, w2, wus, wuu, wsem, vsem, wt, wz,
    p1, f1, g1, gs, e1, a1, rz, t1,
    p2, f2, g2, e2, o2,
    p3, f3, g3, e3, o3, acc,
    pk2, l2, sel2, q2, b2, pk3, l3, q3, b3, pk4, l4, up, uo,
    s1, r1, s2, r2, s3, r3, s4, r4, s5, r5, s6, r6,
):
    gxn, gyn = dims
    gx, gy, gz = lax.axis_index("gx"), lax.axis_index("gy"), lax.axis_index("gz")
    oz = 1 - gz

    nx, ny, nz, c0 = v_h.shape
    fetch = pltpu.make_async_copy(v_h, p1.at[1 : nx + 1, 1 : ny + 1], vsem)
    fetch.start()
    c2 = w2.shape[1]
    loads = [
        pltpu.make_async_copy(src, dst, wsem.at[i])
        for i, (src, dst) in enumerate((
            (wf_h, wf), (wh_h, wh), (w1_h, w1), (w2_h, w2), (wu_h.at[:, c2:], wus), (wu_h.at[:, :c2], wuu),
        ))
    ]

    def on(cond, fn):
        if cond is True:
            fn()
        else:
            pl.when(cond)(fn)

    def exists(dx, dy):
        conds = []
        if dx < 0:
            conds.append(gx > 0)
        if dx > 0:
            conds.append(gx < gxn - 1)
        if dy < 0:
            conds.append(gy > 0)
        if dy > 0:
            conds.append(gy < gyn - 1)
        if not conds:
            return True
        return functools.reduce(jnp.logical_and, conds)

    for x in (0, nx + 1):
        p1[x] = jnp.zeros(p1.shape[1:], BF16)
    for y in (0, ny + 1):
        p1[1 : nx + 1, y] = jnp.zeros((nx, nz, c0), BF16)
    for ref in (g1, p2, g2, p3, g3, l2, l3, l4):
        ref[...] = jnp.zeros(ref.shape, ref.dtype)

    barrier = pltpu.get_barrier_semaphore()
    for s in range(gxn):
        there = lax.rem(gx + s, gxn)
        for dy in (-1, 0, 1):
            for z in (0, 1):
                if s == 0 and dy == 0 and z == 0:
                    continue

                def signal(there=there, dy=dy, z=z):
                    pl.semaphore_signal(
                        barrier, inc=1,
                        device_id={"gx": there, "gy": gy + dy, "gz": oz if z else gz},
                        device_id_type=pl.DeviceIdType.MESH,
                    )

                on(exists(0, dy), signal)
    lines = 1 + (gy > 0).astype(jnp.int32) + (gy < gyn - 1).astype(jnp.int32)

    def edge(block):
        size = block.shape[-2]
        rows = lax.broadcasted_iota(jnp.int32, block.shape, block.ndim - 2)
        return jnp.sum(jnp.where(rows == (size - 1) * oz, block, 0.0), axis=block.ndim - 2, keepdims=True)

    fetch.wait()
    for load in loads:
        load.start()
    for x in range(nx):
        f1[x] = edge(p1[x + 1, 1 : ny + 1].astype(F32))
    pl.semaphore_wait(barrier, 2 * gxn * lines - 1)

    def send(src, dst, ss, rs, x, y, z):
        return pltpu.make_async_remote_copy(
            src_ref=src, dst_ref=dst, send_sem=ss, recv_sem=rs,
            device_id={"gx": x, "gy": y, "gz": z}, device_id_type=pl.DeviceIdType.MESH,
        )

    many_x = jnp.logical_and(gx > 0, gx < gxn - 1)
    many_y = jnp.logical_and(gy > 0, gy < gyn - 1)

    def by_y(fn):
        for b in (1, 2):
            pl.when(many_y if b == 2 else jnp.logical_not(many_y))(functools.partial(fn, b))

    def by_xy(fn):
        for a in (1, 2):
            for b in (1, 2):
                cx_ = many_x if a == 2 else jnp.logical_not(many_x)
                cy_ = many_y if b == 2 else jnp.logical_not(many_y)
                pl.when(jnp.logical_and(cx_, cy_))(functools.partial(fn, a, b))

    def drain(ref, sem):
        pltpu.make_async_copy(ref, ref, sem).wait()

    late = []

    def neighbours(src, pad, face, rim, side, nx, ny, ss, rs):
        for dx, dy in STEPS:
            sx, tx = span(dx, nx, pad)
            sy, ty = span(dy, ny, pad)
            fx, _ = span(dx, nx, 0)
            fy, _ = span(dy, ny, 0)
            copies = [send(face.at[fx, fy], side.at[tx, ty], ss.at[0], rs.at[0], gx + dx, gy + dy, oz)]
            if (dx, dy) != (0, 0):
                k = 1 if dx else 2
                copies.append(send(src.at[sx, sy], rim.at[tx, ty], ss.at[k], rs.at[k], gx + dx, gy + dy, gz))
            for copy in copies:
                on(exists(dx, dy), copy.start)

        def finish(sems):
            def both(a, b):
                drain(side.at[0 : nx + a, 0 : ny + b], sems.at[0])
                drain(rim.at[0:a, 0 : ny + b], sems.at[1])
                drain(rim.at[0:nx, 0:b], sems.at[2])

            by_xy(both)

        late.append(lambda: finish(ss))
        return lambda: finish(rs)

    def shifted(block, fill):
        size = block.shape[-2]
        axis = block.ndim - 2
        rows = lax.broadcasted_iota(jnp.int32, block.shape, axis)
        below = jnp.where(rows == 0, 0.0, pltpu.roll(block, 1, axis))
        above = jnp.where(rows == size - 1, 0.0, pltpu.roll(block, size - 1, axis))
        if fill is not None:
            fill = jnp.broadcast_to(fill, block.shape)
            below = jnp.where(rows == jnp.where(gz == 1, 0, -1), fill, below)
            above = jnp.where(rows == jnp.where(gz == 0, size - 1, -1), fill, above)
        return below, above

    def rounded(x):
        return x.astype(BF16).astype(F32)

    arrived = neighbours(p1, 1, f1, p1, g1, nx, ny, s1, r1)

    k0 = 3 * c0
    for x in (0, nx + 1):
        e1[x] = jnp.zeros(e1.shape[1:], BF16)
    for y in (0, ny + 1):
        e1[1 : nx + 1, y] = jnp.zeros((nx, nz, k0), BF16)

    def widen(at, block):
        block = block.astype(F32)
        below, above = shifted(block, None)
        for k, part in enumerate((below, block, above)):
            e1[at + (slice(None), pl.ds(k * c0, c0))] = part.astype(BF16)

    @pl.loop(1, nx + 1)
    def _(x):
        widen((x, pl.ds(1, ny)), p1[x, 1 : ny + 1])

    loads[0].wait()
    for oy in range(3):
        for plane in range(4):
            at = pl.ds(plane * k0, k0)
            wt[oy, at, :c0] = wf[plane * 3 + oy] if plane < 3 else jnp.zeros((k0, c0), BF16)
            wt[oy, at, c0:] = wf[(plane - 1) * 3 + oy] if plane > 0 else jnp.zeros((k0, c0), BF16)
    for tap in range(9):
        wz[pl.ds(tap * c0, c0)] = wf[tap, pl.ds(pl.multiple_of(2 * oz * c0, c0), c0)]

    @pl.loop(0, nx // 2)
    def _(x):
        total = jnp.zeros((ny * nz, 2 * c0), F32)
        for oy in range(3):
            for half in range(2):
                lhs = [e1[2 * x + 2 * half + i, oy : oy + ny].reshape(ny * nz, k0) for i in range(2)]
                rhs = wt[oy, 2 * half * k0 : 2 * (half + 1) * k0]
                total = total + jnp.dot(jnp.concatenate(lhs, axis=1), rhs, preferred_element_type=F32)
        a1[x] = total

    arrived()
    for x in range(nx + 2):
        for y in range(ny + 2):
            gs[x, y : y + 1] = g1[x, y]
    lhs = [gs[ox : ox + nx, oy : oy + ny].reshape(nx * ny, c0).astype(BF16) for ox in range(3) for oy in range(3)]
    rz[...] = jnp.dot(jnp.concatenate(lhs, axis=1), wz[...], preferred_element_type=F32)
    for x, ox, lane in ((0, 0, 0), (nx + 1, 2, c0)):
        widen((x, pl.ds(1, ny)), p1[x, 1 : ny + 1])
        lhs = [e1[x, oy : oy + ny].reshape(ny * nz, k0) for oy in range(3)]
        rhs = wf[ox * 3 : ox * 3 + 3].reshape(3 * k0, c0)
        part = jnp.dot(jnp.concatenate(lhs, axis=1), rhs, preferred_element_type=F32)
        at = (0 if ox == 0 else nx // 2 - 1, slice(None), pl.ds(lane, c0))
        a1[at] = a1[at] + part
    for y, oy in ((0, 0), (ny + 1, 2)):
        widen((pl.ds(0, nx + 2), y), p1[:, y])
        lhs = [e1[ox : ox + nx, y].reshape(nx * nz, k0) for ox in range(3)]
        rhs = jnp.concatenate([wf[ox * 3 + oy] for ox in range(3)], axis=0)
        part = jnp.dot(jnp.concatenate(lhs, axis=1), rhs, preferred_element_type=F32).reshape(nx, nz, c0)
        for x in range(nx):
            at = (x // 2, pl.ds((0 if oy == 0 else ny - 1) * nz, nz), pl.ds(x % 2 * c0, c0))
            a1[at] = a1[at] + part[x]
    tile = 8
    last = lax.broadcasted_iota(jnp.int32, (tile, c0), 0) == (tile - 1) * oz
    for x in range(nx):
        for y in range(ny):
            at = (x // 2, pl.ds(pl.multiple_of(y * nz + (nz - tile) * oz, tile), tile), pl.ds(x % 2 * c0, c0))
            row = jnp.broadcast_to(rz[x * ny + y : x * ny + y + 1], (tile, c0))
            a1[at] = a1[at] + jnp.where(last, row, 0.0)

    hx, hy, hz = nx // 2, ny // 2, nz // 2

    @pl.loop(0, hx)
    def _(x):
        total = a1[x]
        both = jnp.maximum(jnp.maximum(total[:, :c0], total[:, c0:]), 0.0).reshape(hy, 2, nz, c0)
        t1[...] = jnp.max(both, axis=1)
        small = jnp.maximum(t1[:, pl.ds(0, hz, stride=2), :], t1[:, pl.ds(1, hz, stride=2), :])
        small = rounded(small)
        p2[x + 1, 1 : hy + 1] = small
        f2[x] = edge(small)

    arrived = neighbours(p2, 1, f2, p2, g2, hx, hy, s2, r2)
    arrived()
    rows = hx * hy * hz

    def pack(even, odd, at, block, lane):
        n, size, c = block.shape
        even[at, :, :, pl.ds(lane, c)] = block.reshape(n * size, c).astype(BF16).reshape(n // 2, 2 * size, c)
        block = block[1 : n - 1]
        odd[at, :, :, pl.ds(lane, c)] = block.reshape((n - 2) * size, c).astype(BF16).reshape(n // 2 - 1, 2 * size, c)

    def conv(even, odd, p, g, w):
        for x in range(hx + 2):
            block = p[x]
            c = block.shape[-1]
            below, above = shifted(block, g[x])
            for k, part in enumerate((below, block, above)):
                pack(even, odd, x, part, k * c)
        total = jnp.zeros((rows, w.shape[2]), F32)
        for ox in range(3):
            lhs = [r[ox : ox + hx, lo : lo + hy // 2].reshape(rows, 3 * c) for r, lo in ((even, 0), (odd, 0), (even, 1))]
            rhs = w[ox * 9 : ox * 9 + 9].reshape(9 * c, w.shape[2])
            total = total + jnp.dot(jnp.concatenate(lhs, axis=1), rhs, preferred_element_type=F32)
        return total

    loads[1].wait()
    c1 = wh.shape[2]
    total = conv(e2, o2, p2, g2, wh)
    skip = rounded(jnp.maximum(total, 0.0)).reshape(hx, hy, hz, c1)
    p3[1 : hx + 1, 1 : hy + 1] = skip
    f3[...] = edge(skip)

    cx, cy, cz = hx // 2, hy // 2, hz // 2
    ax = gxn * cx
    group = cz * cx
    m = jnp.max(skip.reshape(cx, 2, cy, 2, hz, c1), axis=(1, 3))
    m = m.reshape(cx * cy * hz, c1)
    m = jnp.maximum(m, pltpu.roll(m, m.shape[0] - 1, 0)).astype(BF16)

    blocks = []
    lane = lax.broadcasted_iota(jnp.int32, (group, cx * cy * hz), 1)
    sub = lax.broadcasted_iota(jnp.int32, (group, cx * cy * hz), 0)
    shift_x = cx.bit_length() - 1
    sub_x = sub & (cx - 1)
    sub_o = sub >> shift_x
    for y in range(cy):
        blocks.append(jnp.where(lane == (sub_x * cy + y) * hz + 2 * sub_o, 1.0, 0.0))
    blocks.append(jnp.where(lane == (sub_x * cy + sub_o) * hz + 2 * (cz - 1) * oz, 1.0, 0.0))
    pick = jnp.concatenate(blocks, axis=0).astype(BF16)
    packets = jnp.dot(pick, m, preferred_element_type=F32).reshape(cy + 1, group, c1).astype(BF16)
    pk2[...] = packets
    l2[gx, 0:cy] = packets[0:cy]

    slots = cy + 5

    def coarse_copy(k, dy, z):
        def make(src_gx, tgt_gx):
            if z == 0:
                src = {0: pl.ds(0, cy), -1: pl.ds(0, 1), 1: pl.ds(cy - 1, 1)}[dy]
                dst = {0: pl.ds(0, cy), 1: pl.ds(cy, 1), -1: pl.ds(cy + 1, 1)}[dy]
            else:
                src = pl.ds(cy, 1)
                dst = {0: pl.ds(cy + 2, 1), 1: pl.ds(cy + 3, 1), -1: pl.ds(cy + 4, 1)}[dy]
            return send(pk2.at[src], l2.at[src_gx, dst], s4.at[k], r4.at[k], tgt_gx, gy + dy, oz if z else gz)

        return make

    def deep_copy(pk, land, ss, rs):
        def choose(k, dy, z):
            def make(src_gx, tgt_gx):
                sy, ty = span(dy, cy, 0)
                sender = gz if src_gx is gx else (oz if z else gz)
                if z == 0:
                    src = pk.at[sy]
                    dst = land.at[src_gx, ty, pl.ds(1, cz)]
                else:
                    src = pk.at[sy, pl.ds((cz - 1) * (1 - sender), 1)]
                    dst = land.at[src_gx, ty, pl.ds((cz + 1) * sender, 1)]
                return send(src, dst, ss.at[k], rs.at[k], tgt_gx, gy + dy, oz if z else gz)

            return make

        return choose

    def narrow_copy(k, dy, z):
        def make(src_gx, tgt_gx):
            sy, ty = span(dy, cy, 0)
            sender = gz if src_gx is gx else (oz if z else gz)
            if z == 0:
                src = pk4.at[tgt_gx, sy]
                dst = l4.at[src_gx, ty, pl.ds(1, cz // 2)]
            else:
                src = pk4.at[tgt_gx, sy, pl.ds((cz // 2 - 1) * (1 - sender), 1)]
                dst = l4.at[src_gx, ty, pl.ds((cz // 2 + 1) * sender, 1)]
            return send(src, dst, s6.at[k], r6.at[k], tgt_gx, gy + dy, oz if z else gz)

        return make

    def column_exchange(choose, away, home):
        for s in list(range(1, gxn)) + [0]:
            there = lax.rem(gx + s, gxn)
            for k, (dy, z) in enumerate(((0, 0), (-1, 0), (1, 0), (0, 1), (-1, 1), (1, 1))):
                if s == 0 and k == 0:
                    continue
                on(exists(0, dy), choose(0 if s else 1 + z, dy, z)(gx, there).start)

        def finish(which):
            def both(b):
                drain(*away(b, which))
                for k in (0, 1):
                    drain(*home(b, k, which))

            by_y(both)

        late.append(lambda: finish(0))
        return lambda: finish(1)

    def blocks_of(land, sems):
        wz = land.shape[2] - 2

        def away(b, which):
            return land.at[0 : gxn - 1, 0 : cy + b, 0 : wz + 1], sems[which].at[0]

        def home(b, k, which):
            return land.at[0, 0 : (cy if k else 0) + b, 0 : 1 if k else wz], sems[which].at[1 + k]

        return away, home

    arrived = column_exchange(
        coarse_copy,
        lambda b, which: (l2.at[0 : gxn - 1, 0 : cy + 1 + 2 * b], (s4, r4)[which].at[0]),
        lambda b, k, which: (l2.at[0, 0 : b + k], (s4, r4)[which].at[1 + k]),
    )

    span_g = slots * group
    width = gxn * span_g
    lane = lax.broadcasted_iota(jnp.int32, (ax, width), 1)
    xs = lax.broadcasted_iota(jnp.int32, (ax, width), 0)
    base = lane - ((xs >> shift_x) * span_g + (xs & (cx - 1)))
    for y in range(-1, cy + 1):
        for z in range(-1, cz + 1):
            if 0 <= z < cz:
                slot = y if 0 <= y < cy else (cy if y < 0 else cy + 1)
                at = slot * group + z * cx
            else:
                slot = cy + 2 if 0 <= y < cy else (cy + 3 if y < 0 else cy + 4)
                line = y if 0 <= y < cy else (cy - 1 if y < 0 else 0)
                mine = (gz == 1) if z < 0 else (gz == 0)
                at = jnp.where(mine, slot * group + line * cx, -width * 4)
            sel2[y + 1, z + 1] = jnp.where(base == at, 1.0, 0.0)

    rim = (cy + 2) * (cz + 2) * ax
    select = sel2[...].reshape(rim, width).astype(BF16)
    arrived()
    skip_arrived = neighbours(p3, 1, f3, p3, g3, hx, hy, s3, r3)
    landed = l2[...].astype(F32).reshape(width, c1).astype(BF16)
    block = jnp.dot(select, landed, preferred_element_type=F32).reshape(cy + 2, cz + 2, ax, c1)

    deep = cy * cz * ax
    fo = w1.shape[2]

    def spread(even, odd, block):
        below, above = shifted(block, None)
        c = block.shape[-1]
        for ox, part in enumerate((below, block, above)):
            whole = part.reshape((cy + 2) * (cz + 2) * ax, c).astype(BF16)
            even[ox] = whole.reshape(cy + 2, cz // 2 + 1, 2 * ax, c)
            inner = part[:, 1 : cz + 1].reshape((cy + 2) * cz * ax, c).astype(BF16)
            odd[ox] = inner.reshape(cy + 2, cz // 2, 2 * ax, c)

    def bottom(even, odd, w):
        total = jnp.zeros((deep, fo), F32)
        c = even.shape[-1]
        for ox in range(3):
            lhs = [
                r[ox, oy : oy + cy, lo : lo + cz // 2].reshape(deep, c)
                for oy in range(3)
                for r, lo in ((even, 0), (odd, 0), (even, 1))
            ]
            rhs = w[ox * 9 : ox * 9 + 9].reshape(9 * c, fo)
            total = total + jnp.dot(jnp.concatenate(lhs, axis=1), rhs, preferred_element_type=F32)
        return jnp.maximum(total, 0.0).reshape(cy, cz, ax, fo).astype(BF16)

    spread(q2, b2, block)
    loads[2].wait()
    first = bottom(q2, b2, w1)
    pk3[...] = first
    l3[gx, 1 : cy + 1, 1 : cz + 1] = first
    arrived = column_exchange(deep_copy(pk3, l3, s5, r5), *blocks_of(l3, (s5, r5)))

    skip_arrived()
    loads[4].wait()
    total = conv(e3, o3, p3, g3, wus)
    acc[...] = total.reshape(hx, hy, hz, c1)

    near = cx + 2
    wide = gxn * cz * near
    lane = lax.broadcasted_iota(jnp.int32, (wide, cz * ax), 1)
    row = lax.broadcasted_iota(jnp.int32, (wide, cz * ax), 0)
    shift_n = near.bit_length() - 1
    shift_z = cz.bit_length() - 1
    at = (row >> (shift_n + shift_z)) * cx + (row & (near - 1)) - 1
    at = jnp.where(jnp.logical_and(at >= 0, at < ax), at, -(cz + 1) * ax)
    share = jnp.where(lane == ((row >> shift_n) & (cz - 1)) * ax + at, 1.0, 0.0).astype(BF16)

    lane = lax.broadcasted_iota(jnp.int32, (hz, (cz + 4) * near), 1)
    zs = lax.broadcasted_iota(jnp.int32, (hz, (cz + 4) * near), 0)
    blocks = []
    for k in range(3):
        for x in range(-1, hx + 1):
            blocks.append(jnp.where(lane == (((zs + (k - 1)) >> 1) + 2) * near + (x >> 1) + 1, 1.0, 0.0))
    for k in range(3):
        blocks += blocks[k * (hx + 2) + 1 : (k + 1) * (hx + 2) - 1]
    pick = jnp.concatenate(blocks, axis=0).astype(BF16)

    arrived()
    spread(q3, b3, jnp.concatenate([l3[g].astype(F32) for g in range(gxn)], axis=-1))
    loads[3].wait()
    second = bottom(q3, b3, w2)
    for y in range(cy):
        line = second[y].astype(F32).reshape(cz * ax, fo).astype(BF16)
        line = jnp.dot(share, line, preferred_element_type=F32)
        pk4[:, y] = line.reshape(gxn, cz // 2, 2 * near, fo).astype(BF16)
    l4[gx, 1 : cy + 1, 1 : cz // 2 + 1] = pk4[gx]
    arrived = column_exchange(narrow_copy, *blocks_of(l4, (s6, r6)))
    arrived()
    rows_o = hx * hz
    loads[5].wait()
    for y in range(cy + 2):
        field = jnp.concatenate([l4[g, y].astype(F32) for g in range(gxn)], axis=-1)
        field = field.reshape((cz + 4) * near, c2).astype(BF16)
        field = jnp.dot(pick, field, preferred_element_type=F32).astype(BF16)
        for k in range(3):
            size = (hx + 2) * hz
            part = field[k * size : (k + 1) * size]
            up[y, :, :, pl.ds(k * c2, c2)] = part.reshape(hx // 2 + 1, 2 * hz, c2)
            part = field[3 * size + k * rows_o : 3 * size + (k + 1) * rows_o]
            uo[y, :, :, pl.ds(k * c2, c2)] = part.reshape(hx // 2, 2 * hz, c2)

    parts = []
    for oy in range(3):
        low, high = (oy + 1) // 2, (hy - 1 + oy + 1) // 2 + 1
        count = high - low
        total = jnp.zeros((count * hx * hz, c1), F32)
        for ox, (r, lo) in enumerate(((up, 0), (uo, 0), (up, 1))):
            lhs = r[low:high, lo : lo + hx // 2].reshape(count * hx * hz, 3 * c2)
            rhs = wuu[(ox * 3 + oy) * 3 : (ox * 3 + oy) * 3 + 3].reshape(3 * c2, c1)
            total = total + jnp.dot(lhs, rhs, preferred_element_type=F32)
        parts.append((low, total.reshape(count, hx, hz, c1)))
    for y in range(hy):
        line = acc[:, y]
        for oy in range(3):
            low, part = parts[oy]
            line = line + part[(y + oy + 1) // 2 - low]
        out[:, y] = line.astype(BF16)

    for fn in late:
        fn()


def on_device(dims, volume, w_full, w_half, w_bottom_in, w_bottom_out, w_up):
    gxn, gyn = dims
    nx, ny, nz, c0 = volume.shape
    c1 = w_half.shape[4]
    c2, fo = w_bottom_out.shape[3:]
    hx, hy, hz = nx // 2, ny // 2, nz // 2
    cx, cy, cz = hx // 2, hy // 2, hz // 2
    ax = gxn * cx
    weights = [
        w_full.reshape(9, 3 * c0, c0),
        w_half.reshape(27, c0, c1),
        w_bottom_in.reshape(27, c1, fo),
        w_bottom_out.reshape(27, c2, fo),
        w_up.reshape(27, c2 + c1, c1),
    ]
    vm = pltpu.VMEM
    dma = pltpu.SemaphoreType.DMA
    scratch = [vm(w.shape, BF16) for w in weights[:4]]
    scratch += [vm((27, c1, c1), BF16), vm((27, c2, c1), BF16), dma((6,)), dma(())]
    scratch += [vm((3, 12 * c0, 2 * c0), BF16), vm((9 * c0, c0), BF16)]
    scratch += [
        vm((nx + 2, ny + 2, nz, c0), BF16), vm((nx, ny, 1, c0), F32), vm((nx + 2, ny + 2, 1, c0), F32),
        vm((nx + 2, ny + 2, c0), F32), vm((nx + 2, ny + 2, nz, 3 * c0), BF16), vm((hx, ny * nz, 2 * c0), F32),
        vm((nx * ny, c0), F32), vm((hy, nz, c0), F32),
        vm((hx + 2, hy + 2, hz, c0), F32), vm((hx, hy, 1, c0), F32), vm((hx + 2, hy + 2, 1, c0), F32),
        vm((hx + 2, hy // 2 + 1, 2 * hz, 3 * c0), BF16), vm((hx + 2, hy // 2, 2 * hz, 3 * c0), BF16),
        vm((hx + 2, hy + 2, hz, c1), F32), vm((hx, hy, 1, c1), F32), vm((hx + 2, hy + 2, 1, c1), F32),
        vm((hx + 2, hy // 2 + 1, 2 * hz, 3 * c1), BF16), vm((hx + 2, hy // 2, 2 * hz, 3 * c1), BF16),
        vm((hx, hy, hz, c1), F32),
        vm((cy + 1, cz * cx, c1), BF16), vm((gxn, cy + 5, cz * cx, c1), BF16),
        vm((cy + 2, cz + 2, ax, gxn * (cy + 5) * cz * cx), F32),
        vm((3, cy + 2, cz // 2 + 1, 2 * ax, c1), BF16), vm((3, cy + 2, cz // 2, 2 * ax, c1), BF16),
        vm((cy, cz, ax, fo), BF16), vm((gxn, cy + 2, cz + 2, ax, fo), BF16),
        vm((3, cy + 2, cz // 2 + 1, 2 * ax, c2), BF16), vm((3, cy + 2, cz // 2, 2 * ax, c2), BF16),
        vm((gxn, cy, cz // 2, 2 * (cx + 2), fo), BF16), vm((gxn, cy + 2, cz // 2 + 2, 2 * (cx + 2), fo), BF16),
        vm((cy + 2, hx // 2 + 1, 2 * hz, 3 * c2), BF16), vm((cy + 2, hx // 2, 2 * hz, 3 * c2), BF16),
    ]
    scratch += [dma((3,))] * 12
    return pl.pallas_call(
        functools.partial(kernel, dims),
        out_shape=jax.ShapeDtypeStruct((hx, hy, hz, c1), BF16),
        in_specs=[pl.BlockSpec(memory_space=pltpu.HBM)] * 6,
        out_specs=pl.BlockSpec(memory_space=pltpu.VMEM),
        scratch_shapes=scratch,
        compiler_params=pltpu.CompilerParams(
            collective_id=0, has_side_effects=True, vmem_limit_bytes=52 * 1024 * 1024
        ),
    )(*[pltpu.with_memory_space_constraint(a, pltpu.HBM) for a in (volume, *weights)])


def solution(mesh):
    dims = (mesh.shape["gx"], mesh.shape["gy"])
    assert mesh.shape["gz"] == 2
    return jax.shard_map(
        functools.partial(on_device, dims),
        mesh=mesh,
        in_specs=(
            P("gx", "gy", "gz", None),
            P(),
            P(),
            P(None, None, None, None, "gx"),
            P(None, None, None, None, "gx"),
            P(),
        ),
        out_specs=P("gx", "gy", "gz", None),
        check_vma=False,
    )
```

```python
import functools

import jax
import jax.numpy as jnp
from jax import lax
from jax.experimental import pallas as pl
from jax.experimental.pallas import tpu as pltpu
from jax.sharding import PartitionSpec as P

F32 = jnp.float32
BF16 = jnp.bfloat16
STEPS = [(dx, dy) for dx in (-1, 0, 1) for dy in (-1, 0, 1)]


def span(d, n, pad):
    if d == 0:
        return pl.ds(pad, n), pl.ds(1, n)
    if d < 0:
        return pl.ds(pad, 1), pl.ds(n + 1, 1)
    return pl.ds(pad + n - 1, 1), pl.ds(0, 1)


def kernel(
    dims,
    v_h, wf_h, wh_h, w1_h, w2_h, wu_h,
    out,
    wf, wh, w1, w2, wus, wuu, wsem, vsem, wt, wz,
    p1, f1, g1, gs, e1, a1, rz, t1,
    p2, f2, g2, e2, o2,
    p3, f3, g3, e3, o3, acc,
    pk2, l2, m2, sel2, selm, q2, b2, pk3, l3, q3, b3, pk4, l4, up, sums, deeps, thirds,
    s1, r1, s2, r2, s3, r3, s4, r4, s5, r5, s6, r6,
):
    gxn, gyn = dims
    gx, gy, gz = lax.axis_index("gx"), lax.axis_index("gy"), lax.axis_index("gz")
    oz = 1 - gz

    nx, ny, nz, c0 = v_h.shape
    fetch = pltpu.make_async_copy(v_h, p1.at[1 : nx + 1, 1 : ny + 1], vsem)
    fetch.start()
    c2 = w2.shape[1]
    loads = [
        pltpu.make_async_copy(src, dst, wsem.at[i])
        for i, (src, dst) in enumerate((
            (wf_h, wf), (wh_h, wh), (w1_h, w1), (w2_h, w2), (wu_h.at[:, c2:], wus), (wu_h.at[:, :c2], wuu),
        ))
    ]

    def on(cond, fn):
        if cond is True:
            fn()
        else:
            pl.when(cond)(fn)

    def exists(dx, dy):
        conds = []
        if dx < 0:
            conds.append(gx > 0)
        if dx > 0:
            conds.append(gx < gxn - 1)
        if dy < 0:
            conds.append(gy > 0)
        if dy > 0:
            conds.append(gy < gyn - 1)
        if not conds:
            return True
        return functools.reduce(jnp.logical_and, conds)

    for x in (0, nx + 1):
        p1[x] = jnp.zeros(p1.shape[1:], BF16)
    for y in (0, ny + 1):
        p1[1 : nx + 1, y] = jnp.zeros((nx, nz, c0), BF16)
    for ref in (g1, m2, l3, l4):
        ref[...] = jnp.zeros(ref.shape, ref.dtype)

    barrier = pltpu.get_barrier_semaphore()
    for s in range(gxn):
        there = lax.rem(gx + s, gxn)
        for dy in (-1, 0, 1):
            for z in (0, 1):
                if s == 0 and dy == 0 and z == 0:
                    continue

                def signal(there=there, dy=dy, z=z):
                    pl.semaphore_signal(
                        barrier, inc=1,
                        device_id={"gx": there, "gy": gy + dy, "gz": oz if z else gz},
                        device_id_type=pl.DeviceIdType.MESH,
                    )

                on(exists(0, dy), signal)
    lines = 1 + (gy > 0).astype(jnp.int32) + (gy < gyn - 1).astype(jnp.int32)

    def edge(block):
        size = block.shape[-2]
        rows = lax.broadcasted_iota(jnp.int32, block.shape, block.ndim - 2)
        return jnp.sum(jnp.where(rows == (size - 1) * oz, block, 0.0), axis=block.ndim - 2, keepdims=True)

    for ref in (g2, g3):
        ref[...] = jnp.zeros(ref.shape, ref.dtype)
    for ref in (p2, p3):
        for x in (0, ref.shape[0] - 1):
            ref[x] = jnp.zeros(ref.shape[1:], BF16)
        for y in (0, ref.shape[1] - 1):
            ref[:, y] = jnp.zeros(ref.shape[:1] + ref.shape[2:], BF16)
    fetch.wait()
    for load in loads:
        load.start()
    for x in range(nx):
        f1[x] = edge(p1[x + 1, 1 : ny + 1].astype(F32))
    pl.semaphore_wait(barrier, 2 * gxn * lines - 1)

    def send(src, dst, ss, rs, x, y, z):
        return pltpu.make_async_remote_copy(
            src_ref=src, dst_ref=dst, send_sem=ss, recv_sem=rs,
            device_id={"gx": x, "gy": y, "gz": z}, device_id_type=pl.DeviceIdType.MESH,
        )

    many_x = jnp.logical_and(gx > 0, gx < gxn - 1)
    many_y = jnp.logical_and(gy > 0, gy < gyn - 1)

    def by_y(fn):
        for b in (1, 2):
            pl.when(many_y if b == 2 else jnp.logical_not(many_y))(functools.partial(fn, b))

    def by_xy(fn):
        for a in (1, 2):
            for b in (1, 2):
                cx_ = many_x if a == 2 else jnp.logical_not(many_x)
                cy_ = many_y if b == 2 else jnp.logical_not(many_y)
                pl.when(jnp.logical_and(cx_, cy_))(functools.partial(fn, a, b))

    def drain(ref, sem):
        pltpu.make_async_copy(ref, ref, sem).wait()

    late = []

    def neighbours(src, pad, face, rim, side, nx, ny, ss, rs):
        for dx, dy in STEPS:
            sx, tx = span(dx, nx, pad)
            sy, ty = span(dy, ny, pad)
            fx, _ = span(dx, nx, 0)
            fy, _ = span(dy, ny, 0)
            copies = [send(face.at[fx, fy], side.at[tx, ty], ss.at[0], rs.at[0], gx + dx, gy + dy, oz)]
            if (dx, dy) != (0, 0):
                k = 1 if dx else 2
                copies.append(send(src.at[sx, sy], rim.at[tx, ty], ss.at[k], rs.at[k], gx + dx, gy + dy, gz))
            for copy in copies:
                on(exists(dx, dy), copy.start)

        def finish(sems):
            def both(a, b):
                drain(side.at[0 : nx + a, 0 : ny + b], sems.at[0])
                drain(rim.at[0:a, 0 : ny + b], sems.at[1])
                drain(rim.at[0:nx, 0:b], sems.at[2])

            by_xy(both)

        late.append(lambda: finish(ss))
        return lambda: finish(rs)

    def shifted(block, fill):
        size = block.shape[-2]
        axis = block.ndim - 2
        rows = lax.broadcasted_iota(jnp.int32, block.shape, axis)
        below = jnp.where(rows == 0, 0.0, pltpu.roll(block, 1, axis))
        above = jnp.where(rows == size - 1, 0.0, pltpu.roll(block, size - 1, axis))
        if fill is not None:
            fill = jnp.broadcast_to(fill, block.shape)
            below = jnp.where(rows == jnp.where(gz == 1, 0, -1), fill, below)
            above = jnp.where(rows == jnp.where(gz == 0, size - 1, -1), fill, above)
        return below, above

    def rounded(x):
        return x.astype(BF16).astype(F32)

    arrived = neighbours(p1, 1, f1, p1, g1, nx, ny, s1, r1)

    k0 = 3 * c0
    for x in (0, nx + 1):
        e1[x] = jnp.zeros(e1.shape[1:], BF16)
    for y in (0, ny + 1):
        e1[1 : nx + 1, y] = jnp.zeros((nx, nz, k0), BF16)

    def widen(at, block):
        block = block.astype(F32)
        below, above = shifted(block, None)
        for k, part in enumerate((below, block, above)):
            e1[at + (slice(None), pl.ds(k * c0, c0))] = part.astype(BF16)

    @pl.loop(1, nx + 1)
    def _(x):
        widen((x, pl.ds(1, ny)), p1[x, 1 : ny + 1])

    loads[0].wait()
    for oy in range(3):
        for plane in range(4):
            at = pl.ds(plane * k0, k0)
            wt[oy, at, :c0] = wf[plane * 3 + oy] if plane < 3 else jnp.zeros((k0, c0), BF16)
            wt[oy, at, c0:] = wf[(plane - 1) * 3 + oy] if plane > 0 else jnp.zeros((k0, c0), BF16)
    for tap in range(9):
        wz[pl.ds(tap * c0, c0)] = wf[tap, pl.ds(pl.multiple_of(2 * oz * c0, c0), c0)]

    @pl.loop(0, nx // 2)
    def _(x):
        total = jnp.zeros((ny * nz, 2 * c0), F32)
        for oy in range(3):
            for half in range(2):
                lhs = [e1[2 * x + 2 * half + i, oy : oy + ny].reshape(ny * nz, k0) for i in range(2)]
                rhs = wt[oy, 2 * half * k0 : 2 * (half + 1) * k0]
                total = total + jnp.dot(jnp.concatenate(lhs, axis=1), rhs, preferred_element_type=F32)
        a1[x] = total

    arrived()
    for x in range(nx + 2):
        for y in range(ny + 2):
            gs[x, y : y + 1] = g1[x, y]
    lhs = [gs[ox : ox + nx, oy : oy + ny].reshape(nx * ny, c0).astype(BF16) for ox in range(3) for oy in range(3)]
    rz[...] = jnp.dot(jnp.concatenate(lhs, axis=1), wz[...], preferred_element_type=F32)
    for x, ox, lane in ((0, 0, 0), (nx + 1, 2, c0)):
        widen((x, pl.ds(1, ny)), p1[x, 1 : ny + 1])
        lhs = [e1[x, oy : oy + ny].reshape(ny * nz, k0) for oy in range(3)]
        rhs = wf[ox * 3 : ox * 3 + 3].reshape(3 * k0, c0)
        part = jnp.dot(jnp.concatenate(lhs, axis=1), rhs, preferred_element_type=F32)
        at = (0 if ox == 0 else nx // 2 - 1, slice(None), pl.ds(lane, c0))
        a1[at] = a1[at] + part
    for y, oy in ((0, 0), (ny + 1, 2)):
        widen((pl.ds(0, nx + 2), y), p1[:, y])
        lhs = [e1[ox : ox + nx, y].reshape(nx * nz, k0) for ox in range(3)]
        rhs = jnp.concatenate([wf[ox * 3 + oy] for ox in range(3)], axis=0)
        part = jnp.dot(jnp.concatenate(lhs, axis=1), rhs, preferred_element_type=F32).reshape(nx, nz, c0)
        for x in range(nx):
            at = (x // 2, pl.ds((0 if oy == 0 else ny - 1) * nz, nz), pl.ds(x % 2 * c0, c0))
            a1[at] = a1[at] + part[x]
    tile = 8
    last = lax.broadcasted_iota(jnp.int32, (tile, c0), 0) == (tile - 1) * oz
    for x in range(nx):
        for y in range(ny):
            at = (x // 2, pl.ds(pl.multiple_of(y * nz + (nz - tile) * oz, tile), tile), pl.ds(x % 2 * c0, c0))
            row = jnp.broadcast_to(rz[x * ny + y : x * ny + y + 1], (tile, c0))
            a1[at] = a1[at] + jnp.where(last, row, 0.0)

    hx, hy, hz = nx // 2, ny // 2, nz // 2

    @pl.loop(0, hx)
    def _(x):
        total = a1[x]
        both = jnp.maximum(jnp.maximum(total[:, :c0], total[:, c0:]), 0.0).reshape(hy, 2, nz, c0)
        t1[...] = jnp.max(both, axis=1)
        small = jnp.maximum(t1[:, pl.ds(0, hz, stride=2), :], t1[:, pl.ds(1, hz, stride=2), :])
        small = rounded(small)
        p2[x + 1, 1 : hy + 1] = small.astype(BF16)
        f2[x] = edge(small)

    arrived = neighbours(p2, 1, f2, p2, g2, hx, hy, s2, r2)
    arrived()
    rows = hx * hy * hz

    def pack(even, odd, at, block, lane):
        n, size, c = block.shape
        even[at, :, :, pl.ds(lane, c)] = block.reshape(n * size, c).astype(BF16).reshape(n // 2, 2 * size, c)
        block = block[1 : n - 1]
        odd[at, :, :, pl.ds(lane, c)] = block.reshape((n - 2) * size, c).astype(BF16).reshape(n // 2 - 1, 2 * size, c)

    def conv(even, odd, p, g, w):
        for x in range(hx + 2):
            block = p[x].astype(F32)
            c = block.shape[-1]
            below, above = shifted(block, g[x])
            for k, part in enumerate((below, block, above)):
                pack(even, odd, x, part, k * c)
        sums[...] = jnp.zeros_like(sums)

        @pl.loop(0, 3)
        def _(ox):
            total = sums[...]
            for oy, (r, lo) in enumerate(((even, 0), (odd, 0), (even, 1))):
                lhs = r[pl.ds(ox, hx), lo : lo + hy // 2].reshape(rows, 3 * c)
                rhs = w[pl.ds(ox * 9 + oy * 3, 3)].reshape(3 * c, w.shape[2])
                total = total + jnp.dot(lhs, rhs, preferred_element_type=F32)
            sums[...] = total

        return sums[...]

    loads[1].wait()
    c1 = wh.shape[2]
    total = conv(e2, o2, p2, g2, wh)
    skip = rounded(jnp.maximum(total, 0.0)).reshape(hx, hy, hz, c1)
    p3[1 : hx + 1, 1 : hy + 1] = skip.astype(BF16)
    f3[...] = edge(skip)

    cx, cy, cz = hx // 2, hy // 2, hz // 2
    ax = gxn * cx
    group = cz * cx
    m = jnp.max(skip.reshape(cx, 2, cy, 2, hz, c1), axis=(1, 3))
    m = m.reshape(cx * cy * hz, c1)
    m = jnp.maximum(m, pltpu.roll(m, m.shape[0] - 1, 0)).astype(BF16)

    blocks = []
    lane = lax.broadcasted_iota(jnp.int32, (group, cx * cy * hz), 1)
    sub = lax.broadcasted_iota(jnp.int32, (group, cx * cy * hz), 0)
    shift_x = cx.bit_length() - 1
    sub_x = sub & (cx - 1)
    sub_o = sub >> shift_x
    for y in range(cy):
        blocks.append(jnp.where(lane == (sub_x * cy + y) * hz + 2 * sub_o, 1.0, 0.0))
    blocks.append(jnp.where(lane == (sub_x * cy + sub_o) * hz + 2 * (cz - 1) * oz, 1.0, 0.0))
    pick = jnp.concatenate(blocks, axis=0).astype(BF16)
    packets = jnp.dot(pick, m, preferred_element_type=F32).reshape(cy + 1, group, c1).astype(BF16)
    pk2[...] = packets
    l2[gx, 0:cy] = packets[0:cy]

    def coarse_copy(k, dy, z):
        def make(src_gx, tgt_gx):
            if z == 0:
                src = {0: pl.ds(0, cy), -1: pl.ds(0, 1), 1: pl.ds(cy - 1, 1)}[dy]
            else:
                src = pl.ds(cy, 1)
            if dy == 0:
                dst = l2.at[src_gx, pl.ds(cy, 1) if z else pl.ds(0, cy)]
            else:
                dst = m2.at[src_gx, pl.ds(2 * z + (1 if dy < 0 else 0), 1)]
            return send(pk2.at[src], dst, s4.at[k], r4.at[k], tgt_gx, gy + dy, oz if z else gz)

        return make

    def deep_copy(pk, land, ss, rs):
        def choose(k, dy, z):
            def make(src_gx, tgt_gx):
                sy, ty = span(dy, cy, 0)
                sender = gz if src_gx is gx else (oz if z else gz)
                if z == 0:
                    src = pk.at[sy]
                    dst = land.at[src_gx, ty, pl.ds(1, cz)]
                else:
                    src = pk.at[sy, pl.ds((cz - 1) * (1 - sender), 1)]
                    dst = land.at[src_gx, ty, pl.ds((cz + 1) * sender, 1)]
                return send(src, dst, ss.at[k], rs.at[k], tgt_gx, gy + dy, oz if z else gz)

            return make

        return choose

    def narrow_copy(k, dy, z):
        def make(src_gx, tgt_gx):
            sy, ty = span(dy, cy, 0)
            sender = gz if src_gx is gx else (oz if z else gz)
            if z == 0:
                src = pk4.at[tgt_gx, sy]
                dst = l4.at[src_gx, ty, pl.ds(1, cz // 2)]
            else:
                src = pk4.at[tgt_gx, sy, pl.ds((cz // 2 - 1) * (1 - sender), 1)]
                dst = l4.at[src_gx, ty, pl.ds((cz // 2 + 1) * sender, 1)]
            return send(src, dst, s6.at[k], r6.at[k], tgt_gx, gy + dy, oz if z else gz)

        return make

    def column_exchange(choose, main, rim):
        far = list(range(1, gxn))
        for s, dy, z in (
            [(s, 0, 0) for s in far]
            + [(s, 0, 1) for s in far + [0]]
            + [(s, dy, 0) for s in far + [0] for dy in (-1, 1)]
            + [(s, dy, 1) for s in far + [0] for dy in (-1, 1)]
        ):
            k = 2 if dy else (0 if s else 1)
            on(exists(0, dy), choose(k, dy, z)(gx, lax.rem(gx + s, gxn)).start)

        def first(which):
            for k, ref in enumerate(main):
                drain(ref, which.at[k])

        def second(which):
            by_y(lambda b: drain(rim(b), which.at[2]))

        return first, second

    def leave(waits, sems):
        late.append(lambda: [wait(sems) for wait in waits])
        return waits

    def parts_of(land):
        wz = land.shape[2] - 2
        main = (land.at[0 : gxn - 1, 0:cy, 0 : wz + 1], land.at[0, 0:cy, 0:1])
        return main, lambda b: land.at[0:gxn, 0:b, 0 : wz + 1]

    main4, rim4 = leave(
        column_exchange(coarse_copy, (l2.at[0 : gxn - 1], l2.at[0, 0:1]), lambda b: m2.at[0:gxn, 0 : 2 * b]), s4
    )

    def one_hot(ref, at, slots):
        width = gxn * slots * group
        lane = lax.broadcasted_iota(jnp.int32, (ax, width), 1)
        xs = lax.broadcasted_iota(jnp.int32, (ax, width), 0)
        base = lane - ((xs >> shift_x) * slots * group + (xs & (cx - 1)))
        ref[at] = jnp.where(base == slots_at, 1.0, 0.0)

    for y in range(-1, cy + 1):
        for z in range(-1, cz + 1):
            inside = 0 <= y < cy
            rim_slot = 0 if y < 0 else 1
            if 0 <= z < cz:
                slots_at = (y if inside else rim_slot) * group + z * cx
            else:
                line = y if inside else (cy - 1 if y < 0 else 0)
                mine = (gz == 1) if z < 0 else (gz == 0)
                slots_at = jnp.where(mine, (cy if inside else 2 + rim_slot) * group + line * cx, -(1 << 20))
            if inside:
                one_hot(sel2, (y, z + 1), cy + 1)
            else:
                one_hot(selm, (rim_slot, z + 1), 4)

    def gathered(ref, land):
        n, width = ref.shape[0], ref.shape[-1]
        select = ref[...].reshape(n * (cz + 2) * ax, width).astype(BF16)
        landed = land[...].astype(F32).reshape(width, c1).astype(BF16)
        return jnp.dot(select, landed, preferred_element_type=F32).reshape(n, cz + 2, ax, c1)

    deep = cy * cz * ax
    fo = w1.shape[2]

    windows = ((0, 0), (1, 0), (0, 1))

    def spread(even, odd, block, row):
        below, above = shifted(block, None)
        n, c = block.shape[0], block.shape[-1]
        for ox, part in enumerate((below, block, above)):
            whole = part.reshape(n * (cz + 2) * ax, c).astype(BF16)
            even[ox, row : row + n] = whole.reshape(n, cz // 2 + 1, 2 * ax, c)
            inner = part[:, 1 : cz + 1].reshape(n * cz * ax, c).astype(BF16)
            odd[ox, row : row + n] = inner.reshape(n, cz // 2, 2 * ax, c)

    def window(pair, ox, row, n):
        c = pair[0].shape[-1]
        lhs = [pair[i][ox, row : row + n, lo : lo + cz // 2].reshape(n * cz * ax, c) for i, lo in windows]
        return jnp.concatenate(lhs, axis=1)

    def bottom_own(pair, w):
        k = 3 * w.shape[1]
        deeps[...] = jnp.zeros_like(deeps)

        @pl.loop(0, 3)
        def _(ox):
            lhs = window(pair, ox, 1, cy)
            rhs = [w[pl.ds(ox * 9 + oy * 3, 3)].reshape(k, fo) for oy in range(3)]
            if fo % 128 == 0:
                total = jnp.dot(lhs, jnp.concatenate(rhs, axis=1), preferred_element_type=F32)
                total = [total[:, oy * fo : (oy + 1) * fo] for oy in range(3)]
            else:
                total = [jnp.dot(lhs, r, preferred_element_type=F32) for r in rhs]
            for oy in range(3):
                deeps[oy] = deeps[oy] + total[oy]

    def bottom_rim(pair, w):
        k = 3 * w.shape[1]
        size = cz * ax
        ends = []
        for row, oy in ((0, 0), (cy + 1, 2)):
            total = jnp.zeros((size, fo), F32)
            for ox in range(3):
                rhs = w[(ox * 3 + oy) * 3 : (ox * 3 + oy) * 3 + 3].reshape(k, fo)
                total = total + jnp.dot(window(pair, ox, row, 1), rhs, preferred_element_type=F32)
            ends.append(total)
        lines = []
        for y in range(cy):
            before = deeps[0, (y - 1) * size : y * size] if y > 0 else ends[0]
            after = deeps[2, (y + 1) * size : (y + 2) * size] if y < cy - 1 else ends[1]
            lines.append(deeps[1, y * size : (y + 1) * size] + before + after)
        return jnp.maximum(jnp.concatenate(lines, axis=0), 0.0).reshape(cy, cz, ax, fo).astype(BF16)

    main4(r4)
    skip_arrived = neighbours(p3, 1, f3, p3, g3, hx, hy, s3, r3)
    spread(q2, b2, gathered(sel2, l2), 1)
    loads[2].wait()
    bottom_own((q2, b2), w1)
    rim4(r4)
    block = gathered(selm, m2)
    spread(q2, b2, block[0:1], 0)
    spread(q2, b2, block[1:2], cy + 1)
    first = bottom_rim((q2, b2), w1)
    pk3[...] = first
    l3[gx, 1 : cy + 1, 1 : cz + 1] = first
    main5, rim5 = leave(column_exchange(deep_copy(pk3, l3, s5, r5), *parts_of(l3)), s5)

    skip_arrived()
    loads[4].wait()
    total = conv(e3, o3, p3, g3, wus)
    acc[...] = total.reshape(hx, hy, hz, c1)

    near = cx + 2
    wide = gxn * cz * near
    lane = lax.broadcasted_iota(jnp.int32, (wide, cz * ax), 1)
    row = lax.broadcasted_iota(jnp.int32, (wide, cz * ax), 0)
    shift_n = near.bit_length() - 1
    shift_z = cz.bit_length() - 1
    at = (row >> (shift_n + shift_z)) * cx + (row & (near - 1)) - 1
    at = jnp.where(jnp.logical_and(at >= 0, at < ax), at, -(cz + 1) * ax)
    share = jnp.where(lane == ((row >> shift_n) & (cz - 1)) * ax + at, 1.0, 0.0).astype(BF16)

    lane = lax.broadcasted_iota(jnp.int32, (hz, (cz + 4) * near), 1)
    zs = lax.broadcasted_iota(jnp.int32, (hz, (cz + 4) * near), 0)
    blocks = []
    for k in range(3):
        for x in range(-1, hx + 1):
            blocks.append(jnp.where(lane == (((zs + (k - 1)) >> 1) + 2) * near + (x >> 1) + 1, 1.0, 0.0))
    for k in range(3):
        blocks += blocks[k * (hx + 2) + 1 : (k + 1) * (hx + 2) - 1]
    pick = jnp.concatenate(blocks, axis=0).astype(BF16)

    def joined(row, n):
        return jnp.concatenate([l3[g, row : row + n].astype(F32) for g in range(gxn)], axis=-1)

    main5(r5)
    spread(q3, b3, joined(1, cy), 1)
    loads[3].wait()
    bottom_own((q3, b3), w2)
    rim5(r5)
    spread(q3, b3, joined(0, 1), 0)
    spread(q3, b3, joined(cy + 1, 1), cy + 1)
    second = bottom_rim((q3, b3), w2)
    for y in range(cy):
        line = second[y].astype(F32).reshape(cz * ax, fo).astype(BF16)
        line = jnp.dot(share, line, preferred_element_type=F32)
        pk4[:, y] = line.reshape(gxn, cz // 2, 2 * near, fo).astype(BF16)
    l4[gx, 1 : cy + 1, 1 : cz // 2 + 1] = pk4[gx]
    main6, rim6 = leave(column_exchange(narrow_copy, *parts_of(l4)), s6)
    size = hx * hz

    def enlarge(y):
        field = jnp.concatenate([l4[g, y].astype(F32) for g in range(gxn)], axis=-1)
        field = field.reshape((cz + 4) * near, c2).astype(BF16)
        field = jnp.dot(pick, field, preferred_element_type=F32).astype(BF16)
        for k in range(3):
            at = pl.ds(k * c2, c2)
            part = field[k * (size + 2 * hz) : (k + 1) * (size + 2 * hz)]
            up[0, y, :, :, at] = part[:size].reshape(hx // 2, 2 * hz, c2)
            up[2, y, :, :, at] = part[2 * hz :].reshape(hx // 2, 2 * hz, c2)
            part = field[3 * (size + 2 * hz) + k * size : 3 * (size + 2 * hz) + (k + 1) * size]
            up[1, y, :, :, at] = part.reshape(hx // 2, 2 * hz, c2)

    thirds[...] = jnp.zeros_like(thirds)
    main6(r6)
    for y in range(1, cy + 1):
        enlarge(y)
    loads[5].wait()

    @pl.loop(0, 3)
    def _(ox):
        lhs = up[ox, 1 : cy + 1].reshape(cy * size, 3 * c2)
        for oy in range(3):
            rhs = wuu[pl.ds(ox * 9 + oy * 3, 3)].reshape(3 * c2, c1)
            thirds[oy] = thirds[oy] + jnp.dot(lhs, rhs, preferred_element_type=F32)

    for y in range(hy):
        line = acc[:, y]
        for oy in range(3):
            at = (y + oy + 1) // 2 - 1
            if 0 <= at < cy:
                line = line + thirds[oy, at * size : (at + 1) * size].reshape(hx, hz, c1)
        if 0 < y < hy - 1:
            out[:, y] = line.astype(BF16)
        else:
            acc[:, y] = line
    rim6(r6)
    for row, oy, y in ((0, 0, 0), (cy + 1, 2, hy - 1)):
        enlarge(row)
        total = jnp.zeros((size, c1), F32)
        for ox in range(3):
            rhs = wuu[(ox * 3 + oy) * 3 : (ox * 3 + oy) * 3 + 3].reshape(3 * c2, c1)
            total = total + jnp.dot(up[ox, row].reshape(size, 3 * c2), rhs, preferred_element_type=F32)
        out[:, y] = (acc[:, y] + total.reshape(hx, hz, c1)).astype(BF16)

    for fn in late:
        fn()


def on_device(dims, volume, w_full, w_half, w_bottom_in, w_bottom_out, w_up):
    gxn, gyn = dims
    nx, ny, nz, c0 = volume.shape
    c1 = w_half.shape[4]
    c2, fo = w_bottom_out.shape[3:]
    hx, hy, hz = nx // 2, ny // 2, nz // 2
    cx, cy, cz = hx // 2, hy // 2, hz // 2
    ax = gxn * cx
    weights = [
        w_full.reshape(9, 3 * c0, c0),
        w_half.reshape(27, c0, c1),
        w_bottom_in.reshape(27, c1, fo),
        w_bottom_out.reshape(27, c2, fo),
        w_up.reshape(27, c2 + c1, c1),
    ]
    vm = pltpu.VMEM
    dma = pltpu.SemaphoreType.DMA
    scratch = [vm(w.shape, BF16) for w in weights[:4]]
    scratch += [vm((27, c1, c1), BF16), vm((27, c2, c1), BF16), dma((6,)), dma(())]
    scratch += [vm((3, 12 * c0, 2 * c0), BF16), vm((9 * c0, c0), BF16)]
    scratch += [
        vm((nx + 2, ny + 2, nz, c0), BF16), vm((nx, ny, 1, c0), F32), vm((nx + 2, ny + 2, 1, c0), F32),
        vm((nx + 2, ny + 2, c0), F32), vm((nx + 2, ny + 2, nz, 3 * c0), BF16), vm((hx, ny * nz, 2 * c0), F32),
        vm((nx * ny, c0), F32), vm((hy, nz, c0), F32),
        vm((hx + 2, hy + 2, hz, c0), BF16), vm((hx, hy, 1, c0), F32), vm((hx + 2, hy + 2, 1, c0), F32),
        vm((hx + 2, hy // 2 + 1, 2 * hz, 3 * c0), BF16), vm((hx + 2, hy // 2, 2 * hz, 3 * c0), BF16),
        vm((hx + 2, hy + 2, hz, c1), BF16), vm((hx, hy, 1, c1), F32), vm((hx + 2, hy + 2, 1, c1), F32),
        vm((hx + 2, hy // 2 + 1, 2 * hz, 3 * c1), BF16), vm((hx + 2, hy // 2, 2 * hz, 3 * c1), BF16),
        vm((hx, hy, hz, c1), F32),
        vm((cy + 1, cz * cx, c1), BF16), vm((gxn, cy + 1, cz * cx, c1), BF16), vm((gxn, 4, cz * cx, c1), BF16),
        vm((cy, cz + 2, ax, gxn * (cy + 1) * cz * cx), F32), vm((2, cz + 2, ax, gxn * 4 * cz * cx), F32),
        vm((3, cy + 2, cz // 2 + 1, 2 * ax, c1), BF16), vm((3, cy + 2, cz // 2, 2 * ax, c1), BF16),
        vm((cy, cz, ax, fo), BF16), vm((gxn, cy + 2, cz + 2, ax, fo), BF16),
        vm((3, cy + 2, cz // 2 + 1, 2 * ax, c2), BF16), vm((3, cy + 2, cz // 2, 2 * ax, c2), BF16),
        vm((gxn, cy, cz // 2, 2 * (cx + 2), fo), BF16), vm((gxn, cy + 2, cz // 2 + 2, 2 * (cx + 2), fo), BF16),
        vm((3, cy + 2, hx // 2, 2 * hz, 3 * c2), BF16),
        vm((hx * hy * hz, c1), F32), vm((3, cy * cz * ax, fo), F32), vm((3, cy * hx * hz, c1), F32),
    ]
    scratch += [dma((3,))] * 12
    return pl.pallas_call(
        functools.partial(kernel, dims),
        out_shape=jax.ShapeDtypeStruct((hx, hy, hz, c1), BF16),
        in_specs=[pl.BlockSpec(memory_space=pltpu.HBM)] * 6,
        out_specs=pl.BlockSpec(memory_space=pltpu.VMEM),
        scratch_shapes=scratch,
        compiler_params=pltpu.CompilerParams(
            collective_id=0, has_side_effects=True, vmem_limit_bytes=52 * 1024 * 1024
        ),
    )(*[pltpu.with_memory_space_constraint(a, pltpu.HBM) for a in (volume, *weights)])


def solution(mesh):
    dims = (mesh.shape["gx"], mesh.shape["gy"])
    assert mesh.shape["gz"] == 2
    return jax.shard_map(
        functools.partial(on_device, dims),
        mesh=mesh,
        in_specs=(
            P("gx", "gy", "gz", None),
            P(),
            P(),
            P(None, None, None, None, "gx"),
            P(None, None, None, None, "gx"),
            P(),
        ),
        out_specs=P("gx", "gy", "gz", None),
        check_vma=False,
    )
```

```python
import functools

import jax
import jax.numpy as jnp
from jax import lax
from jax.experimental import pallas as pl
from jax.experimental.pallas import tpu as pltpu
from jax.sharding import PartitionSpec as P

F32 = jnp.float32
BF16 = jnp.bfloat16
STEPS = [(dx, dy) for dx in (-1, 0, 1) for dy in (-1, 0, 1)]


def span(d, n, pad):
    if d == 0:
        return pl.ds(pad, n), pl.ds(1, n)
    if d < 0:
        return pl.ds(pad, 1), pl.ds(n + 1, 1)
    return pl.ds(pad + n - 1, 1), pl.ds(0, 1)


def halves(pairs, refs):
    for i, ref in enumerate(refs):
        total = None
        for lhs, rhs in pairs[i::2]:
            part = jnp.dot(lhs, rhs, preferred_element_type=F32)
            total = part if total is None else total + part
        ref[...] = total


def kernel(
    dims,
    v_h, wf_h, wh_h, w1_h, w2_h, wu_h,
    out,
    wf, wh, w1, w2, wus, wuu, wsem, vsem, wt, wz,
    p1, f1, g1, gs, e1, a1, rz, t1,
    p2, f2, g2, e2, o2,
    p3, f3, g3, e3, o3, acc,
    pk2, l2, m2, sel2, selm, q2, b2, pk3, l3, q3, b3, pk4, l4, up, sums, deeps, brims, thirds, ends,
    s1, r1, s2, r2, s3, r3, s4, r4, s5, r5, s6, r6,
):
    gxn, gyn = dims
    gx, gy, gz = lax.axis_index("gx"), lax.axis_index("gy"), lax.axis_index("gz")
    oz = 1 - gz

    nx, ny, nz, c0 = v_h.shape
    fetch = pltpu.make_async_copy(v_h, p1.at[1 : nx + 1, 1 : ny + 1], vsem)
    fetch.start()
    c2 = w2.shape[1]
    loads = [
        pltpu.make_async_copy(src, dst, wsem.at[i])
        for i, (src, dst) in enumerate((
            (wf_h, wf), (wh_h, wh), (w1_h, w1), (w2_h, w2), (wu_h.at[:, c2:], wus), (wu_h.at[:, :c2], wuu),
        ))
    ]

    def on(cond, fn):
        if cond is True:
            fn()
        else:
            pl.when(cond)(fn)

    def exists(dx, dy):
        conds = []
        if dx < 0:
            conds.append(gx > 0)
        if dx > 0:
            conds.append(gx < gxn - 1)
        if dy < 0:
            conds.append(gy > 0)
        if dy > 0:
            conds.append(gy < gyn - 1)
        if not conds:
            return True
        return functools.reduce(jnp.logical_and, conds)

    for x in (0, nx + 1):
        p1[x] = jnp.zeros(p1.shape[1:], BF16)
    for y in (0, ny + 1):
        p1[1 : nx + 1, y] = jnp.zeros((nx, nz, c0), BF16)
    for ref in (g1, m2, l3, l4):
        ref[...] = jnp.zeros(ref.shape, ref.dtype)

    barrier = pltpu.get_barrier_semaphore()
    for s in range(gxn):
        there = lax.rem(gx + s, gxn)
        for dy in (-1, 0, 1):
            for z in (0, 1):
                if s == 0 and dy == 0 and z == 0:
                    continue

                def signal(there=there, dy=dy, z=z):
                    pl.semaphore_signal(
                        barrier, inc=1,
                        device_id={"gx": there, "gy": gy + dy, "gz": oz if z else gz},
                        device_id_type=pl.DeviceIdType.MESH,
                    )

                on(exists(0, dy), signal)
    loads[0].start()
    lines = 1 + (gy > 0).astype(jnp.int32) + (gy < gyn - 1).astype(jnp.int32)

    def edge(block):
        size = block.shape[-2]
        rows = lax.broadcasted_iota(jnp.int32, block.shape, block.ndim - 2)
        return jnp.sum(jnp.where(rows == (size - 1) * oz, block, 0.0), axis=block.ndim - 2, keepdims=True)

    for ref in (g2, g3):
        ref[...] = jnp.zeros(ref.shape, ref.dtype)
    for ref in (p2, p3):
        for x in (0, ref.shape[0] - 1):
            ref[x] = jnp.zeros(ref.shape[1:], BF16)
        for y in (0, ref.shape[1] - 1):
            ref[:, y] = jnp.zeros(ref.shape[:1] + ref.shape[2:], BF16)
    fetch.wait()
    for load in loads[1:]:
        load.start()
    for x in range(nx):
        f1[x] = edge(p1[x + 1, 1 : ny + 1].astype(F32))
    pl.semaphore_wait(barrier, 2 * gxn * lines - 1)

    def send(src, dst, ss, rs, x, y, z):
        return pltpu.make_async_remote_copy(
            src_ref=src, dst_ref=dst, send_sem=ss, recv_sem=rs,
            device_id={"gx": x, "gy": y, "gz": z}, device_id_type=pl.DeviceIdType.MESH,
        )

    many_x = jnp.logical_and(gx > 0, gx < gxn - 1)
    many_y = jnp.logical_and(gy > 0, gy < gyn - 1)

    def by_y(fn):
        for b in (1, 2):
            pl.when(many_y if b == 2 else jnp.logical_not(many_y))(functools.partial(fn, b))

    def by_xy(fn):
        for a in (1, 2):
            for b in (1, 2):
                cx_ = many_x if a == 2 else jnp.logical_not(many_x)
                cy_ = many_y if b == 2 else jnp.logical_not(many_y)
                pl.when(jnp.logical_and(cx_, cy_))(functools.partial(fn, a, b))

    def drain(ref, sem):
        pltpu.make_async_copy(ref, ref, sem).wait()

    stage = pl.when(gx < gxn)
    late = []

    def neighbours(src, pad, face, rim, side, nx, ny, ss, rs):
        for dx, dy in STEPS:
            sx, tx = span(dx, nx, pad)
            sy, ty = span(dy, ny, pad)
            fx, _ = span(dx, nx, 0)
            fy, _ = span(dy, ny, 0)
            copies = [send(face.at[fx, fy], side.at[tx, ty], ss.at[0], rs.at[0], gx + dx, gy + dy, oz)]
            if (dx, dy) != (0, 0):
                k = 1 if dx else 2
                copies.append(send(src.at[sx, sy], rim.at[tx, ty], ss.at[k], rs.at[k], gx + dx, gy + dy, gz))
            for copy in copies:
                on(exists(dx, dy), copy.start)

        def finish(sems):
            def both(a, b):
                drain(side.at[0 : nx + a, 0 : ny + b], sems.at[0])
                drain(rim.at[0:a, 0 : ny + b], sems.at[1])
                drain(rim.at[0:nx, 0:b], sems.at[2])

            by_xy(both)

        late.append(lambda: finish(ss))
        return lambda: finish(rs)

    def shifted(block, fill):
        size = block.shape[-2]
        axis = block.ndim - 2
        rows = lax.broadcasted_iota(jnp.int32, block.shape, axis)
        below = jnp.where(rows == 0, 0.0, pltpu.roll(block, 1, axis))
        above = jnp.where(rows == size - 1, 0.0, pltpu.roll(block, size - 1, axis))
        if fill is not None:
            fill = jnp.broadcast_to(fill, block.shape)
            below = jnp.where(rows == jnp.where(gz == 1, 0, -1), fill, below)
            above = jnp.where(rows == jnp.where(gz == 0, size - 1, -1), fill, above)
        return below, above

    def rounded(x):
        return x.astype(BF16).astype(F32)

    arrived = neighbours(p1, 1, f1, p1, g1, nx, ny, s1, r1)

    k0 = 3 * c0
    for x in (0, nx + 1):
        e1[x] = jnp.zeros(e1.shape[1:], BF16)
    for y in (0, ny + 1):
        e1[1 : nx + 1, y] = jnp.zeros((nx, nz, k0), BF16)

    def widen(at, block):
        block = block.astype(F32)
        below, above = shifted(block, None)
        for k, part in enumerate((below, block, above)):
            e1[at + (slice(None), pl.ds(k * c0, c0))] = part.astype(BF16)

    @pl.loop(1, nx + 1)
    def _(x):
        widen((x, pl.ds(1, ny)), p1[x, 1 : ny + 1])

    loads[0].wait()
    for oy in range(3):
        for plane in range(4):
            at = pl.ds(plane * k0, k0)
            wt[oy, at, :c0] = wf[plane * 3 + oy] if plane < 3 else jnp.zeros((k0, c0), BF16)
            wt[oy, at, c0:] = wf[(plane - 1) * 3 + oy] if plane > 0 else jnp.zeros((k0, c0), BF16)
    for tap in range(9):
        wz[pl.ds(tap * c0, c0)] = wf[tap, pl.ds(pl.multiple_of(2 * oz * c0, c0), c0)]

    @pl.loop(0, nx // 2)
    def _(x):
        total = jnp.zeros((ny * nz, 2 * c0), F32)
        for oy in range(3):
            for half in range(2):
                lhs = [e1[2 * x + 2 * half + i, oy : oy + ny].reshape(ny * nz, k0) for i in range(2)]
                rhs = wt[oy, 2 * half * k0 : 2 * (half + 1) * k0]
                total = total + jnp.dot(jnp.concatenate(lhs, axis=1), rhs, preferred_element_type=F32)
        a1[x] = total

    arrived()
    for x in range(nx + 2):
        for y in range(ny + 2):
            gs[x, y : y + 1] = g1[x, y]
    @stage
    def _():
        lhs = [gs[ox : ox + nx, oy : oy + ny].reshape(nx * ny, c0).astype(BF16) for ox in range(3) for oy in range(3)]
        rz[...] = jnp.dot(jnp.concatenate(lhs, axis=1), wz[...], preferred_element_type=F32)
        for x, ox, lane in ((0, 0, 0), (nx + 1, 2, c0)):
            widen((x, pl.ds(1, ny)), p1[x, 1 : ny + 1])
            lhs = [e1[x, oy : oy + ny].reshape(ny * nz, k0) for oy in range(3)]
            rhs = wf[ox * 3 : ox * 3 + 3].reshape(3 * k0, c0)
            part = jnp.dot(jnp.concatenate(lhs, axis=1), rhs, preferred_element_type=F32)
            at = (0 if ox == 0 else nx // 2 - 1, slice(None), pl.ds(lane, c0))
            a1[at] = a1[at] + part
        for y, oy in ((0, 0), (ny + 1, 2)):
            widen((pl.ds(0, nx + 2), y), p1[:, y])
            lhs = [e1[ox : ox + nx, y].reshape(nx * nz, k0) for ox in range(3)]
            rhs = jnp.concatenate([wf[ox * 3 + oy] for ox in range(3)], axis=0)
            part = jnp.dot(jnp.concatenate(lhs, axis=1), rhs, preferred_element_type=F32).reshape(nx, nz, c0)
            for x in range(nx):
                at = (x // 2, pl.ds((0 if oy == 0 else ny - 1) * nz, nz), pl.ds(x % 2 * c0, c0))
                a1[at] = a1[at] + part[x]

    tile = 8
    last = lax.broadcasted_iota(jnp.int32, (tile, c0), 0) == (tile - 1) * oz
    for x in range(nx):
        for y in range(ny):
            at = (x // 2, pl.ds(pl.multiple_of(y * nz + (nz - tile) * oz, tile), tile), pl.ds(x % 2 * c0, c0))
            row = jnp.broadcast_to(rz[x * ny + y : x * ny + y + 1], (tile, c0))
            a1[at] = a1[at] + jnp.where(last, row, 0.0)

    hx, hy, hz = nx // 2, ny // 2, nz // 2

    @pl.loop(0, hx)
    def _(x):
        total = a1[x]
        both = jnp.maximum(jnp.maximum(total[:, :c0], total[:, c0:]), 0.0).reshape(hy, 2, nz, c0)
        t1[...] = jnp.max(both, axis=1)
        small = jnp.maximum(t1[:, pl.ds(0, hz, stride=2), :], t1[:, pl.ds(1, hz, stride=2), :])
        small = rounded(small)
        p2[x + 1, 1 : hy + 1] = small.astype(BF16)
        f2[x] = edge(small)

    arrived = neighbours(p2, 1, f2, p2, g2, hx, hy, s2, r2)
    arrived()
    rows = hx * hy * hz

    def pack(even, odd, at, block, lane):
        n, size, c = block.shape
        even[at, :, :, pl.ds(lane, c)] = block.reshape(n * size, c).astype(BF16).reshape(n // 2, 2 * size, c)
        block = block[1 : n - 1]
        odd[at, :, :, pl.ds(lane, c)] = block.reshape((n - 2) * size, c).astype(BF16).reshape(n // 2 - 1, 2 * size, c)

    def conv(even, odd, p, g, w):
        for x in range(hx + 2):
            block = p[x].astype(F32)
            c = block.shape[-1]
            below, above = shifted(block, g[x])
            for k, part in enumerate((below, block, above)):
                pack(even, odd, x, part, k * c)
        @stage
        def _():
            pairs = []
            for ox in range(3):
                for oy, (r, lo) in enumerate(((even, 0), (odd, 0), (even, 1))):
                    rhs = w[ox * 9 + oy * 3 : ox * 9 + oy * 3 + 3].reshape(3 * c, w.shape[2])
                    pairs.append((r[ox : ox + hx, lo : lo + hy // 2].reshape(rows, 3 * c), rhs))
            halves(pairs, (sums.at[0], sums.at[1]))

        return sums[0] + sums[1]

    loads[1].wait()
    c1 = wh.shape[2]
    total = conv(e2, o2, p2, g2, wh)
    skip = rounded(jnp.maximum(total, 0.0)).reshape(hx, hy, hz, c1)
    p3[1 : hx + 1, 1 : hy + 1] = skip.astype(BF16)
    f3[...] = edge(skip)

    cx, cy, cz = hx // 2, hy // 2, hz // 2
    ax = gxn * cx
    group = cz * cx
    m = jnp.max(skip.reshape(cx, 2, cy, 2, hz, c1), axis=(1, 3))
    m = m.reshape(cx * cy * hz, c1)
    m = jnp.maximum(m, pltpu.roll(m, m.shape[0] - 1, 0)).astype(BF16)

    blocks = []
    lane = lax.broadcasted_iota(jnp.int32, (group, cx * cy * hz), 1)
    sub = lax.broadcasted_iota(jnp.int32, (group, cx * cy * hz), 0)
    shift_x = cx.bit_length() - 1
    sub_x = sub & (cx - 1)
    sub_o = sub >> shift_x
    for y in range(cy):
        blocks.append(jnp.where(lane == (sub_x * cy + y) * hz + 2 * sub_o, 1.0, 0.0))
    blocks.append(jnp.where(lane == (sub_x * cy + sub_o) * hz + 2 * (cz - 1) * oz, 1.0, 0.0))
    pick = jnp.concatenate(blocks, axis=0).astype(BF16)
    packets = jnp.dot(pick, m, preferred_element_type=F32).reshape(cy + 1, group, c1).astype(BF16)
    pk2[...] = packets
    l2[gx, 0:cy] = packets[0:cy]

    def coarse_copy(k, dy, z):
        def make(src_gx, tgt_gx):
            if z == 0:
                src = {0: pl.ds(0, cy), -1: pl.ds(0, 1), 1: pl.ds(cy - 1, 1)}[dy]
            else:
                src = pl.ds(cy, 1)
            if dy == 0:
                dst = l2.at[src_gx, pl.ds(cy, 1) if z else pl.ds(0, cy)]
            else:
                dst = m2.at[src_gx, pl.ds(2 * z + (1 if dy < 0 else 0), 1)]
            return send(pk2.at[src], dst, s4.at[k], r4.at[k], tgt_gx, gy + dy, oz if z else gz)

        return make

    def deep_copy(pk, land, ss, rs):
        def choose(k, dy, z):
            def make(src_gx, tgt_gx):
                sy, ty = span(dy, cy, 0)
                sender = gz if src_gx is gx else (oz if z else gz)
                if z == 0:
                    src = pk.at[sy]
                    dst = land.at[src_gx, ty, pl.ds(1, cz)]
                else:
                    src = pk.at[sy, pl.ds((cz - 1) * (1 - sender), 1)]
                    dst = land.at[src_gx, ty, pl.ds((cz + 1) * sender, 1)]
                return send(src, dst, ss.at[k], rs.at[k], tgt_gx, gy + dy, oz if z else gz)

            return make

        return choose

    def narrow_copy(k, dy, z):
        def make(src_gx, tgt_gx):
            sy, ty = span(dy, cy, 0)
            sender = gz if src_gx is gx else (oz if z else gz)
            if z == 0:
                src = pk4.at[tgt_gx, sy]
                dst = l4.at[src_gx, ty, pl.ds(1, cz // 2)]
            else:
                src = pk4.at[tgt_gx, sy, pl.ds((cz // 2 - 1) * (1 - sender), 1)]
                dst = l4.at[src_gx, ty, pl.ds((cz // 2 + 1) * sender, 1)]
            return send(src, dst, s6.at[k], r6.at[k], tgt_gx, gy + dy, oz if z else gz)

        return make

    def column_exchange(choose, main, rim):
        far = list(range(1, gxn))
        for s, dy, z in (
            [(s, 0, 0) for s in far]
            + [(s, 0, 1) for s in far + [0]]
            + [(s, dy, 0) for s in far + [0] for dy in (-1, 1)]
            + [(s, dy, 1) for s in far + [0] for dy in (-1, 1)]
        ):
            k = 2 if dy else (0 if s else 1)
            on(exists(0, dy), choose(k, dy, z)(gx, lax.rem(gx + s, gxn)).start)

        def first(which):
            for k, ref in enumerate(main):
                drain(ref, which.at[k])

        def second(which):
            by_y(lambda b: drain(rim(b), which.at[2]))

        return first, second

    def leave(waits, sems):
        late.append(lambda: [wait(sems) for wait in waits])
        return waits

    def parts_of(land):
        wz = land.shape[2] - 2
        main = (land.at[0 : gxn - 1, 0:cy, 0 : wz + 1], land.at[0, 0:cy, 0:1])
        return main, lambda b: land.at[0:gxn, 0:b, 0 : wz + 1]

    main4, rim4 = leave(
        column_exchange(coarse_copy, (l2.at[0 : gxn - 1], l2.at[0, 0:1]), lambda b: m2.at[0:gxn, 0 : 2 * b]), s4
    )

    def one_hot(ref, at, slots):
        width = gxn * slots * group
        lane = lax.broadcasted_iota(jnp.int32, (ax, width), 1)
        xs = lax.broadcasted_iota(jnp.int32, (ax, width), 0)
        base = lane - ((xs >> shift_x) * slots * group + (xs & (cx - 1)))
        ref[at] = jnp.where(base == slots_at, 1.0, 0.0)

    for y in range(-1, cy + 1):
        for z in range(-1, cz + 1):
            inside = 0 <= y < cy
            rim_slot = 0 if y < 0 else 1
            if 0 <= z < cz:
                slots_at = (y if inside else rim_slot) * group + z * cx
            else:
                line = y if inside else (cy - 1 if y < 0 else 0)
                mine = (gz == 1) if z < 0 else (gz == 0)
                slots_at = jnp.where(mine, (cy if inside else 2 + rim_slot) * group + line * cx, -(1 << 20))
            if inside:
                one_hot(sel2, (y, z + 1), cy + 1)
            else:
                one_hot(selm, (rim_slot, z + 1), 4)

    def gathered(ref, land):
        n, width = ref.shape[0], ref.shape[-1]
        select = ref[...].reshape(n * (cz + 2) * ax, width).astype(BF16)
        landed = land[...].astype(F32).reshape(width, c1).astype(BF16)
        return jnp.dot(select, landed, preferred_element_type=F32).reshape(n, cz + 2, ax, c1)

    deep = cy * cz * ax
    fo = w1.shape[2]

    windows = ((0, 0), (1, 0), (0, 1))

    def spread(even, odd, block, row):
        below, above = shifted(block, None)
        n, c = block.shape[0], block.shape[-1]
        for ox, part in enumerate((below, block, above)):
            whole = part.reshape(n * (cz + 2) * ax, c).astype(BF16)
            even[ox, row : row + n] = whole.reshape(n, cz // 2 + 1, 2 * ax, c)
            inner = part[:, 1 : cz + 1].reshape(n * cz * ax, c).astype(BF16)
            odd[ox, row : row + n] = inner.reshape(n, cz // 2, 2 * ax, c)

    def window(pair, ox, row, n):
        c = pair[0].shape[-1]
        lhs = [pair[i][ox, row : row + n, lo : lo + cz // 2].reshape(n * cz * ax, c) for i, lo in windows]
        return jnp.concatenate(lhs, axis=1)

    def bottom_own(pair, w):
        @stage
        def _():
            k = 3 * w.shape[1]
            pairs = []
            for ox in range(3):
                lhs = window(pair, ox, 1, cy)
                rhs = [w[ox * 9 + oy * 3 : ox * 9 + oy * 3 + 3].reshape(k, fo) for oy in range(3)]
                rhs = jnp.concatenate(rhs, axis=1)
                pairs += [(lhs[:, : k // 2], rhs[: k // 2]), (lhs[:, k // 2 :], rhs[k // 2 :])]
            halves(pairs, (deeps.at[0], deeps.at[1]))

    def bottom_rim(pair, w):
        k = 3 * w.shape[1]
        size = cz * ax
        @stage
        def _():
            for side, (row, oy) in enumerate(((0, 0), (cy + 1, 2))):
                total = jnp.zeros((size, fo), F32)
                for ox in range(3):
                    rhs = w[(ox * 3 + oy) * 3 : (ox * 3 + oy) * 3 + 3].reshape(k, fo)
                    total = total + jnp.dot(window(pair, ox, row, 1), rhs, preferred_element_type=F32)
                brims[side] = total

        def own(oy, y):
            at = (pl.ds(y * size, size), pl.ds(oy * fo, fo))
            return deeps[(0, *at)] + deeps[(1, *at)]

        lines = []
        for y in range(cy):
            before = own(0, y - 1) if y > 0 else brims[0]
            after = own(2, y + 1) if y < cy - 1 else brims[1]
            lines.append(own(1, y) + before + after)
        return jnp.maximum(jnp.concatenate(lines, axis=0), 0.0).reshape(cy, cz, ax, fo).astype(BF16)

    main4(r4)
    skip_arrived = neighbours(p3, 1, f3, p3, g3, hx, hy, s3, r3)
    spread(q2, b2, gathered(sel2, l2), 1)
    loads[2].wait()
    bottom_own((q2, b2), w1)
    rim4(r4)
    block = gathered(selm, m2)
    spread(q2, b2, block[0:1], 0)
    spread(q2, b2, block[1:2], cy + 1)
    first = bottom_rim((q2, b2), w1)
    pk3[...] = first
    l3[gx, 1 : cy + 1, 1 : cz + 1] = first
    main5, rim5 = leave(column_exchange(deep_copy(pk3, l3, s5, r5), *parts_of(l3)), s5)

    skip_arrived()
    loads[4].wait()
    total = conv(e3, o3, p3, g3, wus)
    acc[...] = total.reshape(hx, hy, hz, c1)

    near = cx + 2
    wide = gxn * cz * near
    lane = lax.broadcasted_iota(jnp.int32, (wide, cz * ax), 1)
    row = lax.broadcasted_iota(jnp.int32, (wide, cz * ax), 0)
    shift_n = near.bit_length() - 1
    shift_z = cz.bit_length() - 1
    at = (row >> (shift_n + shift_z)) * cx + (row & (near - 1)) - 1
    at = jnp.where(jnp.logical_and(at >= 0, at < ax), at, -(cz + 1) * ax)
    share = jnp.where(lane == ((row >> shift_n) & (cz - 1)) * ax + at, 1.0, 0.0).astype(BF16)

    lane = lax.broadcasted_iota(jnp.int32, (hz, (cz + 4) * near), 1)
    zs = lax.broadcasted_iota(jnp.int32, (hz, (cz + 4) * near), 0)
    blocks = []
    for k in range(3):
        for x in range(-1, hx + 1):
            blocks.append(jnp.where(lane == (((zs + (k - 1)) >> 1) + 2) * near + (x >> 1) + 1, 1.0, 0.0))
    for k in range(3):
        blocks += blocks[k * (hx + 2) + 1 : (k + 1) * (hx + 2) - 1]
    pick = jnp.concatenate(blocks, axis=0).astype(BF16)

    def joined(row, n):
        return jnp.concatenate([l3[g, row : row + n].astype(F32) for g in range(gxn)], axis=-1)

    main5(r5)
    spread(q3, b3, joined(1, cy), 1)
    loads[3].wait()
    bottom_own((q3, b3), w2)
    rim5(r5)
    spread(q3, b3, joined(0, 1), 0)
    spread(q3, b3, joined(cy + 1, 1), cy + 1)
    second = bottom_rim((q3, b3), w2)
    for y in range(cy):
        line = second[y].astype(F32).reshape(cz * ax, fo).astype(BF16)
        line = jnp.dot(share, line, preferred_element_type=F32)
        pk4[:, y] = line.reshape(gxn, cz // 2, 2 * near, fo).astype(BF16)
    l4[gx, 1 : cy + 1, 1 : cz // 2 + 1] = pk4[gx]
    main6, rim6 = leave(column_exchange(narrow_copy, *parts_of(l4)), s6)
    size = hx * hz

    def enlarge(ys):
        fields = [l4[g, y].astype(F32).reshape((cz + 4) * near, fo) for y in ys for g in range(gxn)]
        fields = jnp.concatenate(fields, axis=-1).astype(BF16)
        fields = jnp.dot(pick, fields, preferred_element_type=F32).astype(BF16)
        for i, y in enumerate(ys):
            field = fields[:, i * c2 : (i + 1) * c2]
            for k in range(3):
                at = pl.ds(k * c2, c2)
                part = field[k * (size + 2 * hz) : (k + 1) * (size + 2 * hz)]
                up[0, y, :, :, at] = part[:size].reshape(hx // 2, 2 * hz, c2)
                up[2, y, :, :, at] = part[2 * hz :].reshape(hx // 2, 2 * hz, c2)
                part = field[3 * (size + 2 * hz) + k * size : 3 * (size + 2 * hz) + (k + 1) * size]
                up[1, y, :, :, at] = part.reshape(hx // 2, 2 * hz, c2)

    main6(r6)
    enlarge(range(1, cy + 1))
    loads[5].wait()

    @stage
    def _():
        for oy in range(3):
            pairs = []
            for ox in range(3):
                for k in range(3):
                    lhs = up[ox, 1 : cy + 1, :, :, pl.ds(k * c2, c2)].reshape(cy * size, c2)
                    pairs.append((lhs, wuu[ox * 9 + oy * 3 + k]))
            halves(pairs, (thirds.at[0, oy], thirds.at[1, oy]))

    for y in range(hy):
        line = acc[:, y]
        for oy in range(3):
            at = (y + oy + 1) // 2 - 1
            if 0 <= at < cy:
                part = thirds[0, oy, at * size : (at + 1) * size] + thirds[1, oy, at * size : (at + 1) * size]
                line = line + part.reshape(hx, hz, c1)
        if 0 < y < hy - 1:
            out[:, y] = line.astype(BF16)
        else:
            acc[:, y] = line
    rim6(r6)
    enlarge((0, cy + 1))
    @stage
    def _():
        for side, (row, oy) in enumerate(((0, 0), (cy + 1, 2))):
            total = jnp.zeros((size, c1), F32)
            for ox in range(3):
                rhs = wuu[(ox * 3 + oy) * 3 : (ox * 3 + oy) * 3 + 3].reshape(3 * c2, c1)
                total = total + jnp.dot(up[ox, row].reshape(size, 3 * c2), rhs, preferred_element_type=F32)
            ends[side] = total

    for side, y in enumerate((0, hy - 1)):
        out[:, y] = (acc[:, y] + ends[side].reshape(hx, hz, c1)).astype(BF16)

    for fn in late:
        fn()


def on_device(dims, volume, w_full, w_half, w_bottom_in, w_bottom_out, w_up):
    gxn, gyn = dims
    nx, ny, nz, c0 = volume.shape
    c1 = w_half.shape[4]
    c2, fo = w_bottom_out.shape[3:]
    hx, hy, hz = nx // 2, ny // 2, nz // 2
    cx, cy, cz = hx // 2, hy // 2, hz // 2
    ax = gxn * cx
    weights = [
        w_full.reshape(9, 3 * c0, c0),
        w_half.reshape(27, c0, c1),
        w_bottom_in.reshape(27, c1, fo),
        w_bottom_out.reshape(27, c2, fo),
        w_up.reshape(27, c2 + c1, c1),
    ]
    vm = pltpu.VMEM
    dma = pltpu.SemaphoreType.DMA
    scratch = [vm(w.shape, BF16) for w in weights[:4]]
    scratch += [vm((27, c1, c1), BF16), vm((27, c2, c1), BF16), dma((6,)), dma(())]
    scratch += [vm((3, 12 * c0, 2 * c0), BF16), vm((9 * c0, c0), BF16)]
    scratch += [
        vm((nx + 2, ny + 2, nz, c0), BF16), vm((nx, ny, 1, c0), F32), vm((nx + 2, ny + 2, 1, c0), F32),
        vm((nx + 2, ny + 2, c0), F32), vm((nx + 2, ny + 2, nz, 3 * c0), BF16), vm((hx, ny * nz, 2 * c0), F32),
        vm((nx * ny, c0), F32), vm((hy, nz, c0), F32),
        vm((hx + 2, hy + 2, hz, c0), BF16), vm((hx, hy, 1, c0), F32), vm((hx + 2, hy + 2, 1, c0), F32),
        vm((hx + 2, hy // 2 + 1, 2 * hz, 3 * c0), BF16), vm((hx + 2, hy // 2, 2 * hz, 3 * c0), BF16),
        vm((hx + 2, hy + 2, hz, c1), BF16), vm((hx, hy, 1, c1), F32), vm((hx + 2, hy + 2, 1, c1), F32),
        vm((hx + 2, hy // 2 + 1, 2 * hz, 3 * c1), BF16), vm((hx + 2, hy // 2, 2 * hz, 3 * c1), BF16),
        vm((hx, hy, hz, c1), F32),
        vm((cy + 1, cz * cx, c1), BF16), vm((gxn, cy + 1, cz * cx, c1), BF16), vm((gxn, 4, cz * cx, c1), BF16),
        vm((cy, cz + 2, ax, gxn * (cy + 1) * cz * cx), F32), vm((2, cz + 2, ax, gxn * 4 * cz * cx), F32),
        vm((3, cy + 2, cz // 2 + 1, 2 * ax, c1), BF16), vm((3, cy + 2, cz // 2, 2 * ax, c1), BF16),
        vm((cy, cz, ax, fo), BF16), vm((gxn, cy + 2, cz + 2, ax, fo), BF16),
        vm((3, cy + 2, cz // 2 + 1, 2 * ax, c2), BF16), vm((3, cy + 2, cz // 2, 2 * ax, c2), BF16),
        vm((gxn, cy, cz // 2, 2 * (cx + 2), fo), BF16), vm((gxn, cy + 2, cz // 2 + 2, 2 * (cx + 2), fo), BF16),
        vm((3, cy + 2, hx // 2, 2 * hz, 3 * c2), BF16),
        vm((2, hx * hy * hz, c1), F32), vm((2, cy * cz * ax, 3 * fo), F32), vm((2, cz * ax, fo), F32),
        vm((2, 3, cy * hx * hz, c1), F32), vm((2, hx * hz, c1), F32),
    ]
    scratch += [dma((3,))] * 12
    return pl.pallas_call(
        functools.partial(kernel, dims),
        out_shape=jax.ShapeDtypeStruct((hx, hy, hz, c1), BF16),
        in_specs=[pl.BlockSpec(memory_space=pltpu.HBM)] * 6,
        out_specs=pl.BlockSpec(memory_space=pltpu.VMEM),
        scratch_shapes=scratch,
        compiler_params=pltpu.CompilerParams(
            collective_id=0, has_side_effects=True, vmem_limit_bytes=52 * 1024 * 1024
        ),
    )(*[pltpu.with_memory_space_constraint(a, pltpu.HBM) for a in (volume, *weights)])


def solution(mesh):
    dims = (mesh.shape["gx"], mesh.shape["gy"])
    assert mesh.shape["gz"] == 2
    return jax.shard_map(
        functools.partial(on_device, dims),
        mesh=mesh,
        in_specs=(
            P("gx", "gy", "gz", None),
            P(),
            P(),
            P(None, None, None, None, "gx"),
            P(None, None, None, None, "gx"),
            P(),
        ),
        out_specs=P("gx", "gy", "gz", None),
        check_vma=False,
    )
```

```python
import functools

import jax
import jax.numpy as jnp
from jax import lax
from jax.experimental import pallas as pl
from jax.experimental.pallas import tpu as pltpu
from jax.sharding import PartitionSpec as P

F32 = jnp.float32
BF16 = jnp.bfloat16
STEPS = [(dx, dy) for dx in (-1, 0, 1) for dy in (-1, 0, 1)]


def span(d, n, pad):
    if d == 0:
        return pl.ds(pad, n), pl.ds(1, n)
    if d < 0:
        return pl.ds(pad, 1), pl.ds(n + 1, 1)
    return pl.ds(pad + n - 1, 1), pl.ds(0, 1)


def halves(pairs, refs):
    for i, ref in enumerate(refs):
        total = None
        for lhs, rhs in pairs[i::2]:
            part = jnp.dot(lhs, rhs, preferred_element_type=F32)
            total = part if total is None else total + part
        ref[...] = total


def kernel(
    dims,
    v_h, wf_h, wh_h, w1_h, w2_h, wu_h,
    out,
    wf, wh, w1, w2, wus, wuu, wsem, vsem, wt, wz,
    p1, f1, g1, gs, e1, a1, rz, t1,
    p2, f2, g2, e2, o2,
    p3, f3, g3, e3, o3, acc,
    pk2, l2, m2, sel2, selm, q2, b2, pk3, l3, q3, b3, pk4, l4, up, sums, deeps, brims, thirds, ends,
    s1, r1, s2, r2, s3, r3, s4, r4, s5, r5, s6, r6,
):
    gxn, gyn = dims
    gx, gy, gz = lax.axis_index("gx"), lax.axis_index("gy"), lax.axis_index("gz")
    oz = 1 - gz

    nx, ny, nz, c0 = v_h.shape
    fetch = pltpu.make_async_copy(v_h, p1.at[1 : nx + 1, 1 : ny + 1], vsem)
    fetch.start()
    c2 = w2.shape[1]
    loads = [
        pltpu.make_async_copy(src, dst, wsem.at[i])
        for i, (src, dst) in enumerate((
            (wf_h, wf), (wh_h, wh), (w1_h, w1), (w2_h, w2), (wu_h.at[:, c2:], wus), (wu_h.at[:, :c2], wuu),
        ))
    ]

    def on(cond, fn):
        if cond is True:
            fn()
        else:
            pl.when(cond)(fn)

    def exists(dx, dy):
        conds = []
        if dx < 0:
            conds.append(gx > 0)
        if dx > 0:
            conds.append(gx < gxn - 1)
        if dy < 0:
            conds.append(gy > 0)
        if dy > 0:
            conds.append(gy < gyn - 1)
        if not conds:
            return True
        return functools.reduce(jnp.logical_and, conds)

    for x in (0, nx + 1):
        p1[x] = jnp.zeros(p1.shape[1:], BF16)
    for y in (0, ny + 1):
        p1[1 : nx + 1, y] = jnp.zeros((nx, nz, c0), BF16)
    for ref in (g1, m2, l3, l4):
        ref[...] = jnp.zeros(ref.shape, ref.dtype)

    barrier = pltpu.get_barrier_semaphore()
    for s in range(gxn):
        there = lax.rem(gx + s, gxn)
        for dy in (-1, 0, 1):
            for z in (0, 1):
                if s == 0 and dy == 0 and z == 0:
                    continue

                def signal(there=there, dy=dy, z=z):
                    pl.semaphore_signal(
                        barrier, inc=1,
                        device_id={"gx": there, "gy": gy + dy, "gz": oz if z else gz},
                        device_id_type=pl.DeviceIdType.MESH,
                    )

                on(exists(0, dy), signal)
    loads[0].start()
    lines = 1 + (gy > 0).astype(jnp.int32) + (gy < gyn - 1).astype(jnp.int32)

    def edge(block):
        size = block.shape[-2]
        rows = lax.broadcasted_iota(jnp.int32, block.shape, block.ndim - 2)
        return jnp.sum(jnp.where(rows == (size - 1) * oz, block, 0.0), axis=block.ndim - 2, keepdims=True)

    for ref in (g2, g3):
        ref[...] = jnp.zeros(ref.shape, ref.dtype)
    for ref in (p2, p3):
        for x in (0, ref.shape[0] - 1):
            ref[x] = jnp.zeros(ref.shape[1:], BF16)
        for y in (0, ref.shape[1] - 1):
            ref[:, y] = jnp.zeros(ref.shape[:1] + ref.shape[2:], BF16)
    fetch.wait()
    for load in loads[1:]:
        load.start()
    for x in range(nx):
        f1[x] = edge(p1[x + 1, 1 : ny + 1].astype(F32))
    pl.semaphore_wait(barrier, 2 * gxn * lines - 1)

    def send(src, dst, ss, rs, x, y, z):
        return pltpu.make_async_remote_copy(
            src_ref=src, dst_ref=dst, send_sem=ss, recv_sem=rs,
            device_id={"gx": x, "gy": y, "gz": z}, device_id_type=pl.DeviceIdType.MESH,
        )

    many_x = jnp.logical_and(gx > 0, gx < gxn - 1)
    many_y = jnp.logical_and(gy > 0, gy < gyn - 1)

    def by_y(fn):
        for b in (1, 2):
            pl.when(many_y if b == 2 else jnp.logical_not(many_y))(functools.partial(fn, b))

    def by_xy(fn):
        for a in (1, 2):
            for b in (1, 2):
                cx_ = many_x if a == 2 else jnp.logical_not(many_x)
                cy_ = many_y if b == 2 else jnp.logical_not(many_y)
                pl.when(jnp.logical_and(cx_, cy_))(functools.partial(fn, a, b))

    def drain(ref, sem):
        pltpu.make_async_copy(ref, ref, sem).wait()

    stage = pl.when(gx < gxn)
    short = jnp.minimum(gx, gxn - 1 - gx)
    farthest = []
    for i in range(gxn - 1, 0, -1):
        paired = gx + ((i + 1) // 2 if i % 2 else -(i // 2))
        rest = jnp.where(gx < gxn - 1 - gx, gx + (i - short), gx - (i - short))
        farthest.append(jnp.where(i <= 2 * short, paired, rest))

    late = []

    def neighbours(src, pad, face, rim, side, nx, ny, ss, rs):
        for dx, dy in STEPS:
            sx, tx = span(dx, nx, pad)
            sy, ty = span(dy, ny, pad)
            fx, _ = span(dx, nx, 0)
            fy, _ = span(dy, ny, 0)
            copies = [send(face.at[fx, fy], side.at[tx, ty], ss.at[0], rs.at[0], gx + dx, gy + dy, oz)]
            if (dx, dy) != (0, 0):
                k = 1 if dx else 2
                copies.append(send(src.at[sx, sy], rim.at[tx, ty], ss.at[k], rs.at[k], gx + dx, gy + dy, gz))
            for copy in copies:
                on(exists(dx, dy), copy.start)

        def finish(sems):
            def both(a, b):
                drain(side.at[0 : nx + a, 0 : ny + b], sems.at[0])
                drain(rim.at[0:a, 0 : ny + b], sems.at[1])
                drain(rim.at[0:nx, 0:b], sems.at[2])

            by_xy(both)

        late.append(lambda: finish(ss))
        return lambda: finish(rs)

    def shifted(block, fill):
        size = block.shape[-2]
        axis = block.ndim - 2
        rows = lax.broadcasted_iota(jnp.int32, block.shape, axis)
        below = jnp.where(rows == 0, 0.0, pltpu.roll(block, 1, axis))
        above = jnp.where(rows == size - 1, 0.0, pltpu.roll(block, size - 1, axis))
        if fill is not None:
            fill = jnp.broadcast_to(fill, block.shape)
            below = jnp.where(rows == jnp.where(gz == 1, 0, -1), fill, below)
            above = jnp.where(rows == jnp.where(gz == 0, size - 1, -1), fill, above)
        return below, above

    def rounded(x):
        return x.astype(BF16).astype(F32)

    arrived = neighbours(p1, 1, f1, p1, g1, nx, ny, s1, r1)

    k0 = 3 * c0
    for x in (0, nx + 1):
        e1[x] = jnp.zeros(e1.shape[1:], BF16)
    for y in (0, ny + 1):
        e1[1 : nx + 1, y] = jnp.zeros((nx, nz, k0), BF16)

    def widen(at, block):
        block = block.astype(F32)
        below, above = shifted(block, None)
        for k, part in enumerate((below, block, above)):
            e1[at + (slice(None), pl.ds(k * c0, c0))] = part.astype(BF16)

    @pl.loop(1, nx + 1)
    def _(x):
        widen((x, pl.ds(1, ny)), p1[x, 1 : ny + 1])

    loads[0].wait()
    for oy in range(3):
        for plane in range(4):
            at = pl.ds(plane * k0, k0)
            wt[oy, at, :c0] = wf[plane * 3 + oy] if plane < 3 else jnp.zeros((k0, c0), BF16)
            wt[oy, at, c0:] = wf[(plane - 1) * 3 + oy] if plane > 0 else jnp.zeros((k0, c0), BF16)
    for tap in range(9):
        wz[pl.ds(tap * c0, c0)] = wf[tap, pl.ds(pl.multiple_of(2 * oz * c0, c0), c0)]

    group1 = 2 if nx % 4 == 0 else 1

    @pl.loop(0, nx // (2 * group1))
    def _(step):
        total = jnp.zeros((group1 * ny * nz, 2 * c0), F32)
        for oy in range(3):
            for half in range(2):
                lhs = []
                for i in range(2):
                    planes = [2 * (step * group1 + n) + 2 * half + i for n in range(group1)]
                    planes = [e1[x, oy : oy + ny].reshape(ny * nz, k0) for x in planes]
                    lhs.append(jnp.concatenate(planes, axis=0))
                rhs = wt[oy, 2 * half * k0 : 2 * (half + 1) * k0]
                total = total + jnp.dot(jnp.concatenate(lhs, axis=1), rhs, preferred_element_type=F32)
        for n in range(group1):
            a1[step * group1 + n] = total[n * ny * nz : (n + 1) * ny * nz]

    arrived()
    for x in range(nx + 2):
        for y in range(ny + 2):
            gs[x, y : y + 1] = g1[x, y]
    @stage
    def _():
        lhs = [gs[ox : ox + nx, oy : oy + ny].reshape(nx * ny, c0).astype(BF16) for ox in range(3) for oy in range(3)]
        rz[...] = jnp.dot(jnp.concatenate(lhs, axis=1), wz[...], preferred_element_type=F32)
        for x, ox, lane in ((0, 0, 0), (nx + 1, 2, c0)):
            widen((x, pl.ds(1, ny)), p1[x, 1 : ny + 1])
            lhs = [e1[x, oy : oy + ny].reshape(ny * nz, k0) for oy in range(3)]
            rhs = wf[ox * 3 : ox * 3 + 3].reshape(3 * k0, c0)
            part = jnp.dot(jnp.concatenate(lhs, axis=1), rhs, preferred_element_type=F32)
            at = (0 if ox == 0 else nx // 2 - 1, slice(None), pl.ds(lane, c0))
            a1[at] = a1[at] + part
        for y, oy in ((0, 0), (ny + 1, 2)):
            widen((pl.ds(0, nx + 2), y), p1[:, y])
            lhs = [e1[ox : ox + nx, y].reshape(nx * nz, k0) for ox in range(3)]
            rhs = jnp.concatenate([wf[ox * 3 + oy] for ox in range(3)], axis=0)
            part = jnp.dot(jnp.concatenate(lhs, axis=1), rhs, preferred_element_type=F32).reshape(nx, nz, c0)
            for x in range(nx):
                at = (x // 2, pl.ds((0 if oy == 0 else ny - 1) * nz, nz), pl.ds(x % 2 * c0, c0))
                a1[at] = a1[at] + part[x]

    tile = 8
    last = lax.broadcasted_iota(jnp.int32, (tile, c0), 0) == (tile - 1) * oz
    for x in range(nx):
        for y in range(ny):
            at = (x // 2, pl.ds(pl.multiple_of(y * nz + (nz - tile) * oz, tile), tile), pl.ds(x % 2 * c0, c0))
            row = jnp.broadcast_to(rz[x * ny + y : x * ny + y + 1], (tile, c0))
            a1[at] = a1[at] + jnp.where(last, row, 0.0)

    hx, hy, hz = nx // 2, ny // 2, nz // 2

    @pl.loop(0, hx)
    def _(x):
        total = a1[x]
        both = jnp.maximum(jnp.maximum(total[:, :c0], total[:, c0:]), 0.0).reshape(hy, 2, nz, c0)
        t1[...] = jnp.max(both, axis=1)
        small = jnp.maximum(t1[:, pl.ds(0, hz, stride=2), :], t1[:, pl.ds(1, hz, stride=2), :])
        small = rounded(small)
        p2[x + 1, 1 : hy + 1] = small.astype(BF16)
        f2[x] = edge(small)

    arrived = neighbours(p2, 1, f2, p2, g2, hx, hy, s2, r2)
    arrived()
    rows = hx * hy * hz

    def pack(even, odd, at, block, lane):
        n, size, c = block.shape
        even[at, :, :, pl.ds(lane, c)] = block.reshape(n * size, c).astype(BF16).reshape(n // 2, 2 * size, c)
        block = block[1 : n - 1]
        odd[at, :, :, pl.ds(lane, c)] = block.reshape((n - 2) * size, c).astype(BF16).reshape(n // 2 - 1, 2 * size, c)

    def conv(even, odd, p, g, w):
        for x in range(hx + 2):
            block = p[x].astype(F32)
            c = block.shape[-1]
            below, above = shifted(block, g[x])
            for k, part in enumerate((below, block, above)):
                pack(even, odd, x, part, k * c)
        @stage
        def _():
            pairs = []
            for ox in range(3):
                for oy, (r, lo) in enumerate(((even, 0), (odd, 0), (even, 1))):
                    rhs = w[ox * 9 + oy * 3 : ox * 9 + oy * 3 + 3].reshape(3 * c, w.shape[2])
                    pairs.append((r[ox : ox + hx, lo : lo + hy // 2].reshape(rows, 3 * c), rhs))
            halves(pairs, (sums.at[0], sums.at[1]))

        return sums[0] + sums[1]

    loads[1].wait()
    c1 = wh.shape[2]
    total = conv(e2, o2, p2, g2, wh)
    skip = rounded(jnp.maximum(total, 0.0)).reshape(hx, hy, hz, c1)
    p3[1 : hx + 1, 1 : hy + 1] = skip.astype(BF16)

    cx, cy, cz = hx // 2, hy // 2, hz // 2
    ax = gxn * cx
    group = cz * cx
    m = jnp.max(skip.reshape(cx, 2, cy, 2, hz, c1), axis=(1, 3))
    m = m.reshape(cx * cy * hz, c1)
    m = jnp.maximum(m, pltpu.roll(m, m.shape[0] - 1, 0)).astype(BF16)

    blocks = []
    lane = lax.broadcasted_iota(jnp.int32, (group, cx * cy * hz), 1)
    sub = lax.broadcasted_iota(jnp.int32, (group, cx * cy * hz), 0)
    shift_x = cx.bit_length() - 1
    sub_x = sub & (cx - 1)
    sub_o = sub >> shift_x
    for y in range(cy):
        blocks.append(jnp.where(lane == (sub_x * cy + y) * hz + 2 * sub_o, 1.0, 0.0))
    blocks.append(jnp.where(lane == (sub_x * cy + sub_o) * hz + 2 * (cz - 1) * oz, 1.0, 0.0))
    pick = jnp.concatenate(blocks, axis=0).astype(BF16)
    packets = jnp.dot(pick, m, preferred_element_type=F32).reshape(cy + 1, group, c1).astype(BF16)
    pk2[...] = packets
    l2[gx, 0:cy] = packets[0:cy]

    def coarse_copy(k, dy, z):
        def make(src_gx, tgt_gx):
            if z == 0:
                src = {0: pl.ds(0, cy), -1: pl.ds(0, 1), 1: pl.ds(cy - 1, 1)}[dy]
            else:
                src = pl.ds(cy, 1)
            if dy == 0:
                dst = l2.at[src_gx, pl.ds(cy, 1) if z else pl.ds(0, cy)]
            else:
                dst = m2.at[src_gx, pl.ds(2 * z + (1 if dy < 0 else 0), 1)]
            return send(pk2.at[src], dst, s4.at[k], r4.at[k], tgt_gx, gy + dy, oz if z else gz)

        return make

    def deep_copy(pk, land, ss, rs):
        def choose(k, dy, z):
            def make(src_gx, tgt_gx):
                sy, ty = span(dy, cy, 0)
                sender = gz if src_gx is gx else (oz if z else gz)
                if z == 0:
                    src = pk.at[sy]
                    dst = land.at[src_gx, ty, pl.ds(1, cz)]
                else:
                    src = pk.at[sy, pl.ds((cz - 1) * (1 - sender), 1)]
                    dst = land.at[src_gx, ty, pl.ds((cz + 1) * sender, 1)]
                return send(src, dst, ss.at[k], rs.at[k], tgt_gx, gy + dy, oz if z else gz)

            return make

        return choose

    def narrow_copy(k, dy, z):
        def make(src_gx, tgt_gx):
            sy, ty = span(dy, cy, 0)
            sender = gz if src_gx is gx else (oz if z else gz)
            if z == 0:
                src = pk4.at[tgt_gx, sy]
                dst = l4.at[src_gx, ty, pl.ds(1, cz // 2)]
            else:
                src = pk4.at[tgt_gx, sy, pl.ds((cz // 2 - 1) * (1 - sender), 1)]
                dst = l4.at[src_gx, ty, pl.ds((cz // 2 + 1) * sender, 1)]
            return send(src, dst, s6.at[k], r6.at[k], tgt_gx, gy + dy, oz if z else gz)

        return make

    def column_exchange(choose, main, rim):
        order = [(there, 0, z, 0) for there in farthest for z in (0, 1)]
        order += [(gx, 0, 1, 1)]
        order += [(there, dy, z, 2) for there in farthest + [gx] for z in (0, 1) for dy in (-1, 1)]
        for there, dy, z, k in order:
            on(exists(0, dy), choose(k, dy, z)(gx, there).start)

        def first(which):
            for k, ref in enumerate(main):
                drain(ref, which.at[k])

        def second(which):
            by_y(lambda b: drain(rim(b), which.at[2]))

        return first, second

    def leave(waits, sems):
        late.append(lambda: [wait(sems) for wait in waits])
        return waits

    def parts_of(land):
        wz = land.shape[2] - 2
        main = (land.at[0 : gxn - 1, 0:cy, 0 : wz + 1], land.at[0, 0:cy, 0:1])
        return main, lambda b: land.at[0:gxn, 0:b, 0 : wz + 1]

    main4, rim4 = leave(
        column_exchange(coarse_copy, (l2.at[0 : gxn - 1], l2.at[0, 0:1]), lambda b: m2.at[0:gxn, 0 : 2 * b]), s4
    )
    for x in range(hx):
        f3[x] = edge(p3[x + 1, 1 : hy + 1].astype(F32))

    def one_hot(ref, at, slots):
        width = gxn * slots * group
        lane = lax.broadcasted_iota(jnp.int32, (ax, width), 1)
        xs = lax.broadcasted_iota(jnp.int32, (ax, width), 0)
        base = lane - ((xs >> shift_x) * slots * group + (xs & (cx - 1)))
        ref[at] = jnp.where(base == slots_at, 1.0, 0.0)

    for y in range(-1, cy + 1):
        for z in range(-1, cz + 1):
            inside = 0 <= y < cy
            rim_slot = 0 if y < 0 else 1
            if 0 <= z < cz:
                slots_at = (y if inside else rim_slot) * group + z * cx
            else:
                line = y if inside else (cy - 1 if y < 0 else 0)
                mine = (gz == 1) if z < 0 else (gz == 0)
                slots_at = jnp.where(mine, (cy if inside else 2 + rim_slot) * group + line * cx, -(1 << 20))
            if inside:
                one_hot(sel2, (y, z + 1), cy + 1)
            else:
                one_hot(selm, (rim_slot, z + 1), 4)

    def gathered(ref, land):
        n, width = ref.shape[0], ref.shape[-1]
        select = ref[...].reshape(n * (cz + 2) * ax, width).astype(BF16)
        landed = land[...].astype(F32).reshape(width, c1).astype(BF16)
        return jnp.dot(select, landed, preferred_element_type=F32).reshape(n, cz + 2, ax, c1)

    deep = cy * cz * ax
    fo = w1.shape[2]

    windows = ((0, 0), (1, 0), (0, 1))

    def spread(even, odd, block, row):
        below, above = shifted(block, None)
        n, c = block.shape[0], block.shape[-1]
        for ox, part in enumerate((below, block, above)):
            whole = part.reshape(n * (cz + 2) * ax, c).astype(BF16)
            even[ox, row : row + n] = whole.reshape(n, cz // 2 + 1, 2 * ax, c)
            inner = part[:, 1 : cz + 1].reshape(n * cz * ax, c).astype(BF16)
            odd[ox, row : row + n] = inner.reshape(n, cz // 2, 2 * ax, c)

    def window(pair, ox, row, n):
        c = pair[0].shape[-1]
        lhs = [pair[i][ox, row : row + n, lo : lo + cz // 2].reshape(n * cz * ax, c) for i, lo in windows]
        return jnp.concatenate(lhs, axis=1)

    def bottom_own(pair, w):
        @stage
        def _():
            k = 3 * w.shape[1]
            pairs = []
            for ox in range(3):
                lhs = window(pair, ox, 1, cy)
                rhs = [w[ox * 9 + oy * 3 : ox * 9 + oy * 3 + 3].reshape(k, fo) for oy in range(3)]
                rhs = jnp.concatenate(rhs, axis=1)
                pairs += [(lhs[:, : k // 2], rhs[: k // 2]), (lhs[:, k // 2 :], rhs[k // 2 :])]
            halves(pairs, (deeps.at[0], deeps.at[1]))

    def bottom_rim(pair, w):
        k = 3 * w.shape[1]
        size = cz * ax
        @stage
        def _():
            for side, (row, oy) in enumerate(((0, 0), (cy + 1, 2))):
                total = jnp.zeros((size, fo), F32)
                for ox in range(3):
                    rhs = w[(ox * 3 + oy) * 3 : (ox * 3 + oy) * 3 + 3].reshape(k, fo)
                    total = total + jnp.dot(window(pair, ox, row, 1), rhs, preferred_element_type=F32)
                brims[side] = total

        def own(oy, y):
            at = (pl.ds(y * size, size), pl.ds(oy * fo, fo))
            return deeps[(0, *at)] + deeps[(1, *at)]

        lines = []
        for y in range(cy):
            before = own(0, y - 1) if y > 0 else brims[0]
            after = own(2, y + 1) if y < cy - 1 else brims[1]
            lines.append(own(1, y) + before + after)
        return jnp.maximum(jnp.concatenate(lines, axis=0), 0.0).reshape(cy, cz, ax, fo).astype(BF16)

    main4(r4)
    spread(q2, b2, gathered(sel2, l2), 1)
    loads[2].wait()
    bottom_own((q2, b2), w1)
    rim4(r4)
    block = gathered(selm, m2)
    spread(q2, b2, block[0:1], 0)
    spread(q2, b2, block[1:2], cy + 1)
    first = bottom_rim((q2, b2), w1)
    pk3[...] = first
    l3[gx, 1 : cy + 1, 1 : cz + 1] = first
    main5, rim5 = leave(column_exchange(deep_copy(pk3, l3, s5, r5), *parts_of(l3)), s5)

    skip_arrived = neighbours(p3, 1, f3, p3, g3, hx, hy, s3, r3)
    near = cx + 2
    wide = gxn * cz * near
    lane = lax.broadcasted_iota(jnp.int32, (wide, cz * ax), 1)
    row = lax.broadcasted_iota(jnp.int32, (wide, cz * ax), 0)
    shift_n = near.bit_length() - 1
    shift_z = cz.bit_length() - 1
    at = (row >> (shift_n + shift_z)) * cx + (row & (near - 1)) - 1
    at = jnp.where(jnp.logical_and(at >= 0, at < ax), at, -(cz + 1) * ax)
    share = jnp.where(lane == ((row >> shift_n) & (cz - 1)) * ax + at, 1.0, 0.0).astype(BF16)

    lane = lax.broadcasted_iota(jnp.int32, (hz, (cz + 4) * near), 1)
    zs = lax.broadcasted_iota(jnp.int32, (hz, (cz + 4) * near), 0)
    blocks = []
    for k in range(3):
        for x in range(-1, hx + 1):
            blocks.append(jnp.where(lane == (((zs + (k - 1)) >> 1) + 2) * near + (x >> 1) + 1, 1.0, 0.0))
    for k in range(3):
        blocks += blocks[k * (hx + 2) + 1 : (k + 1) * (hx + 2) - 1]
    pick = jnp.concatenate(blocks, axis=0).astype(BF16)

    def joined(row, n):
        return jnp.concatenate([l3[g, row : row + n].astype(F32) for g in range(gxn)], axis=-1)

    main5(r5)
    spread(q3, b3, joined(1, cy), 1)
    loads[3].wait()
    bottom_own((q3, b3), w2)
    rim5(r5)
    spread(q3, b3, joined(0, 1), 0)
    spread(q3, b3, joined(cy + 1, 1), cy + 1)
    second = bottom_rim((q3, b3), w2)
    for y in range(cy):
        line = second[y].astype(F32).reshape(cz * ax, fo).astype(BF16)
        line = jnp.dot(share, line, preferred_element_type=F32)
        pk4[:, y] = line.reshape(gxn, cz // 2, 2 * near, fo).astype(BF16)
    l4[gx, 1 : cy + 1, 1 : cz // 2 + 1] = pk4[gx]
    main6, rim6 = leave(column_exchange(narrow_copy, *parts_of(l4)), s6)
    size = hx * hz

    def enlarge(ys):
        fields = [l4[g, y].astype(F32).reshape((cz + 4) * near, fo) for y in ys for g in range(gxn)]
        fields = jnp.concatenate(fields, axis=-1).astype(BF16)
        fields = jnp.dot(pick, fields, preferred_element_type=F32).astype(BF16)
        for i, y in enumerate(ys):
            field = fields[:, i * c2 : (i + 1) * c2]
            for k in range(3):
                at = pl.ds(k * c2, c2)
                part = field[k * (size + 2 * hz) : (k + 1) * (size + 2 * hz)]
                up[0, y, :, :, at] = part[:size].reshape(hx // 2, 2 * hz, c2)
                up[2, y, :, :, at] = part[2 * hz :].reshape(hx // 2, 2 * hz, c2)
                part = field[3 * (size + 2 * hz) + k * size : 3 * (size + 2 * hz) + (k + 1) * size]
                up[1, y, :, :, at] = part.reshape(hx // 2, 2 * hz, c2)

    skip_arrived()
    loads[4].wait()
    total = conv(e3, o3, p3, g3, wus)
    acc[...] = total.reshape(hx, hy, hz, c1)

    main6(r6)
    enlarge(range(1, cy + 1))
    loads[5].wait()

    @stage
    def _():
        pairs = []
        for ox in range(3):
            for k in range(3):
                lhs = up[ox, 1 : cy + 1, :, :, pl.ds(k * c2, c2)].reshape(cy * size, c2)
                pairs.append((lhs, wuu[ox * 9 + 3 + k]))
        halves(pairs, (thirds.at[0], thirds.at[1]))

    rim6(r6)
    enlarge((0, cy + 1))

    @stage
    def _():
        for side, oy in enumerate((0, 2)):
            total = jnp.zeros(((cy + 1) * size, c1), F32)
            for ox in range(3):
                lhs = up[ox, side : side + cy + 1].reshape((cy + 1) * size, 3 * c2)
                rhs = wuu[(ox * 3 + oy) * 3 : (ox * 3 + oy) * 3 + 3].reshape(3 * c2, c1)
                total = total + jnp.dot(lhs, rhs, preferred_element_type=F32)
            ends[side] = total

    for y in range(hy):
        low, mid, high = (y + 1) // 2, (y + 2) // 2 - 1, (y + 3) // 2 - 1
        total = ends[0, low * size : (low + 1) * size] + ends[1, high * size : (high + 1) * size]
        total = total + thirds[0, mid * size : (mid + 1) * size] + thirds[1, mid * size : (mid + 1) * size]
        out[:, y] = (acc[:, y] + total.reshape(hx, hz, c1)).astype(BF16)

    for fn in late:
        fn()


def on_device(dims, volume, w_full, w_half, w_bottom_in, w_bottom_out, w_up):
    gxn, gyn = dims
    nx, ny, nz, c0 = volume.shape
    c1 = w_half.shape[4]
    c2, fo = w_bottom_out.shape[3:]
    hx, hy, hz = nx // 2, ny // 2, nz // 2
    cx, cy, cz = hx // 2, hy // 2, hz // 2
    ax = gxn * cx
    weights = [
        w_full.reshape(9, 3 * c0, c0),
        w_half.reshape(27, c0, c1),
        w_bottom_in.reshape(27, c1, fo),
        w_bottom_out.reshape(27, c2, fo),
        w_up.reshape(27, c2 + c1, c1),
    ]
    vm = pltpu.VMEM
    dma = pltpu.SemaphoreType.DMA
    scratch = [vm(w.shape, BF16) for w in weights[:4]]
    scratch += [vm((27, c1, c1), BF16), vm((27, c2, c1), BF16), dma((6,)), dma(())]
    scratch += [vm((3, 12 * c0, 2 * c0), BF16), vm((9 * c0, c0), BF16)]
    scratch += [
        vm((nx + 2, ny + 2, nz, c0), BF16), vm((nx, ny, 1, c0), F32), vm((nx + 2, ny + 2, 1, c0), F32),
        vm((nx + 2, ny + 2, c0), F32), vm((nx + 2, ny + 2, nz, 3 * c0), BF16), vm((hx, ny * nz, 2 * c0), F32),
        vm((nx * ny, c0), F32), vm((hy, nz, c0), F32),
        vm((hx + 2, hy + 2, hz, c0), BF16), vm((hx, hy, 1, c0), F32), vm((hx + 2, hy + 2, 1, c0), F32),
        vm((hx + 2, hy // 2 + 1, 2 * hz, 3 * c0), BF16), vm((hx + 2, hy // 2, 2 * hz, 3 * c0), BF16),
        vm((hx + 2, hy + 2, hz, c1), BF16), vm((hx, hy, 1, c1), F32), vm((hx + 2, hy + 2, 1, c1), F32),
        vm((hx + 2, hy // 2 + 1, 2 * hz, 3 * c1), BF16), vm((hx + 2, hy // 2, 2 * hz, 3 * c1), BF16),
        vm((hx, hy, hz, c1), F32),
        vm((cy + 1, cz * cx, c1), BF16), vm((gxn, cy + 1, cz * cx, c1), BF16), vm((gxn, 4, cz * cx, c1), BF16),
        vm((cy, cz + 2, ax, gxn * (cy + 1) * cz * cx), F32), vm((2, cz + 2, ax, gxn * 4 * cz * cx), F32),
        vm((3, cy + 2, cz // 2 + 1, 2 * ax, c1), BF16), vm((3, cy + 2, cz // 2, 2 * ax, c1), BF16),
        vm((cy, cz, ax, fo), BF16), vm((gxn, cy + 2, cz + 2, ax, fo), BF16),
        vm((3, cy + 2, cz // 2 + 1, 2 * ax, c2), BF16), vm((3, cy + 2, cz // 2, 2 * ax, c2), BF16),
        vm((gxn, cy, cz // 2, 2 * (cx + 2), fo), BF16), vm((gxn, cy + 2, cz // 2 + 2, 2 * (cx + 2), fo), BF16),
        vm((3, cy + 2, hx // 2, 2 * hz, 3 * c2), BF16),
        vm((2, hx * hy * hz, c1), F32), vm((2, cy * cz * ax, 3 * fo), F32), vm((2, cz * ax, fo), F32),
        vm((2, cy * hx * hz, c1), F32), vm((2, (cy + 1) * hx * hz, c1), F32),
    ]
    scratch += [dma((3,))] * 12
    return pl.pallas_call(
        functools.partial(kernel, dims),
        out_shape=jax.ShapeDtypeStruct((hx, hy, hz, c1), BF16),
        in_specs=[pl.BlockSpec(memory_space=pltpu.HBM)] * 6,
        out_specs=pl.BlockSpec(memory_space=pltpu.VMEM),
        scratch_shapes=scratch,
        compiler_params=pltpu.CompilerParams(
            collective_id=0, has_side_effects=True, vmem_limit_bytes=52 * 1024 * 1024
        ),
    )(*[pltpu.with_memory_space_constraint(a, pltpu.HBM) for a in (volume, *weights)])


def solution(mesh):
    dims = (mesh.shape["gx"], mesh.shape["gy"])
    assert mesh.shape["gz"] == 2
    return jax.shard_map(
        functools.partial(on_device, dims),
        mesh=mesh,
        in_specs=(
            P("gx", "gy", "gz", None),
            P(),
            P(),
            P(None, None, None, None, "gx"),
            P(None, None, None, None, "gx"),
            P(),
        ),
        out_specs=P("gx", "gy", "gz", None),
        check_vma=False,
    )
```

```python
import functools

import jax
import jax.numpy as jnp
from jax import lax
from jax.experimental import pallas as pl
from jax.experimental.pallas import tpu as pltpu
from jax.sharding import PartitionSpec as P

F32 = jnp.float32
BF16 = jnp.bfloat16
STEPS = [(dx, dy) for dx in (-1, 0, 1) for dy in (-1, 0, 1)]


def span(d, n, pad):
    if d == 0:
        return pl.ds(pad, n), pl.ds(1, n)
    if d < 0:
        return pl.ds(pad, 1), pl.ds(n + 1, 1)
    return pl.ds(pad + n - 1, 1), pl.ds(0, 1)


def halves(pairs, refs):
    for i, ref in enumerate(refs):
        total = None
        for lhs, rhs in pairs[i::2]:
            part = jnp.dot(lhs, rhs, preferred_element_type=F32)
            total = part if total is None else total + part
        ref[...] = total


def kernel(
    dims,
    v_h, wf_h, wh_h, w1_h, w2_h, wu_h,
    out,
    wh, w1, w2, wus, wuu, wsem, vsem, fsem, wt, wz,
    p1, f1, g1, gs, e1, a1, rz, t1,
    p2, f2, g2, e2, o2,
    p3, f3, g3, e3, o3, acc,
    pk2, l2, m2, sel2, selm, q2, b2, pk3, l3, q3, b3, pk4, l4, up, sums, deeps, brims, thirds, ends,
    s1, r1, s2, r2, s3, r3, s4, r4, s5, r5, s6, r6,
):
    gxn, gyn = dims
    gx, gy, gz = lax.axis_index("gx"), lax.axis_index("gy"), lax.axis_index("gz")
    oz = 1 - gz

    nx, ny, nz, c0 = v_h.shape
    fetch = pltpu.make_async_copy(v_h, p1.at[1 : nx + 1, 1 : ny + 1], vsem)
    fetch.start()
    c2 = w2.shape[1]
    loads = [
        pltpu.make_async_copy(src, dst, wsem.at[i])
        for i, (src, dst) in enumerate((
            (wh_h, wh), (w1_h, w1), (w2_h, w2), (wu_h.at[:, c2:], wus), (wu_h.at[:, :c2], wuu),
        ))
    ]

    def on(cond, fn):
        if cond is True:
            fn()
        else:
            pl.when(cond)(fn)

    def exists(dx, dy):
        conds = []
        if dx < 0:
            conds.append(gx > 0)
        if dx > 0:
            conds.append(gx < gxn - 1)
        if dy < 0:
            conds.append(gy > 0)
        if dy > 0:
            conds.append(gy < gyn - 1)
        if not conds:
            return True
        return functools.reduce(jnp.logical_and, conds)

    for x in (0, nx + 1):
        p1[x] = jnp.zeros(p1.shape[1:], BF16)
    for y in (0, ny + 1):
        p1[1 : nx + 1, y] = jnp.zeros((nx, nz, c0), BF16)
    m2[...] = jnp.zeros_like(m2)
    for x in (0, nx + 1):
        g1[x] = jnp.zeros(g1.shape[1:], F32)
    for y in (0, ny + 1):
        g1[:, y] = jnp.zeros((nx + 2, 1, c0), F32)

    barrier = pltpu.get_barrier_semaphore()
    for s in range(gxn):
        there = lax.rem(gx + s, gxn)
        for dy in (-1, 0, 1):
            for z in (0, 1):
                if s == 0 and dy == 0 and z == 0:
                    continue

                def signal(there=there, dy=dy, z=z):
                    pl.semaphore_signal(
                        barrier, inc=1,
                        device_id={"gx": there, "gy": gy + dy, "gz": oz if z else gz},
                        device_id_type=pl.DeviceIdType.MESH,
                    )

                on(exists(0, dy), signal)
    k0 = 3 * c0
    for oy in range(3):
        for first, lane in ((0, 0), (1, c0)):
            dst = wt.at[oy, first : first + 3, :, lane : lane + c0]
            pltpu.make_async_copy(wf_h.at[:, oy], dst, fsem).start()
    lines = 1 + (gy > 0).astype(jnp.int32) + (gy < gyn - 1).astype(jnp.int32)

    def edge(block):
        size = block.shape[-2]
        rows = lax.broadcasted_iota(jnp.int32, block.shape, block.ndim - 2)
        return jnp.sum(jnp.where(rows == (size - 1) * oz, block, 0.0), axis=block.ndim - 2, keepdims=True)

    for ref in (g2, g3):
        ref[...] = jnp.zeros(ref.shape, ref.dtype)
    for ref in (p2, p3):
        for x in (0, ref.shape[0] - 1):
            ref[x] = jnp.zeros(ref.shape[1:], BF16)
        for y in (0, ref.shape[1] - 1):
            ref[:, y] = jnp.zeros(ref.shape[:1] + ref.shape[2:], BF16)
    for x in (0, nx + 1):
        e1[x] = jnp.zeros(e1.shape[1:], BF16)
    for y in (0, ny + 1):
        e1[1 : nx + 1, y] = jnp.zeros((nx, nz, k0), BF16)
    for oy in range(3):
        wt[oy, 3, :, :c0] = jnp.zeros((k0, c0), BF16)
        wt[oy, 0, :, c0:] = jnp.zeros((k0, c0), BF16)
    fetch.wait()
    for load in loads:
        load.start()
    for x in range(nx):
        f1[x] = edge(p1[x + 1, 1 : ny + 1].astype(F32))
    pl.semaphore_wait(barrier, 2 * gxn * lines - 1)

    def send(src, dst, ss, rs, x, y, z):
        return pltpu.make_async_remote_copy(
            src_ref=src, dst_ref=dst, send_sem=ss, recv_sem=rs,
            device_id={"gx": x, "gy": y, "gz": z}, device_id_type=pl.DeviceIdType.MESH,
        )

    many_x = jnp.logical_and(gx > 0, gx < gxn - 1)
    many_y = jnp.logical_and(gy > 0, gy < gyn - 1)

    def by_y(fn):
        for b in (1, 2):
            pl.when(many_y if b == 2 else jnp.logical_not(many_y))(functools.partial(fn, b))

    def by_xy(fn):
        for a in (1, 2):
            for b in (1, 2):
                cx_ = many_x if a == 2 else jnp.logical_not(many_x)
                cy_ = many_y if b == 2 else jnp.logical_not(many_y)
                pl.when(jnp.logical_and(cx_, cy_))(functools.partial(fn, a, b))

    def drain(ref, sem):
        pltpu.make_async_copy(ref, ref, sem).wait()

    stage = pl.when(gx < gxn)
    short = jnp.minimum(gx, gxn - 1 - gx)
    farthest = []
    for i in range(gxn - 1, 0, -1):
        paired = gx + ((i + 1) // 2 if i % 2 else -(i // 2))
        rest = jnp.where(gx < gxn - 1 - gx, gx + (i - short), gx - (i - short))
        farthest.append(jnp.where(i <= 2 * short, paired, rest))

    late = []

    def neighbours(src, pad, face, rim, side, nx, ny, ss, rs):
        copies = []
        for dx, dy in STEPS:
            sx, tx = span(dx, nx, pad)
            sy, ty = span(dy, ny, pad)
            fx, _ = span(dx, nx, 0)
            fy, _ = span(dy, ny, 0)
            hops = abs(dx) + abs(dy)
            to = (gx + dx, gy + dy)
            copies.append((hops + 1, exists(dx, dy), send(face.at[fx, fy], side.at[tx, ty], ss.at[0], rs.at[0], *to, oz)))
            if hops:
                k = 1 if dx else 2
                copy = send(src.at[sx, sy], rim.at[tx, ty], ss.at[k], rs.at[k], *to, gz)
                copies.append((hops, exists(dx, dy), copy))
        for _, cond, copy in sorted(copies, key=lambda entry: -entry[0]):
            on(cond, copy.start)

        def finish(sems):
            def both(a, b):
                drain(side.at[0 : nx + a, 0 : ny + b], sems.at[0])
                drain(rim.at[0:a, 0 : ny + b], sems.at[1])
                drain(rim.at[0:nx, 0:b], sems.at[2])

            by_xy(both)

        late.append(lambda: finish(ss))
        return lambda: finish(rs)

    def shifted(block, fill):
        size = block.shape[-2]
        axis = block.ndim - 2
        rows = lax.broadcasted_iota(jnp.int32, block.shape, axis)
        below = jnp.where(rows == 0, 0.0, pltpu.roll(block, 1, axis))
        above = jnp.where(rows == size - 1, 0.0, pltpu.roll(block, size - 1, axis))
        if fill is not None:
            fill = jnp.broadcast_to(fill, block.shape)
            below = jnp.where(rows == jnp.where(gz == 1, 0, -1), fill, below)
            above = jnp.where(rows == jnp.where(gz == 0, size - 1, -1), fill, above)
        return below, above

    def rounded(x):
        return x.astype(BF16).astype(F32)

    arrived = neighbours(p1, 1, f1, p1, g1, nx, ny, s1, r1)

    def widen(at, block):
        block = block.astype(F32)
        below, above = shifted(block, None)
        for k, part in enumerate((below, block, above)):
            e1[at + (slice(None), pl.ds(k * c0, c0))] = part.astype(BF16)

    @pl.loop(1, nx + 1)
    def _(x):
        widen((x, pl.ds(1, ny)), p1[x, 1 : ny + 1])

    drain(wt.at[:, 0:3], fsem)

    group1 = 2 if nx % 4 == 0 else 1

    @pl.loop(0, nx // (2 * group1))
    def _(step):
        total = jnp.zeros((group1 * ny * nz, 2 * c0), F32)
        for oy in range(3):
            for half in range(2):
                lhs = []
                for i in range(2):
                    planes = [2 * (step * group1 + n) + 2 * half + i for n in range(group1)]
                    planes = [e1[x, oy : oy + ny].reshape(ny * nz, k0) for x in planes]
                    lhs.append(jnp.concatenate(planes, axis=0))
                rhs = wt[oy, 2 * half : 2 * half + 2].reshape(2 * k0, 2 * c0)
                total = total + jnp.dot(jnp.concatenate(lhs, axis=1), rhs, preferred_element_type=F32)
        for n in range(group1):
            a1[step * group1 + n] = total[n * ny * nz : (n + 1) * ny * nz]

    for ox in range(3):
        for oy in range(3):
            tap = wt[oy, ox, pl.ds(pl.multiple_of(2 * oz * c0, c0), c0), :c0]
            wz[(ox * 3 + oy) * c0 : (ox * 3 + oy + 1) * c0] = tap
    arrived()
    for x in range(nx + 2):
        for y in range(ny + 2):
            gs[x, y : y + 1] = g1[x, y]
    @stage
    def _():
        lhs = [gs[ox : ox + nx, oy : oy + ny].reshape(nx * ny, c0).astype(BF16) for ox in range(3) for oy in range(3)]
        rz[...] = jnp.dot(jnp.concatenate(lhs, axis=1), wz[...], preferred_element_type=F32)
        for x, ox, lane in ((0, 0, 0), (nx + 1, 2, c0)):
            widen((x, pl.ds(1, ny)), p1[x, 1 : ny + 1])
            lhs = [e1[x, oy : oy + ny].reshape(ny * nz, k0) for oy in range(3)]
            rhs = jnp.concatenate([wt[oy, ox, :, :c0] for oy in range(3)], axis=0)
            part = jnp.dot(jnp.concatenate(lhs, axis=1), rhs, preferred_element_type=F32)
            at = (0 if ox == 0 else nx // 2 - 1, slice(None), pl.ds(lane, c0))
            a1[at] = a1[at] + part
        for y, oy in ((0, 0), (ny + 1, 2)):
            widen((pl.ds(0, nx + 2), y), p1[:, y])
            lhs = [e1[ox : ox + nx, y].reshape(nx * nz, k0) for ox in range(3)]
            rhs = jnp.concatenate([wt[oy, ox, :, :c0] for ox in range(3)], axis=0)
            part = jnp.dot(jnp.concatenate(lhs, axis=1), rhs, preferred_element_type=F32).reshape(nx, nz, c0)
            for x in range(nx):
                at = (x // 2, pl.ds((0 if oy == 0 else ny - 1) * nz, nz), pl.ds(x % 2 * c0, c0))
                a1[at] = a1[at] + part[x]

    tile = 8
    last = lax.broadcasted_iota(jnp.int32, (tile, c0), 0) == (tile - 1) * oz
    for x in range(nx):
        for y in range(ny):
            at = (x // 2, pl.ds(pl.multiple_of(y * nz + (nz - tile) * oz, tile), tile), pl.ds(x % 2 * c0, c0))
            row = jnp.broadcast_to(rz[x * ny + y : x * ny + y + 1], (tile, c0))
            a1[at] = a1[at] + jnp.where(last, row, 0.0)

    hx, hy, hz = nx // 2, ny // 2, nz // 2

    @pl.loop(0, hx)
    def _(x):
        total = a1[x]
        both = jnp.maximum(jnp.maximum(total[:, :c0], total[:, c0:]), 0.0).reshape(hy, 2, nz, c0)
        t1[...] = jnp.max(both, axis=1)
        small = jnp.maximum(t1[:, pl.ds(0, hz, stride=2), :], t1[:, pl.ds(1, hz, stride=2), :])
        small = rounded(small)
        p2[x + 1, 1 : hy + 1] = small.astype(BF16)
        f2[x] = edge(small)

    arrived = neighbours(p2, 1, f2, p2, g2, hx, hy, s2, r2)
    for ref in (l3, l4):
        ref[...] = jnp.zeros(ref.shape, ref.dtype)
    arrived()
    rows = hx * hy * hz

    def pack(even, odd, at, block, lane):
        n, size, c = block.shape
        even[at, :, :, pl.ds(lane, c)] = block.reshape(n * size, c).astype(BF16).reshape(n // 2, 2 * size, c)
        block = block[1 : n - 1]
        odd[at, :, :, pl.ds(lane, c)] = block.reshape((n - 2) * size, c).astype(BF16).reshape(n // 2 - 1, 2 * size, c)

    def conv(even, odd, p, g, w):
        for x in range(hx + 2):
            block = p[x].astype(F32)
            c = block.shape[-1]
            below, above = shifted(block, g[x])
            for k, part in enumerate((below, block, above)):
                pack(even, odd, x, part, k * c)
        @stage
        def _():
            pairs = []
            for ox in range(3):
                for oy, (r, lo) in enumerate(((even, 0), (odd, 0), (even, 1))):
                    rhs = w[ox * 9 + oy * 3 : ox * 9 + oy * 3 + 3].reshape(3 * c, w.shape[2])
                    pairs.append((r[ox : ox + hx, lo : lo + hy // 2].reshape(rows, 3 * c), rhs))
            halves(pairs, (sums.at[0], sums.at[1]))

        return sums[0] + sums[1]

    loads[0].wait()
    c1 = wh.shape[2]
    total = conv(e2, o2, p2, g2, wh)
    skip = rounded(jnp.maximum(total, 0.0)).reshape(hx, hy, hz, c1)
    p3[1 : hx + 1, 1 : hy + 1] = skip.astype(BF16)

    cx, cy, cz = hx // 2, hy // 2, hz // 2
    ax = gxn * cx
    group = cz * cx
    m = jnp.max(skip.reshape(cx, 2, cy, 2, hz, c1), axis=(1, 3))
    m = m.reshape(cx * cy * hz, c1)
    m = jnp.maximum(m, pltpu.roll(m, m.shape[0] - 1, 0)).astype(BF16)

    blocks = []
    lane = lax.broadcasted_iota(jnp.int32, (group, cx * cy * hz), 1)
    sub = lax.broadcasted_iota(jnp.int32, (group, cx * cy * hz), 0)
    shift_x = cx.bit_length() - 1
    sub_x = sub & (cx - 1)
    sub_o = sub >> shift_x
    for y in range(cy):
        blocks.append(jnp.where(lane == (sub_x * cy + y) * hz + 2 * sub_o, 1.0, 0.0))
    blocks.append(jnp.where(lane == (sub_x * cy + sub_o) * hz + 2 * (cz - 1) * oz, 1.0, 0.0))
    pick = jnp.concatenate(blocks, axis=0).astype(BF16)
    packets = jnp.dot(pick, m, preferred_element_type=F32).reshape(cy + 1, group, c1).astype(BF16)
    pk2[...] = packets
    l2[gx, 0:cy] = packets[0:cy]

    def coarse_copy(k, dy, z):
        def make(src_gx, tgt_gx):
            if z == 0:
                src = {0: pl.ds(0, cy), -1: pl.ds(0, 1), 1: pl.ds(cy - 1, 1)}[dy]
            else:
                src = pl.ds(cy, 1)
            if dy == 0:
                dst = l2.at[src_gx, pl.ds(cy, 1) if z else pl.ds(0, cy)]
            else:
                dst = m2.at[src_gx, pl.ds(2 * z + (1 if dy < 0 else 0), 1)]
            return send(pk2.at[src], dst, s4.at[k], r4.at[k], tgt_gx, gy + dy, oz if z else gz)

        return make

    def deep_copy(pk, land, ss, rs):
        def choose(k, dy, z):
            def make(src_gx, tgt_gx):
                sy, ty = span(dy, cy, 0)
                sender = gz if src_gx is gx else (oz if z else gz)
                if z == 0:
                    src = pk.at[sy]
                    dst = land.at[src_gx, ty, pl.ds(1, cz)]
                else:
                    src = pk.at[sy, pl.ds((cz - 1) * (1 - sender), 1)]
                    dst = land.at[src_gx, ty, pl.ds((cz + 1) * sender, 1)]
                return send(src, dst, ss.at[k], rs.at[k], tgt_gx, gy + dy, oz if z else gz)

            return make

        return choose

    def narrow_copy(k, dy, z):
        def make(src_gx, tgt_gx):
            sy, ty = span(dy, cy, 0)
            sender = gz if src_gx is gx else (oz if z else gz)
            if z == 0:
                src = pk4.at[tgt_gx, sy]
                dst = l4.at[src_gx, ty, pl.ds(1, cz // 2)]
            else:
                src = pk4.at[tgt_gx, sy, pl.ds((cz // 2 - 1) * (1 - sender), 1)]
                dst = l4.at[src_gx, ty, pl.ds((cz // 2 + 1) * sender, 1)]
            return send(src, dst, s6.at[k], r6.at[k], tgt_gx, gy + dy, oz if z else gz)

        return make

    def column_exchange(choose, main, rim):
        order = [(there, 0, z, 0) for there in farthest for z in (1, 0)]
        order += [(gx, 0, 1, 1)]
        order += [(there, dy, z, 2) for there in farthest + [gx] for z in (1, 0) for dy in (-1, 1)]
        for there, dy, z, k in order:
            on(exists(0, dy), choose(k, dy, z)(gx, there).start)

        def first(which):
            for k, ref in enumerate(main):
                drain(ref, which.at[k])

        def second(which):
            by_y(lambda b: drain(rim(b), which.at[2]))

        return first, second

    def leave(waits, sems):
        late.append(lambda: [wait(sems) for wait in waits])
        return waits

    def parts_of(land):
        wz = land.shape[2] - 2
        main = (land.at[0 : gxn - 1, 0:cy, 0 : wz + 1], land.at[0, 0:cy, 0:1])
        return main, lambda b: land.at[0:gxn, 0:b, 0 : wz + 1]

    main4, rim4 = leave(
        column_exchange(coarse_copy, (l2.at[0 : gxn - 1], l2.at[0, 0:1]), lambda b: m2.at[0:gxn, 0 : 2 * b]), s4
    )
    for x in range(hx):
        f3[x] = edge(p3[x + 1, 1 : hy + 1].astype(F32))

    def one_hot(ref, at, slots):
        width = gxn * slots * group
        lane = lax.broadcasted_iota(jnp.int32, (ax, width), 1)
        xs = lax.broadcasted_iota(jnp.int32, (ax, width), 0)
        base = lane - ((xs >> shift_x) * slots * group + (xs & (cx - 1)))
        ref[at] = jnp.where(base == slots_at, 1.0, 0.0)

    for y in range(-1, cy + 1):
        for z in range(-1, cz + 1):
            inside = 0 <= y < cy
            rim_slot = 0 if y < 0 else 1
            if 0 <= z < cz:
                slots_at = (y if inside else rim_slot) * group + z * cx
            else:
                line = y if inside else (cy - 1 if y < 0 else 0)
                mine = (gz == 1) if z < 0 else (gz == 0)
                slots_at = jnp.where(mine, (cy if inside else 2 + rim_slot) * group + line * cx, -(1 << 20))
            if inside:
                one_hot(sel2, (y, z + 1), cy + 1)
            else:
                one_hot(selm, (rim_slot, z + 1), 4)

    def gathered(ref, land):
        n, width = ref.shape[0], ref.shape[-1]
        select = ref[...].reshape(n * (cz + 2) * ax, width).astype(BF16)
        landed = land[...].astype(F32).reshape(width, c1).astype(BF16)
        return jnp.dot(select, landed, preferred_element_type=F32).reshape(n, cz + 2, ax, c1)

    deep = cy * cz * ax
    fo = w1.shape[2]

    windows = ((0, 0), (1, 0), (0, 1))

    def spread(even, odd, block, row):
        below, above = shifted(block, None)
        n, c = block.shape[0], block.shape[-1]
        for ox, part in enumerate((below, block, above)):
            whole = part.reshape(n * (cz + 2) * ax, c).astype(BF16)
            even[ox, row : row + n] = whole.reshape(n, cz // 2 + 1, 2 * ax, c)
            inner = part[:, 1 : cz + 1].reshape(n * cz * ax, c).astype(BF16)
            odd[ox, row : row + n] = inner.reshape(n, cz // 2, 2 * ax, c)

    def window(pair, ox, row, n):
        c = pair[0].shape[-1]
        lhs = [pair[i][ox, row : row + n, lo : lo + cz // 2].reshape(n * cz * ax, c) for i, lo in windows]
        return jnp.concatenate(lhs, axis=1)

    def bottom_own(pair, w):
        @stage
        def _():
            k = 3 * w.shape[1]
            pairs = []
            for ox in range(3):
                lhs = window(pair, ox, 1, cy)
                rhs = [w[ox * 9 + oy * 3 : ox * 9 + oy * 3 + 3].reshape(k, fo) for oy in range(3)]
                rhs = jnp.concatenate(rhs, axis=1)
                pairs += [(lhs[:, : k // 2], rhs[: k // 2]), (lhs[:, k // 2 :], rhs[k // 2 :])]
            halves(pairs, (deeps.at[0], deeps.at[1]))

    def bottom_rim(pair, w):
        k = 3 * w.shape[1]
        size = cz * ax
        @stage
        def _():
            for side, (row, oy) in enumerate(((0, 0), (cy + 1, 2))):
                total = jnp.zeros((size, fo), F32)
                for ox in range(3):
                    rhs = w[(ox * 3 + oy) * 3 : (ox * 3 + oy) * 3 + 3].reshape(k, fo)
                    total = total + jnp.dot(window(pair, ox, row, 1), rhs, preferred_element_type=F32)
                brims[side] = total

        def own(oy, y):
            at = (pl.ds(y * size, size), pl.ds(oy * fo, fo))
            return deeps[(0, *at)] + deeps[(1, *at)]

        lines = []
        for y in range(cy):
            before = own(0, y - 1) if y > 0 else brims[0]
            after = own(2, y + 1) if y < cy - 1 else brims[1]
            lines.append(own(1, y) + before + after)
        return jnp.maximum(jnp.concatenate(lines, axis=0), 0.0).reshape(cy, cz, ax, fo).astype(BF16)

    main4(r4)
    spread(q2, b2, gathered(sel2, l2), 1)
    loads[1].wait()
    bottom_own((q2, b2), w1)
    rim4(r4)
    block = gathered(selm, m2)
    spread(q2, b2, block[0:1], 0)
    spread(q2, b2, block[1:2], cy + 1)
    first = bottom_rim((q2, b2), w1)
    pk3[...] = first
    l3[gx, 1 : cy + 1, 1 : cz + 1] = first
    main5, rim5 = leave(column_exchange(deep_copy(pk3, l3, s5, r5), *parts_of(l3)), s5)

    skip_arrived = neighbours(p3, 1, f3, p3, g3, hx, hy, s3, r3)
    near = cx + 2
    wide = gxn * cz * near
    lane = lax.broadcasted_iota(jnp.int32, (wide, cz * ax), 1)
    row = lax.broadcasted_iota(jnp.int32, (wide, cz * ax), 0)
    shift_n = near.bit_length() - 1
    shift_z = cz.bit_length() - 1
    at = (row >> (shift_n + shift_z)) * cx + (row & (near - 1)) - 1
    at = jnp.where(jnp.logical_and(at >= 0, at < ax), at, -(cz + 1) * ax)
    share = jnp.where(lane == ((row >> shift_n) & (cz - 1)) * ax + at, 1.0, 0.0).astype(BF16)

    lane = lax.broadcasted_iota(jnp.int32, (hz, (cz + 4) * near), 1)
    zs = lax.broadcasted_iota(jnp.int32, (hz, (cz + 4) * near), 0)
    blocks = []
    for k in range(3):
        for x in range(-1, hx + 1):
            blocks.append(jnp.where(lane == (((zs + (k - 1)) >> 1) + 2) * near + (x >> 1) + 1, 1.0, 0.0))
    for k in range(3):
        blocks += blocks[k * (hx + 2) + 1 : (k + 1) * (hx + 2) - 1]
    pick = jnp.concatenate(blocks, axis=0).astype(BF16)

    def joined(row, n):
        return jnp.concatenate([l3[g, row : row + n].astype(F32) for g in range(gxn)], axis=-1)

    main5(r5)
    spread(q3, b3, joined(1, cy), 1)
    loads[2].wait()
    bottom_own((q3, b3), w2)
    rim5(r5)
    spread(q3, b3, joined(0, 1), 0)
    spread(q3, b3, joined(cy + 1, 1), cy + 1)
    second = bottom_rim((q3, b3), w2)
    for y in range(cy):
        line = second[y].astype(F32).reshape(cz * ax, fo).astype(BF16)
        line = jnp.dot(share, line, preferred_element_type=F32)
        pk4[:, y] = line.reshape(gxn, cz // 2, 2 * near, fo).astype(BF16)
    l4[gx, 1 : cy + 1, 1 : cz // 2 + 1] = pk4[gx]
    main6, rim6 = leave(column_exchange(narrow_copy, *parts_of(l4)), s6)
    size = hx * hz

    def enlarge(ys):
        fields = [l4[g, y].astype(F32).reshape((cz + 4) * near, fo) for y in ys for g in range(gxn)]
        fields = jnp.concatenate(fields, axis=-1).astype(BF16)
        fields = jnp.dot(pick, fields, preferred_element_type=F32).astype(BF16)
        for i, y in enumerate(ys):
            field = fields[:, i * c2 : (i + 1) * c2]
            for k in range(3):
                at = pl.ds(k * c2, c2)
                part = field[k * (size + 2 * hz) : (k + 1) * (size + 2 * hz)]
                up[0, y, :, :, at] = part[:size].reshape(hx // 2, 2 * hz, c2)
                up[2, y, :, :, at] = part[2 * hz :].reshape(hx // 2, 2 * hz, c2)
                part = field[3 * (size + 2 * hz) + k * size : 3 * (size + 2 * hz) + (k + 1) * size]
                up[1, y, :, :, at] = part.reshape(hx // 2, 2 * hz, c2)

    skip_arrived()
    loads[3].wait()
    total = conv(e3, o3, p3, g3, wus)
    acc[...] = total.reshape(hx, hy, hz, c1)

    main6(r6)
    enlarge(range(1, cy + 1))
    loads[4].wait()

    @stage
    def _():
        pairs = []
        for ox in range(3):
            for k in range(3):
                lhs = up[ox, 1 : cy + 1, :, :, pl.ds(k * c2, c2)].reshape(cy * size, c2)
                pairs.append((lhs, wuu[ox * 9 + 3 + k]))
        halves(pairs, (thirds.at[0], thirds.at[1]))

    rim6(r6)
    enlarge((0, cy + 1))

    @stage
    def _():
        for side, oy in enumerate((0, 2)):
            total = jnp.zeros(((cy + 1) * size, c1), F32)
            for ox in range(3):
                lhs = up[ox, side : side + cy + 1].reshape((cy + 1) * size, 3 * c2)
                rhs = wuu[(ox * 3 + oy) * 3 : (ox * 3 + oy) * 3 + 3].reshape(3 * c2, c1)
                total = total + jnp.dot(lhs, rhs, preferred_element_type=F32)
            ends[side] = total

    for y in range(hy):
        low, mid, high = (y + 1) // 2, (y + 2) // 2 - 1, (y + 3) // 2 - 1
        total = ends[0, low * size : (low + 1) * size] + ends[1, high * size : (high + 1) * size]
        total = total + thirds[0, mid * size : (mid + 1) * size] + thirds[1, mid * size : (mid + 1) * size]
        out[:, y] = (acc[:, y] + total.reshape(hx, hz, c1)).astype(BF16)

    for fn in late:
        fn()


def on_device(dims, volume, w_full, w_half, w_bottom_in, w_bottom_out, w_up):
    gxn, gyn = dims
    nx, ny, nz, c0 = volume.shape
    c1 = w_half.shape[4]
    c2, fo = w_bottom_out.shape[3:]
    hx, hy, hz = nx // 2, ny // 2, nz // 2
    cx, cy, cz = hx // 2, hy // 2, hz // 2
    ax = gxn * cx
    weights = [
        w_full.reshape(3, 3, 3 * c0, c0),
        w_half.reshape(27, c0, c1),
        w_bottom_in.reshape(27, c1, fo),
        w_bottom_out.reshape(27, c2, fo),
        w_up.reshape(27, c2 + c1, c1),
    ]
    vm = pltpu.VMEM
    dma = pltpu.SemaphoreType.DMA
    scratch = [vm(w.shape, BF16) for w in weights[1:4]]
    scratch += [vm((27, c1, c1), BF16), vm((27, c2, c1), BF16), dma((5,)), dma(()), dma(())]
    scratch += [vm((3, 4, 3 * c0, 2 * c0), BF16), vm((9 * c0, c0), BF16)]
    scratch += [
        vm((nx + 2, ny + 2, nz, c0), BF16), vm((nx, ny, 1, c0), F32), vm((nx + 2, ny + 2, 1, c0), F32),
        vm((nx + 2, ny + 2, c0), F32), vm((nx + 2, ny + 2, nz, 3 * c0), BF16), vm((hx, ny * nz, 2 * c0), F32),
        vm((nx * ny, c0), F32), vm((hy, nz, c0), F32),
        vm((hx + 2, hy + 2, hz, c0), BF16), vm((hx, hy, 1, c0), F32), vm((hx + 2, hy + 2, 1, c0), F32),
        vm((hx + 2, hy // 2 + 1, 2 * hz, 3 * c0), BF16), vm((hx + 2, hy // 2, 2 * hz, 3 * c0), BF16),
        vm((hx + 2, hy + 2, hz, c1), BF16), vm((hx, hy, 1, c1), F32), vm((hx + 2, hy + 2, 1, c1), F32),
        vm((hx + 2, hy // 2 + 1, 2 * hz, 3 * c1), BF16), vm((hx + 2, hy // 2, 2 * hz, 3 * c1), BF16),
        vm((hx, hy, hz, c1), F32),
        vm((cy + 1, cz * cx, c1), BF16), vm((gxn, cy + 1, cz * cx, c1), BF16), vm((gxn, 4, cz * cx, c1), BF16),
        vm((cy, cz + 2, ax, gxn * (cy + 1) * cz * cx), F32), vm((2, cz + 2, ax, gxn * 4 * cz * cx), F32),
        vm((3, cy + 2, cz // 2 + 1, 2 * ax, c1), BF16), vm((3, cy + 2, cz // 2, 2 * ax, c1), BF16),
        vm((cy, cz, ax, fo), BF16), vm((gxn, cy + 2, cz + 2, ax, fo), BF16),
        vm((3, cy + 2, cz // 2 + 1, 2 * ax, c2), BF16), vm((3, cy + 2, cz // 2, 2 * ax, c2), BF16),
        vm((gxn, cy, cz // 2, 2 * (cx + 2), fo), BF16), vm((gxn, cy + 2, cz // 2 + 2, 2 * (cx + 2), fo), BF16),
        vm((3, cy + 2, hx // 2, 2 * hz, 3 * c2), BF16),
        vm((2, hx * hy * hz, c1), F32), vm((2, cy * cz * ax, 3 * fo), F32), vm((2, cz * ax, fo), F32),
        vm((2, cy * hx * hz, c1), F32), vm((2, (cy + 1) * hx * hz, c1), F32),
    ]
    scratch += [dma((3,))] * 12
    return pl.pallas_call(
        functools.partial(kernel, dims),
        out_shape=jax.ShapeDtypeStruct((hx, hy, hz, c1), BF16),
        in_specs=[pl.BlockSpec(memory_space=pltpu.HBM)] * 6,
        out_specs=pl.BlockSpec(memory_space=pltpu.VMEM),
        scratch_shapes=scratch,
        compiler_params=pltpu.CompilerParams(
            collective_id=0, has_side_effects=True, vmem_limit_bytes=52 * 1024 * 1024
        ),
    )(*[pltpu.with_memory_space_constraint(a, pltpu.HBM) for a in (volume, *weights)])


def solution(mesh):
    dims = (mesh.shape["gx"], mesh.shape["gy"])
    assert mesh.shape["gz"] == 2
    return jax.shard_map(
        functools.partial(on_device, dims),
        mesh=mesh,
        in_specs=(
            P("gx", "gy", "gz", None),
            P(),
            P(),
            P(None, None, None, None, "gx"),
            P(None, None, None, None, "gx"),
            P(),
        ),
        out_specs=P("gx", "gy", "gz", None),
        check_vma=False,
    )
```

```python
import functools

import jax
import jax.numpy as jnp
from jax import lax
from jax.experimental import pallas as pl
from jax.experimental.pallas import tpu as pltpu
from jax.sharding import PartitionSpec as P

F32 = jnp.float32
BF16 = jnp.bfloat16
STEPS = [(dx, dy) for dx in (-1, 0, 1) for dy in (-1, 0, 1)]


def span(d, n, pad):
    if d == 0:
        return pl.ds(pad, n), pl.ds(1, n)
    if d < 0:
        return pl.ds(pad, 1), pl.ds(n + 1, 1)
    return pl.ds(pad + n - 1, 1), pl.ds(0, 1)


def halves(pairs, refs):
    for i, ref in enumerate(refs):
        total = None
        for lhs, rhs in pairs[i::2]:
            part = jnp.dot(lhs, rhs, preferred_element_type=F32)
            total = part if total is None else total + part
        ref[...] = total


def kernel(
    dims,
    v_h, wf_h, wh_h, w1_h, w2_h, wu_h,
    out,
    wh, w1, w2, wus, wuu, wsem, vsem, fsem, wt, wz,
    p1, f1, g1, gs, e1, a1, rz, t1,
    p2, f2, g2, e2, o2,
    p3, f3, g3, e3, o3, acc,
    pk2, l2, m2, sel2, selm, q2, b2, pk3, l3, q3, b3, pk4, l4, up, sums, deeps, brims, thirds, ends,
    s1, r1, s2, r2, s3, r3, s4, r4, s5, r5, s6, r6,
):
    gxn, gyn = dims
    gx, gy, gz = lax.axis_index("gx"), lax.axis_index("gy"), lax.axis_index("gz")
    oz = 1 - gz

    nx, ny, nz, c0 = v_h.shape
    fetch = pltpu.make_async_copy(v_h, p1.at[1 : nx + 1, 1 : ny + 1], vsem)
    fetch.start()
    c2 = w2.shape[1]
    loads = [
        pltpu.make_async_copy(src, dst, wsem.at[i])
        for i, (src, dst) in enumerate((
            (wh_h, wh), (w1_h, w1), (w2_h, w2), (wu_h.at[:, c2:], wus), (wu_h.at[:, :c2], wuu),
        ))
    ]

    def on(cond, fn):
        if cond is True:
            fn()
        else:
            pl.when(cond)(fn)

    def exists(dx, dy):
        conds = []
        if dx < 0:
            conds.append(gx > 0)
        if dx > 0:
            conds.append(gx < gxn - 1)
        if dy < 0:
            conds.append(gy > 0)
        if dy > 0:
            conds.append(gy < gyn - 1)
        if not conds:
            return True
        return functools.reduce(jnp.logical_and, conds)

    for x in (0, nx + 1):
        p1[x] = jnp.zeros(p1.shape[1:], BF16)
    for y in (0, ny + 1):
        p1[1 : nx + 1, y] = jnp.zeros((nx, nz, c0), BF16)
    m2[...] = jnp.zeros_like(m2)
    for x in (0, nx + 1):
        g1[x] = jnp.zeros(g1.shape[1:], F32)
    for y in (0, ny + 1):
        g1[:, y] = jnp.zeros((nx + 2, 1, c0), F32)

    barrier = pltpu.get_barrier_semaphore()
    for s in range(gxn):
        there = lax.rem(gx + s, gxn)
        for dy in (-1, 0, 1):
            for z in (0, 1):
                if s == 0 and dy == 0 and z == 0:
                    continue

                def signal(there=there, dy=dy, z=z):
                    pl.semaphore_signal(
                        barrier, inc=1,
                        device_id={"gx": there, "gy": gy + dy, "gz": oz if z else gz},
                        device_id_type=pl.DeviceIdType.MESH,
                    )

                on(exists(0, dy), signal)
    k0 = 3 * c0
    for oy in range(3):
        for first, lane in ((0, 0), (1, c0)):
            dst = wt.at[oy, first : first + 3, :, lane : lane + c0]
            pltpu.make_async_copy(wf_h.at[:, oy], dst, fsem).start()
    lines = 1 + (gy > 0).astype(jnp.int32) + (gy < gyn - 1).astype(jnp.int32)

    def edge(block):
        size = block.shape[-2]
        rows = lax.broadcasted_iota(jnp.int32, block.shape, block.ndim - 2)
        return jnp.sum(jnp.where(rows == (size - 1) * oz, block, 0.0), axis=block.ndim - 2, keepdims=True)

    for ref in (g2, g3):
        ref[...] = jnp.zeros(ref.shape, ref.dtype)
    for ref in (p2, p3):
        for x in (0, ref.shape[0] - 1):
            ref[x] = jnp.zeros(ref.shape[1:], BF16)
        for y in (0, ref.shape[1] - 1):
            ref[:, y] = jnp.zeros(ref.shape[:1] + ref.shape[2:], BF16)
    for x in (0, nx + 1):
        e1[x] = jnp.zeros(e1.shape[1:], BF16)
    for y in (0, ny + 1):
        e1[1 : nx + 1, y] = jnp.zeros((nx, nz, k0), BF16)
    for oy in range(3):
        wt[oy, 3, :, :c0] = jnp.zeros((k0, c0), BF16)
        wt[oy, 0, :, c0:] = jnp.zeros((k0, c0), BF16)
    fetch.wait()
    for load in loads:
        load.start()
    for x in range(nx):
        f1[x] = edge(p1[x + 1, 1 : ny + 1].astype(F32))
    pl.semaphore_wait(barrier, 2 * gxn * lines - 1)

    def send(src, dst, ss, rs, x, y, z):
        return pltpu.make_async_remote_copy(
            src_ref=src, dst_ref=dst, send_sem=ss, recv_sem=rs,
            device_id={"gx": x, "gy": y, "gz": z}, device_id_type=pl.DeviceIdType.MESH,
        )

    many_x = jnp.logical_and(gx > 0, gx < gxn - 1)
    many_y = jnp.logical_and(gy > 0, gy < gyn - 1)

    def by_y(fn):
        for b in (1, 2):
            pl.when(many_y if b == 2 else jnp.logical_not(many_y))(functools.partial(fn, b))

    def by_xy(fn):
        for a in (1, 2):
            for b in (1, 2):
                cx_ = many_x if a == 2 else jnp.logical_not(many_x)
                cy_ = many_y if b == 2 else jnp.logical_not(many_y)
                pl.when(jnp.logical_and(cx_, cy_))(functools.partial(fn, a, b))

    def drain(ref, sem):
        pltpu.make_async_copy(ref, ref, sem).wait()

    stage = pl.when(gx < gxn)
    short = jnp.minimum(gx, gxn - 1 - gx)
    farthest = []
    for i in range(gxn - 1, 0, -1):
        paired = gx + ((i + 1) // 2 if i % 2 else -(i // 2))
        rest = jnp.where(gx < gxn - 1 - gx, gx + (i - short), gx - (i - short))
        farthest.append(jnp.where(i <= 2 * short, paired, rest))

    late = []

    def neighbours(src, pad, face, rim, side, nx, ny, ss, rs):
        copies = []
        for dx, dy in STEPS:
            sx, tx = span(dx, nx, pad)
            sy, ty = span(dy, ny, pad)
            fx, _ = span(dx, nx, 0)
            fy, _ = span(dy, ny, 0)
            hops = abs(dx) + abs(dy)
            to = (gx + dx, gy + dy)
            copies.append((hops + 1, exists(dx, dy), send(face.at[fx, fy], side.at[tx, ty], ss.at[0], rs.at[0], *to, oz)))
            if hops:
                k = 1 if dx else 2
                copy = send(src.at[sx, sy], rim.at[tx, ty], ss.at[k], rs.at[k], *to, gz)
                copies.append((hops, exists(dx, dy), copy))
        for _, cond, copy in sorted(copies, key=lambda entry: -entry[0]):
            on(cond, copy.start)

        def finish(sems):
            def both(a, b):
                drain(side.at[0 : nx + a, 0 : ny + b], sems.at[0])
                drain(rim.at[0:a, 0 : ny + b], sems.at[1])
                drain(rim.at[0:nx, 0:b], sems.at[2])

            by_xy(both)

        late.append(lambda: finish(ss))
        return lambda: finish(rs)

    def shifted(block, fill):
        size = block.shape[-2]
        axis = block.ndim - 2
        rows = lax.broadcasted_iota(jnp.int32, block.shape, axis)
        below = jnp.where(rows == 0, 0.0, pltpu.roll(block, 1, axis))
        above = jnp.where(rows == size - 1, 0.0, pltpu.roll(block, size - 1, axis))
        if fill is not None:
            fill = jnp.broadcast_to(fill, block.shape)
            below = jnp.where(rows == jnp.where(gz == 1, 0, -1), fill, below)
            above = jnp.where(rows == jnp.where(gz == 0, size - 1, -1), fill, above)
        return below, above

    def rounded(x):
        return x.astype(BF16).astype(F32)

    arrived = neighbours(p1, 1, f1, p1, g1, nx, ny, s1, r1)

    def widen(at, block):
        block = block.astype(F32)
        below, above = shifted(block, None)
        for k, part in enumerate((below, block, above)):
            e1[at + (slice(None), pl.ds(k * c0, c0))] = part.astype(BF16)

    @pl.loop(1, nx + 1)
    def _(x):
        widen((x, pl.ds(1, ny)), p1[x, 1 : ny + 1])

    drain(wt.at[:, 0:3], fsem)

    group1 = 2 if nx % 4 == 0 else 1

    @pl.loop(0, nx // (2 * group1))
    def _(step):
        total = jnp.zeros((group1 * ny * nz, 2 * c0), F32)
        for oy in range(3):
            for half in range(2):
                lhs = []
                for i in range(2):
                    planes = [2 * (step * group1 + n) + 2 * half + i for n in range(group1)]
                    planes = [e1[x, oy : oy + ny].reshape(ny * nz, k0) for x in planes]
                    lhs.append(jnp.concatenate(planes, axis=0))
                rhs = wt[oy, 2 * half : 2 * half + 2].reshape(2 * k0, 2 * c0)
                total = total + jnp.dot(jnp.concatenate(lhs, axis=1), rhs, preferred_element_type=F32)
        for n in range(group1):
            a1[step * group1 + n] = total[n * ny * nz : (n + 1) * ny * nz]

    for ox in range(3):
        for oy in range(3):
            tap = wt[oy, ox, pl.ds(pl.multiple_of(2 * oz * c0, c0), c0), :c0]
            wz[(ox * 3 + oy) * c0 : (ox * 3 + oy + 1) * c0] = tap
    arrived()
    for x in range(nx + 2):
        for y in range(ny + 2):
            gs[x, y : y + 1] = g1[x, y]
    @stage
    def _():
        lhs = [gs[ox : ox + nx, oy : oy + ny].reshape(nx * ny, c0).astype(BF16) for ox in range(3) for oy in range(3)]
        rz[...] = jnp.dot(jnp.concatenate(lhs, axis=1), wz[...], preferred_element_type=F32)
        for x, ox, lane in ((0, 0, 0), (nx + 1, 2, c0)):
            widen((x, pl.ds(1, ny)), p1[x, 1 : ny + 1])
            lhs = [e1[x, oy : oy + ny].reshape(ny * nz, k0) for oy in range(3)]
            rhs = jnp.concatenate([wt[oy, ox, :, :c0] for oy in range(3)], axis=0)
            part = jnp.dot(jnp.concatenate(lhs, axis=1), rhs, preferred_element_type=F32)
            at = (0 if ox == 0 else nx // 2 - 1, slice(None), pl.ds(lane, c0))
            a1[at] = a1[at] + part
        for y, oy in ((0, 0), (ny + 1, 2)):
            widen((pl.ds(0, nx + 2), y), p1[:, y])
            lhs = [e1[ox : ox + nx, y].reshape(nx * nz, k0) for ox in range(3)]
            rhs = jnp.concatenate([wt[oy, ox, :, :c0] for ox in range(3)], axis=0)
            part = jnp.dot(jnp.concatenate(lhs, axis=1), rhs, preferred_element_type=F32).reshape(nx, nz, c0)
            for x in range(nx):
                at = (x // 2, pl.ds((0 if oy == 0 else ny - 1) * nz, nz), pl.ds(x % 2 * c0, c0))
                a1[at] = a1[at] + part[x]

    tile = 8
    last = lax.broadcasted_iota(jnp.int32, (tile, c0), 0) == (tile - 1) * oz
    for x in range(nx):
        for y in range(ny):
            at = (x // 2, pl.ds(pl.multiple_of(y * nz + (nz - tile) * oz, tile), tile), pl.ds(x % 2 * c0, c0))
            row = jnp.broadcast_to(rz[x * ny + y : x * ny + y + 1], (tile, c0))
            a1[at] = a1[at] + jnp.where(last, row, 0.0)

    hx, hy, hz = nx // 2, ny // 2, nz // 2

    @pl.loop(0, hx)
    def _(x):
        total = a1[x]
        both = jnp.maximum(jnp.maximum(total[:, :c0], total[:, c0:]), 0.0).reshape(hy, 2, nz, c0)
        t1[...] = jnp.max(both, axis=1)
        small = jnp.maximum(t1[:, pl.ds(0, hz, stride=2), :], t1[:, pl.ds(1, hz, stride=2), :])
        small = rounded(small)
        p2[x + 1, 1 : hy + 1] = small.astype(BF16)
        f2[x] = edge(small)

    arrived = neighbours(p2, 1, f2, p2, g2, hx, hy, s2, r2)
    for ref in (l3, l4):
        ref[...] = jnp.zeros(ref.shape, ref.dtype)
    arrived()
    rows = hx * hy * hz

    def pack(even, odd, at, block, lane):
        n, size, c = block.shape
        even[at, :, :, pl.ds(lane, c)] = block.reshape(n * size, c).astype(BF16).reshape(n // 2, 2 * size, c)
        block = block[1 : n - 1]
        odd[at, :, :, pl.ds(lane, c)] = block.reshape((n - 2) * size, c).astype(BF16).reshape(n // 2 - 1, 2 * size, c)

    def conv(even, odd, p, g, w):
        for x in range(hx + 2):
            block = p[x].astype(F32)
            c = block.shape[-1]
            below, above = shifted(block, g[x])
            for k, part in enumerate((below, block, above)):
                pack(even, odd, x, part, k * c)
        @stage
        def _():
            pairs = []
            for ox in range(3):
                for oy, (r, lo) in enumerate(((even, 0), (odd, 0), (even, 1))):
                    rhs = w[ox * 9 + oy * 3 : ox * 9 + oy * 3 + 3].reshape(3 * c, w.shape[2])
                    pairs.append((r[ox : ox + hx, lo : lo + hy // 2].reshape(rows, 3 * c), rhs))
            halves(pairs, (sums.at[0], sums.at[1]))

        return sums[0] + sums[1]

    loads[0].wait()
    c1 = wh.shape[2]
    total = conv(e2, o2, p2, g2, wh)
    skip = rounded(jnp.maximum(total, 0.0)).reshape(hx, hy, hz, c1)
    p3[1 : hx + 1, 1 : hy + 1] = skip.astype(BF16)

    cx, cy, cz = hx // 2, hy // 2, hz // 2
    ax = gxn * cx
    group = cz * cx
    m = jnp.max(skip.reshape(cx, 2, cy, 2, hz, c1), axis=(1, 3))
    m = m.reshape(cx * cy * hz, c1)
    m = jnp.maximum(m, pltpu.roll(m, m.shape[0] - 1, 0)).astype(BF16)

    blocks = []
    lane = lax.broadcasted_iota(jnp.int32, (group, cx * cy * hz), 1)
    sub = lax.broadcasted_iota(jnp.int32, (group, cx * cy * hz), 0)
    shift_x = cx.bit_length() - 1
    sub_x = sub & (cx - 1)
    sub_o = sub >> shift_x
    for y in range(cy):
        blocks.append(jnp.where(lane == (sub_x * cy + y) * hz + 2 * sub_o, 1.0, 0.0))
    blocks.append(jnp.where(lane == (sub_x * cy + sub_o) * hz + 2 * (cz - 1) * oz, 1.0, 0.0))
    pick = jnp.concatenate(blocks, axis=0).astype(BF16)
    packets = jnp.dot(pick, m, preferred_element_type=F32).reshape(cy + 1, group, c1).astype(BF16)
    pk2[...] = packets
    l2[gx, 0:cy] = packets[0:cy]

    def coarse_copy(k, dy, z):
        def make(src_gx, tgt_gx):
            if z == 0:
                src = {0: pl.ds(0, cy), -1: pl.ds(0, 1), 1: pl.ds(cy - 1, 1)}[dy]
            else:
                src = pl.ds(cy, 1)
            if dy == 0:
                dst = l2.at[src_gx, pl.ds(cy, 1) if z else pl.ds(0, cy)]
            else:
                dst = m2.at[src_gx, pl.ds(2 * z + (1 if dy < 0 else 0), 1)]
            return send(pk2.at[src], dst, s4.at[k], r4.at[k], tgt_gx, gy + dy, oz if z else gz)

        return make

    def deep_copy(pk, land, ss, rs):
        def choose(k, dy, z):
            def make(src_gx, tgt_gx):
                sy, ty = span(dy, cy, 0)
                sender = gz if src_gx is gx else (oz if z else gz)
                if z == 0:
                    src = pk.at[sy]
                    dst = land.at[src_gx, ty, pl.ds(1, cz)]
                else:
                    src = pk.at[sy, pl.ds((cz - 1) * (1 - sender), 1)]
                    dst = land.at[src_gx, ty, pl.ds((cz + 1) * sender, 1)]
                return send(src, dst, ss.at[k], rs.at[k], tgt_gx, gy + dy, oz if z else gz)

            return make

        return choose

    def narrow_copy(k, dy, z):
        def make(src_gx, tgt_gx):
            sy, ty = span(dy, cy, 0)
            sender = gz if src_gx is gx else (oz if z else gz)
            if z == 0:
                src = pk4.at[tgt_gx, sy]
                dst = l4.at[src_gx, ty, pl.ds(1, cz // 2)]
            else:
                src = pk4.at[tgt_gx, sy, pl.ds((cz // 2 - 1) * (1 - sender), 1)]
                dst = l4.at[src_gx, ty, pl.ds((cz // 2 + 1) * sender, 1)]
            return send(src, dst, s6.at[k], r6.at[k], tgt_gx, gy + dy, oz if z else gz)

        return make

    upper = lax.rem(gy, 2) == 1
    lower = lax.rem(gy, 2) == 0
    across = {-1: jnp.logical_and(lower, gy > 0), 1: jnp.logical_and(upper, gy < gyn - 1)}
    within = {-1: upper, 1: lower}

    def column_exchange(choose, main, rim, relay, carry, ss, rs):
        order = [(there, 0, z, 0) for there in farthest for z in (1, 0)]
        order += [(gx, 0, 1, 1)]
        for there, dy, z, k in order:
            choose(k, dy, z)(gx, there).start()
        for there in farthest + [gx]:
            for z in (1, 0):
                for dy in (-1, 1):
                    on(across[dy], choose(2, dy, z)(gx, there).start)

        def own(which):
            for k, ref in enumerate(main):
                drain(ref, which.at[k])

        def edges(which):
            for dy in (-1, 1):
                on(across[dy], lambda: drain(rim, which.at[2]))
            drain(relay, which.at[3])

        def arrive():
            own(rs)
            for dy in (-1, 1):
                for src, dst in carry(dy):
                    on(within[dy], send(src, dst, ss.at[3], rs.at[3], gx, gy + dy, gz).start)

        def finish():
            own(ss)
            edges(ss)

        late.append(finish)
        return arrive, lambda: edges(rs)

    def parts_of(land):
        wz = land.shape[2] - 2

        def carry(dy):
            rows = (cy, 0) if dy > 0 else (1, cy + 1)
            return [tuple(land.at[:, row] for row in rows)]

        main = (land.at[0 : gxn - 1, 0:cy, 0 : wz + 1], land.at[0, 0:cy, 0:1])
        return main, land.at[0:gxn, 0:1, 0 : wz + 1], land.at[:, 0], carry

    def carry_lines(dy):
        pairs = ((cy - 1, 0), (cy, 2)) if dy > 0 else ((0, 1), (cy, 3))
        return [(l2.at[:, line], m2.at[:, slot]) for line, slot in pairs]

    main4, rim4 = column_exchange(
        coarse_copy, (l2.at[0 : gxn - 1], l2.at[0, 0:1]), m2.at[:, 0:2], m2.at[:, 0:2], carry_lines, s4, r4
    )
    for x in range(hx):
        f3[x] = edge(p3[x + 1, 1 : hy + 1].astype(F32))

    def one_hot(ref, at, slots):
        width = gxn * slots * group
        lane = lax.broadcasted_iota(jnp.int32, (ax, width), 1)
        xs = lax.broadcasted_iota(jnp.int32, (ax, width), 0)
        base = lane - ((xs >> shift_x) * slots * group + (xs & (cx - 1)))
        ref[at] = jnp.where(base == slots_at, 1.0, 0.0)

    for y in range(-1, cy + 1):
        for z in range(-1, cz + 1):
            inside = 0 <= y < cy
            rim_slot = 0 if y < 0 else 1
            if 0 <= z < cz:
                slots_at = (y if inside else rim_slot) * group + z * cx
            else:
                line = y if inside else (cy - 1 if y < 0 else 0)
                mine = (gz == 1) if z < 0 else (gz == 0)
                slots_at = jnp.where(mine, (cy if inside else 2 + rim_slot) * group + line * cx, -(1 << 20))
            if inside:
                one_hot(sel2, (y, z + 1), cy + 1)
            else:
                one_hot(selm, (rim_slot, z + 1), 4)

    def gathered(ref, land):
        n, width = ref.shape[0], ref.shape[-1]
        select = ref[...].reshape(n * (cz + 2) * ax, width).astype(BF16)
        landed = land[...].astype(F32).reshape(width, c1).astype(BF16)
        return jnp.dot(select, landed, preferred_element_type=F32).reshape(n, cz + 2, ax, c1)

    deep = cy * cz * ax
    fo = w1.shape[2]

    windows = ((0, 0), (1, 0), (0, 1))

    def spread(even, odd, block, row):
        below, above = shifted(block, None)
        n, c = block.shape[0], block.shape[-1]
        for ox, part in enumerate((below, block, above)):
            whole = part.reshape(n * (cz + 2) * ax, c).astype(BF16)
            even[ox, row : row + n] = whole.reshape(n, cz // 2 + 1, 2 * ax, c)
            inner = part[:, 1 : cz + 1].reshape(n * cz * ax, c).astype(BF16)
            odd[ox, row : row + n] = inner.reshape(n, cz // 2, 2 * ax, c)

    def window(pair, ox, row, n):
        c = pair[0].shape[-1]
        lhs = [pair[i][ox, row : row + n, lo : lo + cz // 2].reshape(n * cz * ax, c) for i, lo in windows]
        return jnp.concatenate(lhs, axis=1)

    def bottom_own(pair, w):
        @stage
        def _():
            k = 3 * w.shape[1]
            pairs = []
            for ox in range(3):
                lhs = window(pair, ox, 1, cy)
                rhs = [w[ox * 9 + oy * 3 : ox * 9 + oy * 3 + 3].reshape(k, fo) for oy in range(3)]
                rhs = jnp.concatenate(rhs, axis=1)
                pairs += [(lhs[:, : k // 2], rhs[: k // 2]), (lhs[:, k // 2 :], rhs[k // 2 :])]
            halves(pairs, (deeps.at[0], deeps.at[1]))

    def bottom_rim(pair, w):
        k = 3 * w.shape[1]
        size = cz * ax
        @stage
        def _():
            for side, (row, oy) in enumerate(((0, 0), (cy + 1, 2))):
                total = jnp.zeros((size, fo), F32)
                for ox in range(3):
                    rhs = w[(ox * 3 + oy) * 3 : (ox * 3 + oy) * 3 + 3].reshape(k, fo)
                    total = total + jnp.dot(window(pair, ox, row, 1), rhs, preferred_element_type=F32)
                brims[side] = total

        def own(oy, y):
            at = (pl.ds(y * size, size), pl.ds(oy * fo, fo))
            return deeps[(0, *at)] + deeps[(1, *at)]

        lines = []
        for y in range(cy):
            before = own(0, y - 1) if y > 0 else brims[0]
            after = own(2, y + 1) if y < cy - 1 else brims[1]
            lines.append(own(1, y) + before + after)
        return jnp.maximum(jnp.concatenate(lines, axis=0), 0.0).reshape(cy, cz, ax, fo).astype(BF16)

    main4()
    spread(q2, b2, gathered(sel2, l2), 1)
    loads[1].wait()
    bottom_own((q2, b2), w1)
    rim4()
    block = gathered(selm, m2)
    spread(q2, b2, block[0:1], 0)
    spread(q2, b2, block[1:2], cy + 1)
    first = bottom_rim((q2, b2), w1)
    pk3[...] = first
    l3[gx, 1 : cy + 1, 1 : cz + 1] = first
    main5, rim5 = column_exchange(deep_copy(pk3, l3, s5, r5), *parts_of(l3), s5, r5)

    skip_arrived = neighbours(p3, 1, f3, p3, g3, hx, hy, s3, r3)
    near = cx + 2
    wide = gxn * cz * near
    lane = lax.broadcasted_iota(jnp.int32, (wide, cz * ax), 1)
    row = lax.broadcasted_iota(jnp.int32, (wide, cz * ax), 0)
    shift_n = near.bit_length() - 1
    shift_z = cz.bit_length() - 1
    at = (row >> (shift_n + shift_z)) * cx + (row & (near - 1)) - 1
    at = jnp.where(jnp.logical_and(at >= 0, at < ax), at, -(cz + 1) * ax)
    share = jnp.where(lane == ((row >> shift_n) & (cz - 1)) * ax + at, 1.0, 0.0).astype(BF16)

    lane = lax.broadcasted_iota(jnp.int32, (hz, (cz + 4) * near), 1)
    zs = lax.broadcasted_iota(jnp.int32, (hz, (cz + 4) * near), 0)
    blocks = []
    for k in range(3):
        for x in range(-1, hx + 1):
            blocks.append(jnp.where(lane == (((zs + (k - 1)) >> 1) + 2) * near + (x >> 1) + 1, 1.0, 0.0))
    for k in range(3):
        blocks += blocks[k * (hx + 2) + 1 : (k + 1) * (hx + 2) - 1]
    pick = jnp.concatenate(blocks, axis=0).astype(BF16)

    def joined(row, n):
        return jnp.concatenate([l3[g, row : row + n].astype(F32) for g in range(gxn)], axis=-1)

    main5()
    spread(q3, b3, joined(1, cy), 1)
    loads[2].wait()
    bottom_own((q3, b3), w2)
    rim5()
    spread(q3, b3, joined(0, 1), 0)
    spread(q3, b3, joined(cy + 1, 1), cy + 1)
    second = bottom_rim((q3, b3), w2)
    for y in range(cy):
        line = second[y].astype(F32).reshape(cz * ax, fo).astype(BF16)
        line = jnp.dot(share, line, preferred_element_type=F32)
        pk4[:, y] = line.reshape(gxn, cz // 2, 2 * near, fo).astype(BF16)
    l4[gx, 1 : cy + 1, 1 : cz // 2 + 1] = pk4[gx]
    main6, rim6 = column_exchange(narrow_copy, *parts_of(l4), s6, r6)
    size = hx * hz

    def enlarge(ys):
        fields = [l4[g, y].astype(F32).reshape((cz + 4) * near, fo) for y in ys for g in range(gxn)]
        fields = jnp.concatenate(fields, axis=-1).astype(BF16)
        fields = jnp.dot(pick, fields, preferred_element_type=F32).astype(BF16)
        for i, y in enumerate(ys):
            field = fields[:, i * c2 : (i + 1) * c2]
            for k in range(3):
                at = pl.ds(k * c2, c2)
                part = field[k * (size + 2 * hz) : (k + 1) * (size + 2 * hz)]
                up[0, y, :, :, at] = part[:size].reshape(hx // 2, 2 * hz, c2)
                up[2, y, :, :, at] = part[2 * hz :].reshape(hx // 2, 2 * hz, c2)
                part = field[3 * (size + 2 * hz) + k * size : 3 * (size + 2 * hz) + (k + 1) * size]
                up[1, y, :, :, at] = part.reshape(hx // 2, 2 * hz, c2)

    skip_arrived()
    loads[3].wait()
    total = conv(e3, o3, p3, g3, wus)
    acc[...] = total.reshape(hx, hy, hz, c1)

    main6()
    enlarge(range(1, cy + 1))
    loads[4].wait()

    @stage
    def _():
        pairs = []
        for ox in range(3):
            for k in range(3):
                lhs = up[ox, 1 : cy + 1, :, :, pl.ds(k * c2, c2)].reshape(cy * size, c2)
                pairs.append((lhs, wuu[ox * 9 + 3 + k]))
        halves(pairs, (thirds.at[0], thirds.at[1]))

    rim6()
    enlarge((0, cy + 1))

    @stage
    def _():
        for side, oy in enumerate((0, 2)):
            total = jnp.zeros(((cy + 1) * size, c1), F32)
            for ox in range(3):
                lhs = up[ox, side : side + cy + 1].reshape((cy + 1) * size, 3 * c2)
                rhs = wuu[(ox * 3 + oy) * 3 : (ox * 3 + oy) * 3 + 3].reshape(3 * c2, c1)
                total = total + jnp.dot(lhs, rhs, preferred_element_type=F32)
            ends[side] = total

    for y in range(hy):
        low, mid, high = (y + 1) // 2, (y + 2) // 2 - 1, (y + 3) // 2 - 1
        total = ends[0, low * size : (low + 1) * size] + ends[1, high * size : (high + 1) * size]
        total = total + thirds[0, mid * size : (mid + 1) * size] + thirds[1, mid * size : (mid + 1) * size]
        out[:, y] = (acc[:, y] + total.reshape(hx, hz, c1)).astype(BF16)

    for fn in late:
        fn()


def on_device(dims, volume, w_full, w_half, w_bottom_in, w_bottom_out, w_up):
    gxn, gyn = dims
    nx, ny, nz, c0 = volume.shape
    c1 = w_half.shape[4]
    c2, fo = w_bottom_out.shape[3:]
    hx, hy, hz = nx // 2, ny // 2, nz // 2
    cx, cy, cz = hx // 2, hy // 2, hz // 2
    ax = gxn * cx
    weights = [
        w_full.reshape(3, 3, 3 * c0, c0),
        w_half.reshape(27, c0, c1),
        w_bottom_in.reshape(27, c1, fo),
        w_bottom_out.reshape(27, c2, fo),
        w_up.reshape(27, c2 + c1, c1),
    ]
    vm = pltpu.VMEM
    dma = pltpu.SemaphoreType.DMA
    scratch = [vm(w.shape, BF16) for w in weights[1:4]]
    scratch += [vm((27, c1, c1), BF16), vm((27, c2, c1), BF16), dma((5,)), dma(()), dma(())]
    scratch += [vm((3, 4, 3 * c0, 2 * c0), BF16), vm((9 * c0, c0), BF16)]
    scratch += [
        vm((nx + 2, ny + 2, nz, c0), BF16), vm((nx, ny, 1, c0), F32), vm((nx + 2, ny + 2, 1, c0), F32),
        vm((nx + 2, ny + 2, c0), F32), vm((nx + 2, ny + 2, nz, 3 * c0), BF16), vm((hx, ny * nz, 2 * c0), F32),
        vm((nx * ny, c0), F32), vm((hy, nz, c0), F32),
        vm((hx + 2, hy + 2, hz, c0), BF16), vm((hx, hy, 1, c0), F32), vm((hx + 2, hy + 2, 1, c0), F32),
        vm((hx + 2, hy // 2 + 1, 2 * hz, 3 * c0), BF16), vm((hx + 2, hy // 2, 2 * hz, 3 * c0), BF16),
        vm((hx + 2, hy + 2, hz, c1), BF16), vm((hx, hy, 1, c1), F32), vm((hx + 2, hy + 2, 1, c1), F32),
        vm((hx + 2, hy // 2 + 1, 2 * hz, 3 * c1), BF16), vm((hx + 2, hy // 2, 2 * hz, 3 * c1), BF16),
        vm((hx, hy, hz, c1), F32),
        vm((cy + 1, cz * cx, c1), BF16), vm((gxn, cy + 1, cz * cx, c1), BF16), vm((gxn, 4, cz * cx, c1), BF16),
        vm((cy, cz + 2, ax, gxn * (cy + 1) * cz * cx), F32), vm((2, cz + 2, ax, gxn * 4 * cz * cx), F32),
        vm((3, cy + 2, cz // 2 + 1, 2 * ax, c1), BF16), vm((3, cy + 2, cz // 2, 2 * ax, c1), BF16),
        vm((cy, cz, ax, fo), BF16), vm((gxn, cy + 2, cz + 2, ax, fo), BF16),
        vm((3, cy + 2, cz // 2 + 1, 2 * ax, c2), BF16), vm((3, cy + 2, cz // 2, 2 * ax, c2), BF16),
        vm((gxn, cy, cz // 2, 2 * (cx + 2), fo), BF16), vm((gxn, cy + 2, cz // 2 + 2, 2 * (cx + 2), fo), BF16),
        vm((3, cy + 2, hx // 2, 2 * hz, 3 * c2), BF16),
        vm((2, hx * hy * hz, c1), F32), vm((2, cy * cz * ax, 3 * fo), F32), vm((2, cz * ax, fo), F32),
        vm((2, cy * hx * hz, c1), F32), vm((2, (cy + 1) * hx * hz, c1), F32),
    ]
    scratch += [dma((3,))] * 6 + [dma((4,))] * 6
    return pl.pallas_call(
        functools.partial(kernel, dims),
        out_shape=jax.ShapeDtypeStruct((hx, hy, hz, c1), BF16),
        in_specs=[pl.BlockSpec(memory_space=pltpu.HBM)] * 6,
        out_specs=pl.BlockSpec(memory_space=pltpu.VMEM),
        scratch_shapes=scratch,
        compiler_params=pltpu.CompilerParams(
            collective_id=0, has_side_effects=True, vmem_limit_bytes=52 * 1024 * 1024
        ),
    )(*[pltpu.with_memory_space_constraint(a, pltpu.HBM) for a in (volume, *weights)])


def solution(mesh):
    dims = (mesh.shape["gx"], mesh.shape["gy"])
    assert mesh.shape["gz"] == 2 and mesh.shape["gy"] % 2 == 0
    return jax.shard_map(
        functools.partial(on_device, dims),
        mesh=mesh,
        in_specs=(
            P("gx", "gy", "gz", None),
            P(),
            P(),
            P(None, None, None, None, "gx"),
            P(None, None, None, None, "gx"),
            P(),
        ),
        out_specs=P("gx", "gy", "gz", None),
        check_vma=False,
    )
```

```python
import functools

import jax
import jax.numpy as jnp
from jax import lax
from jax.experimental import pallas as pl
from jax.experimental.pallas import tpu as pltpu
from jax.sharding import PartitionSpec as P

F32 = jnp.float32
BF16 = jnp.bfloat16
STEPS = [(dx, dy) for dx in (-1, 0, 1) for dy in (-1, 0, 1)]


def span(d, n, pad):
    if d == 0:
        return pl.ds(pad, n), pl.ds(1, n)
    if d < 0:
        return pl.ds(pad, 1), pl.ds(n + 1, 1)
    return pl.ds(pad + n - 1, 1), pl.ds(0, 1)


def halves(pairs, refs):
    for i, ref in enumerate(refs):
        total = None
        for lhs, rhs in pairs[i::2]:
            part = jnp.dot(lhs, rhs, preferred_element_type=F32)
            total = part if total is None else total + part
        ref[...] = total


def kernel(
    dims,
    v_h, wf_h, wh_h, w1_h, w2_h, wu_h,
    out,
    wh, w1, w2, wus, wuu, wsem, vsem, fsem, wt, wz,
    p1, f1, g1, gs, e1, a1, rz, t1,
    p2, f2, g2, e2, o2,
    p3, f3, g3, e3, o3, acc,
    pk2, l2, m2, sel2, selm, q2, b2, pk3, l3, q3, b3, pk4, l4, up, sums, deeps, brims, thirds, ends,
    s1, r1, s2, r2, s3, r3, s4, r4, s5, r5, s6, r6,
):
    gxn, gyn = dims
    gx, gy, gz = lax.axis_index("gx"), lax.axis_index("gy"), lax.axis_index("gz")
    oz = 1 - gz

    nx, ny, nz, c0 = v_h.shape
    fetch = pltpu.make_async_copy(v_h, p1.at[1 : nx + 1, 1 : ny + 1], vsem)
    fetch.start()
    c2 = w2.shape[1]
    loads = [
        pltpu.make_async_copy(src, dst, wsem.at[i])
        for i, (src, dst) in enumerate((
            (wh_h, wh), (w1_h, w1), (w2_h, w2), (wu_h.at[:, c2:], wus), (wu_h.at[:, :c2], wuu),
        ))
    ]

    def on(cond, fn):
        if cond is True:
            fn()
        else:
            pl.when(cond)(fn)

    def exists(dx, dy):
        conds = []
        if dx < 0:
            conds.append(gx > 0)
        if dx > 0:
            conds.append(gx < gxn - 1)
        if dy < 0:
            conds.append(gy > 0)
        if dy > 0:
            conds.append(gy < gyn - 1)
        if not conds:
            return True
        return functools.reduce(jnp.logical_and, conds)

    for x in (0, nx + 1):
        p1[x] = jnp.zeros(p1.shape[1:], BF16)
    for y in (0, ny + 1):
        p1[1 : nx + 1, y] = jnp.zeros((nx, nz, c0), BF16)
    m2[...] = jnp.zeros_like(m2)
    for x in (0, nx + 1):
        g1[x] = jnp.zeros(g1.shape[1:], F32)
    for y in (0, ny + 1):
        g1[:, y] = jnp.zeros((nx + 2, 1, c0), F32)

    barrier = pltpu.get_barrier_semaphore()
    for s in range(gxn):
        there = lax.rem(gx + s, gxn)
        for dy in (-1, 0, 1):
            for z in (0, 1):
                if s == 0 and dy == 0 and z == 0:
                    continue

                def signal(there=there, dy=dy, z=z):
                    pl.semaphore_signal(
                        barrier, inc=1,
                        device_id={"gx": there, "gy": gy + dy, "gz": oz if z else gz},
                        device_id_type=pl.DeviceIdType.MESH,
                    )

                on(exists(0, dy), signal)
    k0 = 3 * c0
    for oy in range(3):
        for first, lane in ((0, 0), (1, c0)):
            dst = wt.at[oy, first : first + 3, :, lane : lane + c0]
            pltpu.make_async_copy(wf_h.at[:, oy], dst, fsem).start()
    lines = 1 + (gy > 0).astype(jnp.int32) + (gy < gyn - 1).astype(jnp.int32)

    def edge(block):
        size = block.shape[-2]
        return jnp.where(oz == 0, block[..., 0:1, :], block[..., size - 1 : size, :])

    for ref in (g2, g3):
        ref[...] = jnp.zeros(ref.shape, ref.dtype)
    for ref in (p2, p3):
        for x in (0, ref.shape[0] - 1):
            ref[x] = jnp.zeros(ref.shape[1:], BF16)
        for y in (0, ref.shape[1] - 1):
            ref[:, y] = jnp.zeros(ref.shape[:1] + ref.shape[2:], BF16)
    for x in (0, nx + 1):
        e1[x] = jnp.zeros(e1.shape[1:], BF16)
    for y in (0, ny + 1):
        e1[1 : nx + 1, y] = jnp.zeros((nx, nz, k0), BF16)
    for oy in range(3):
        wt[oy, 3, :, :c0] = jnp.zeros((k0, c0), BF16)
        wt[oy, 0, :, c0:] = jnp.zeros((k0, c0), BF16)
    fetch.wait()
    for load in loads:
        load.start()
    for x in range(nx):
        f1[x] = edge(p1[x + 1, 1 : ny + 1].astype(F32))
    pl.semaphore_wait(barrier, 2 * gxn * lines - 1)

    def send(src, dst, ss, rs, x, y, z):
        return pltpu.make_async_remote_copy(
            src_ref=src, dst_ref=dst, send_sem=ss, recv_sem=rs,
            device_id={"gx": x, "gy": y, "gz": z}, device_id_type=pl.DeviceIdType.MESH,
        )

    many_x = jnp.logical_and(gx > 0, gx < gxn - 1)
    many_y = jnp.logical_and(gy > 0, gy < gyn - 1)

    def by_y(fn):
        for b in (1, 2):
            pl.when(many_y if b == 2 else jnp.logical_not(many_y))(functools.partial(fn, b))

    def by_xy(fn):
        for a in (1, 2):
            for b in (1, 2):
                cx_ = many_x if a == 2 else jnp.logical_not(many_x)
                cy_ = many_y if b == 2 else jnp.logical_not(many_y)
                pl.when(jnp.logical_and(cx_, cy_))(functools.partial(fn, a, b))

    def drain(ref, sem):
        pltpu.make_async_copy(ref, ref, sem).wait()

    stage = pl.when(gx < gxn)
    short = jnp.minimum(gx, gxn - 1 - gx)
    farthest = []
    for i in range(gxn - 1, 0, -1):
        paired = gx + ((i + 1) // 2 if i % 2 else -(i // 2))
        rest = jnp.where(gx < gxn - 1 - gx, gx + (i - short), gx - (i - short))
        farthest.append(jnp.where(i <= 2 * short, paired, rest))

    late = []

    def neighbours(src, pad, face, rim, side, nx, ny, ss, rs):
        copies = []
        for dx, dy in STEPS:
            sx, tx = span(dx, nx, pad)
            sy, ty = span(dy, ny, pad)
            fx, _ = span(dx, nx, 0)
            fy, _ = span(dy, ny, 0)
            hops = abs(dx) + abs(dy)
            to = (gx + dx, gy + dy)
            copies.append((hops + 1, exists(dx, dy), send(face.at[fx, fy], side.at[tx, ty], ss.at[0], rs.at[0], *to, oz)))
            if hops:
                k = 1 if dx else 2
                copy = send(src.at[sx, sy], rim.at[tx, ty], ss.at[k], rs.at[k], *to, gz)
                copies.append((hops, exists(dx, dy), copy))
        for _, cond, copy in sorted(copies, key=lambda entry: -entry[0]):
            on(cond, copy.start)

        def finish(sems):
            def both(a, b):
                drain(side.at[0 : nx + a, 0 : ny + b], sems.at[0])
                drain(rim.at[0:a, 0 : ny + b], sems.at[1])
                drain(rim.at[0:nx, 0:b], sems.at[2])

            by_xy(both)

        late.append(lambda: finish(ss))
        return lambda: finish(rs)

    def shifted(block, fill):
        size = block.shape[-2]
        axis = block.ndim - 2
        rows = lax.broadcasted_iota(jnp.int32, block.shape, axis)
        below = jnp.where(rows == 0, 0.0, pltpu.roll(block, 1, axis))
        above = jnp.where(rows == size - 1, 0.0, pltpu.roll(block, size - 1, axis))
        if fill is not None:
            fill = jnp.broadcast_to(fill, block.shape)
            below = jnp.where(rows == jnp.where(gz == 1, 0, -1), fill, below)
            above = jnp.where(rows == jnp.where(gz == 0, size - 1, -1), fill, above)
        return below, above

    def rounded(x):
        return x.astype(BF16).astype(F32)

    arrived = neighbours(p1, 1, f1, p1, g1, nx, ny, s1, r1)

    def widen(at, block):
        block = block.astype(F32)
        below, above = shifted(block, None)
        for k, part in enumerate((below, block, above)):
            e1[at + (slice(None), pl.ds(k * c0, c0))] = part.astype(BF16)

    @pl.loop(1, nx + 1)
    def _(x):
        widen((x, pl.ds(1, ny)), p1[x, 1 : ny + 1])

    drain(wt.at[:, 0:3], fsem)

    group1 = 2 if nx % 4 == 0 else 1

    @pl.loop(0, nx // (2 * group1))
    def _(step):
        total = jnp.zeros((group1 * ny * nz, 2 * c0), F32)
        for oy in range(3):
            for half in range(2):
                lhs = []
                for i in range(2):
                    planes = [2 * (step * group1 + n) + 2 * half + i for n in range(group1)]
                    planes = [e1[x, oy : oy + ny].reshape(ny * nz, k0) for x in planes]
                    lhs.append(jnp.concatenate(planes, axis=0))
                rhs = wt[oy, 2 * half : 2 * half + 2].reshape(2 * k0, 2 * c0)
                total = total + jnp.dot(jnp.concatenate(lhs, axis=1), rhs, preferred_element_type=F32)
        for n in range(group1):
            a1[step * group1 + n] = total[n * ny * nz : (n + 1) * ny * nz]

    for ox in range(3):
        for oy in range(3):
            tap = wt[oy, ox, pl.ds(pl.multiple_of(2 * oz * c0, c0), c0), :c0]
            wz[(ox * 3 + oy) * c0 : (ox * 3 + oy + 1) * c0] = tap
    arrived()
    for x in range(nx + 2):
        for y in range(ny + 2):
            gs[x, y : y + 1] = g1[x, y]
    @stage
    def _():
        lhs = [gs[ox : ox + nx, oy : oy + ny].reshape(nx * ny, c0).astype(BF16) for ox in range(3) for oy in range(3)]
        rz[...] = jnp.dot(jnp.concatenate(lhs, axis=1), wz[...], preferred_element_type=F32)
        for x, ox, lane in ((0, 0, 0), (nx + 1, 2, c0)):
            widen((x, pl.ds(1, ny)), p1[x, 1 : ny + 1])
            lhs = [e1[x, oy : oy + ny].reshape(ny * nz, k0) for oy in range(3)]
            rhs = jnp.concatenate([wt[oy, ox, :, :c0] for oy in range(3)], axis=0)
            part = jnp.dot(jnp.concatenate(lhs, axis=1), rhs, preferred_element_type=F32)
            at = (0 if ox == 0 else nx // 2 - 1, slice(None), pl.ds(lane, c0))
            a1[at] = a1[at] + part
        for y, oy in ((0, 0), (ny + 1, 2)):
            widen((pl.ds(0, nx + 2), y), p1[:, y])
            lhs = [e1[ox : ox + nx, y].reshape(nx * nz, k0) for ox in range(3)]
            rhs = jnp.concatenate([wt[oy, ox, :, :c0] for ox in range(3)], axis=0)
            part = jnp.dot(jnp.concatenate(lhs, axis=1), rhs, preferred_element_type=F32).reshape(nx, nz, c0)
            for x in range(nx):
                at = (x // 2, pl.ds((0 if oy == 0 else ny - 1) * nz, nz), pl.ds(x % 2 * c0, c0))
                a1[at] = a1[at] + part[x]

    tile = 8
    last = lax.broadcasted_iota(jnp.int32, (tile, c0), 0) == (tile - 1) * oz
    for x in range(nx):
        for y in range(ny):
            at = (x // 2, pl.ds(pl.multiple_of(y * nz + (nz - tile) * oz, tile), tile), pl.ds(x % 2 * c0, c0))
            row = jnp.broadcast_to(rz[x * ny + y : x * ny + y + 1], (tile, c0))
            a1[at] = a1[at] + jnp.where(last, row, 0.0)

    hx, hy, hz = nx // 2, ny // 2, nz // 2

    @pl.loop(0, hx)
    def _(x):
        total = a1[x]
        both = jnp.maximum(jnp.maximum(total[:, :c0], total[:, c0:]), 0.0).reshape(hy, 2, nz, c0)
        t1[...] = jnp.max(both, axis=1)
        small = jnp.maximum(t1[:, pl.ds(0, hz, stride=2), :], t1[:, pl.ds(1, hz, stride=2), :])
        small = rounded(small)
        p2[x + 1, 1 : hy + 1] = small.astype(BF16)
        f2[x] = edge(small)

    arrived = neighbours(p2, 1, f2, p2, g2, hx, hy, s2, r2)
    for ref in (l3, l4):
        ref[...] = jnp.zeros(ref.shape, ref.dtype)
    arrived()
    rows = hx * hy * hz

    def pack(even, odd, at, block, lane):
        n, size, c = block.shape
        even[at, :, :, pl.ds(lane, c)] = block.reshape(n * size, c).astype(BF16).reshape(n // 2, 2 * size, c)
        block = block[1 : n - 1]
        odd[at, :, :, pl.ds(lane, c)] = block.reshape((n - 2) * size, c).astype(BF16).reshape(n // 2 - 1, 2 * size, c)

    def conv(even, odd, p, g, w):
        for x in range(hx + 2):
            block = p[x].astype(F32)
            c = block.shape[-1]
            below, above = shifted(block, g[x])
            for k, part in enumerate((below, block, above)):
                pack(even, odd, x, part, k * c)
        @stage
        def _():
            pairs = []
            for ox in range(3):
                for oy, (r, lo) in enumerate(((even, 0), (odd, 0), (even, 1))):
                    rhs = w[ox * 9 + oy * 3 : ox * 9 + oy * 3 + 3].reshape(3 * c, w.shape[2])
                    pairs.append((r[ox : ox + hx, lo : lo + hy // 2].reshape(rows, 3 * c), rhs))
            halves(pairs, (sums.at[0], sums.at[1]))

        return sums[0] + sums[1]

    loads[0].wait()
    c1 = wh.shape[2]
    total = conv(e2, o2, p2, g2, wh)
    skip = rounded(jnp.maximum(total, 0.0)).reshape(hx, hy, hz, c1)
    p3[1 : hx + 1, 1 : hy + 1] = skip.astype(BF16)

    cx, cy, cz = hx // 2, hy // 2, hz // 2
    ax = gxn * cx
    group = cz * cx
    m = jnp.max(skip.reshape(cx, 2, cy, 2, hz, c1), axis=(1, 3))
    m = m.reshape(cx * cy * hz, c1)
    m = jnp.maximum(m, pltpu.roll(m, m.shape[0] - 1, 0)).astype(BF16)

    blocks = []
    lane = lax.broadcasted_iota(jnp.int32, (group, cx * cy * hz), 1)
    sub = lax.broadcasted_iota(jnp.int32, (group, cx * cy * hz), 0)
    shift_x = cx.bit_length() - 1
    sub_x = sub & (cx - 1)
    sub_o = sub >> shift_x
    for y in range(cy):
        blocks.append(jnp.where(lane == (sub_x * cy + y) * hz + 2 * sub_o, 1.0, 0.0))
    blocks.append(jnp.where(lane == (sub_x * cy + sub_o) * hz + 2 * (cz - 1) * oz, 1.0, 0.0))
    pick = jnp.concatenate(blocks, axis=0).astype(BF16)
    packets = jnp.dot(pick, m, preferred_element_type=F32).reshape(cy + 1, group, c1).astype(BF16)
    pk2[...] = packets
    l2[gx, 0:cy] = packets[0:cy]

    def coarse_copy(k, dy, z):
        def make(src_gx, tgt_gx):
            if z == 0:
                src = {0: pl.ds(0, cy), -1: pl.ds(0, 1), 1: pl.ds(cy - 1, 1)}[dy]
            else:
                src = pl.ds(cy, 1)
            if dy == 0:
                dst = l2.at[src_gx, pl.ds(cy, 1) if z else pl.ds(0, cy)]
            else:
                dst = m2.at[src_gx, pl.ds(2 * z + (1 if dy < 0 else 0), 1)]
            return send(pk2.at[src], dst, s4.at[k], r4.at[k], tgt_gx, gy + dy, oz if z else gz)

        return make

    def deep_copy(pk, land, ss, rs):
        def choose(k, dy, z):
            def make(src_gx, tgt_gx):
                sy, ty = span(dy, cy, 0)
                sender = gz if src_gx is gx else (oz if z else gz)
                if z == 0:
                    src = pk.at[sy]
                    dst = land.at[src_gx, ty, pl.ds(1, cz)]
                else:
                    src = pk.at[sy, pl.ds((cz - 1) * (1 - sender), 1)]
                    dst = land.at[src_gx, ty, pl.ds((cz + 1) * sender, 1)]
                return send(src, dst, ss.at[k], rs.at[k], tgt_gx, gy + dy, oz if z else gz)

            return make

        return choose

    def narrow_copy(k, dy, z):
        def make(src_gx, tgt_gx):
            sy, ty = span(dy, cy, 0)
            sender = gz if src_gx is gx else (oz if z else gz)
            if z == 0:
                src = pk4.at[tgt_gx, sy]
                dst = l4.at[src_gx, ty, pl.ds(1, cz // 2)]
            else:
                src = pk4.at[tgt_gx, sy, pl.ds((cz // 2 - 1) * (1 - sender), 1)]
                dst = l4.at[src_gx, ty, pl.ds((cz // 2 + 1) * sender, 1)]
            return send(src, dst, s6.at[k], r6.at[k], tgt_gx, gy + dy, oz if z else gz)

        return make

    upper = lax.rem(gy, 2) == 1
    lower = lax.rem(gy, 2) == 0
    across = {-1: jnp.logical_and(lower, gy > 0), 1: jnp.logical_and(upper, gy < gyn - 1)}
    within = {-1: upper, 1: lower}

    def column_exchange(choose, main, rim, relay, carry, ss, rs):
        order = [(there, 0, z, 0) for z in (1, 0) for there in farthest]
        order += [(gx, 0, 1, 1)]
        for there, dy, z, k in order:
            choose(k, dy, z)(gx, there).start()
        for there in farthest + [gx]:
            for z in (1, 0):
                for dy in (-1, 1):
                    on(across[dy], choose(2, dy, z)(gx, there).start)

        def own(which):
            for k, ref in enumerate(main):
                drain(ref, which.at[k])

        def edges(which):
            for dy in (-1, 1):
                on(across[dy], lambda: drain(rim, which.at[2]))
            drain(relay, which.at[3])

        def arrive():
            own(rs)
            for dy in (-1, 1):
                for src, dst in carry(dy):
                    on(within[dy], send(src, dst, ss.at[3], rs.at[3], gx, gy + dy, gz).start)

        def finish():
            own(ss)
            edges(ss)

        late.append(finish)
        return arrive, lambda: edges(rs)

    def parts_of(land):
        wz = land.shape[2] - 2

        def carry(dy):
            rows = (cy, 0) if dy > 0 else (1, cy + 1)
            return [tuple(land.at[:, row] for row in rows)]

        main = (land.at[0 : gxn - 1, 0:cy, 0 : wz + 1], land.at[0, 0:cy, 0:1])
        return main, land.at[0:gxn, 0:1, 0 : wz + 1], land.at[:, 0], carry

    def carry_lines(dy):
        pairs = ((cy - 1, 0), (cy, 2)) if dy > 0 else ((0, 1), (cy, 3))
        return [(l2.at[:, line], m2.at[:, slot]) for line, slot in pairs]

    main4, rim4 = column_exchange(
        coarse_copy, (l2.at[0 : gxn - 1], l2.at[0, 0:1]), m2.at[:, 0:2], m2.at[:, 0:2], carry_lines, s4, r4
    )
    for x in range(hx):
        f3[x] = edge(p3[x + 1, 1 : hy + 1].astype(F32))

    def one_hot(ref, at, slots):
        width = gxn * slots * group
        lane = lax.broadcasted_iota(jnp.int32, (ax, width), 1)
        xs = lax.broadcasted_iota(jnp.int32, (ax, width), 0)
        base = lane - ((xs >> shift_x) * slots * group + (xs & (cx - 1)))
        ref[at] = jnp.where(base == slots_at, 1.0, 0.0)

    for y in range(-1, cy + 1):
        for z in range(-1, cz + 1):
            inside = 0 <= y < cy
            rim_slot = 0 if y < 0 else 1
            if 0 <= z < cz:
                slots_at = (y if inside else rim_slot) * group + z * cx
            else:
                line = y if inside else (cy - 1 if y < 0 else 0)
                mine = (gz == 1) if z < 0 else (gz == 0)
                slots_at = jnp.where(mine, (cy if inside else 2 + rim_slot) * group + line * cx, -(1 << 20))
            if inside:
                one_hot(sel2, (y, z + 1), cy + 1)
            else:
                one_hot(selm, (rim_slot, z + 1), 4)

    def gathered(ref, land):
        n, width = ref.shape[0], ref.shape[-1]
        select = ref[...].reshape(n * (cz + 2) * ax, width).astype(BF16)
        landed = land[...].astype(F32).reshape(width, c1).astype(BF16)
        return jnp.dot(select, landed, preferred_element_type=F32).reshape(n, cz + 2, ax, c1)

    deep = cy * cz * ax
    fo = w1.shape[2]

    windows = ((0, 0), (1, 0), (0, 1))

    def spread(even, odd, block, row):
        below, above = shifted(block, None)
        n, c = block.shape[0], block.shape[-1]
        for ox, part in enumerate((below, block, above)):
            whole = part.reshape(n * (cz + 2) * ax, c).astype(BF16)
            even[ox, row : row + n] = whole.reshape(n, cz // 2 + 1, 2 * ax, c)
            inner = part[:, 1 : cz + 1].reshape(n * cz * ax, c).astype(BF16)
            odd[ox, row : row + n] = inner.reshape(n, cz // 2, 2 * ax, c)

    def window(pair, ox, row, n):
        c = pair[0].shape[-1]
        lhs = [pair[i][ox, row : row + n, lo : lo + cz // 2].reshape(n * cz * ax, c) for i, lo in windows]
        return jnp.concatenate(lhs, axis=1)

    def bottom_own(pair, w):
        @stage
        def _():
            k = 3 * w.shape[1]
            pairs = []
            for ox in range(3):
                lhs = window(pair, ox, 1, cy)
                rhs = [w[ox * 9 + oy * 3 : ox * 9 + oy * 3 + 3].reshape(k, fo) for oy in range(3)]
                rhs = jnp.concatenate(rhs, axis=1)
                pairs += [(lhs[:, : k // 2], rhs[: k // 2]), (lhs[:, k // 2 :], rhs[k // 2 :])]
            halves(pairs, (deeps.at[0], deeps.at[1]))

    def bottom_rim(pair, w):
        k = 3 * w.shape[1]
        size = cz * ax
        @stage
        def _():
            for side, (row, oy) in enumerate(((0, 0), (cy + 1, 2))):
                total = jnp.zeros((size, fo), F32)
                for ox in range(3):
                    rhs = w[(ox * 3 + oy) * 3 : (ox * 3 + oy) * 3 + 3].reshape(k, fo)
                    total = total + jnp.dot(window(pair, ox, row, 1), rhs, preferred_element_type=F32)
                brims[side] = total

        def own(oy, y):
            at = (pl.ds(y * size, size), pl.ds(oy * fo, fo))
            return deeps[(0, *at)] + deeps[(1, *at)]

        lines = []
        for y in range(cy):
            before = own(0, y - 1) if y > 0 else brims[0]
            after = own(2, y + 1) if y < cy - 1 else brims[1]
            lines.append(own(1, y) + before + after)
        return jnp.maximum(jnp.concatenate(lines, axis=0), 0.0).reshape(cy, cz, ax, fo).astype(BF16)

    main4()
    spread(q2, b2, gathered(sel2, l2), 1)
    loads[1].wait()
    bottom_own((q2, b2), w1)
    rim4()
    block = gathered(selm, m2)
    spread(q2, b2, block[0:1], 0)
    spread(q2, b2, block[1:2], cy + 1)
    first = bottom_rim((q2, b2), w1)
    pk3[...] = first
    l3[gx, 1 : cy + 1, 1 : cz + 1] = first
    main5, rim5 = column_exchange(deep_copy(pk3, l3, s5, r5), *parts_of(l3), s5, r5)

    skip_arrived = neighbours(p3, 1, f3, p3, g3, hx, hy, s3, r3)
    near = cx + 2
    wide = gxn * cz * near
    lane = lax.broadcasted_iota(jnp.int32, (wide, cz * ax), 1)
    row = lax.broadcasted_iota(jnp.int32, (wide, cz * ax), 0)
    shift_n = near.bit_length() - 1
    shift_z = cz.bit_length() - 1
    at = (row >> (shift_n + shift_z)) * cx + (row & (near - 1)) - 1
    at = jnp.where(jnp.logical_and(at >= 0, at < ax), at, -(cz + 1) * ax)
    share = jnp.where(lane == ((row >> shift_n) & (cz - 1)) * ax + at, 1.0, 0.0).astype(BF16)

    lane = lax.broadcasted_iota(jnp.int32, (hz, (cz + 4) * near), 1)
    zs = lax.broadcasted_iota(jnp.int32, (hz, (cz + 4) * near), 0)
    blocks = []
    for k in range(3):
        for x in range(-1, hx + 1):
            blocks.append(jnp.where(lane == (((zs + (k - 1)) >> 1) + 2) * near + (x >> 1) + 1, 1.0, 0.0))
    for k in range(3):
        blocks += blocks[k * (hx + 2) + 1 : (k + 1) * (hx + 2) - 1]
    pick = jnp.concatenate(blocks, axis=0).astype(BF16)

    def joined(row, n):
        return jnp.concatenate([l3[g, row : row + n].astype(F32) for g in range(gxn)], axis=-1)

    main5()
    spread(q3, b3, joined(1, cy), 1)
    loads[2].wait()
    bottom_own((q3, b3), w2)
    rim5()
    spread(q3, b3, joined(0, 1), 0)
    spread(q3, b3, joined(cy + 1, 1), cy + 1)
    second = bottom_rim((q3, b3), w2)
    for y in range(cy):
        line = second[y].astype(F32).reshape(cz * ax, fo).astype(BF16)
        line = jnp.dot(share, line, preferred_element_type=F32)
        pk4[:, y] = line.reshape(gxn, cz // 2, 2 * near, fo).astype(BF16)
    l4[gx, 1 : cy + 1, 1 : cz // 2 + 1] = pk4[gx]
    main6, rim6 = column_exchange(narrow_copy, *parts_of(l4), s6, r6)
    size = hx * hz

    def enlarge(ys):
        fields = [l4[g, y].astype(F32).reshape((cz + 4) * near, fo) for y in ys for g in range(gxn)]
        fields = jnp.concatenate(fields, axis=-1).astype(BF16)
        fields = jnp.dot(pick, fields, preferred_element_type=F32).astype(BF16)
        for i, y in enumerate(ys):
            field = fields[:, i * c2 : (i + 1) * c2]
            for k in range(3):
                at = pl.ds(k * c2, c2)
                part = field[k * (size + 2 * hz) : (k + 1) * (size + 2 * hz)]
                up[0, y, :, :, at] = part[:size].reshape(hx // 2, 2 * hz, c2)
                up[2, y, :, :, at] = part[2 * hz :].reshape(hx // 2, 2 * hz, c2)
                part = field[3 * (size + 2 * hz) + k * size : 3 * (size + 2 * hz) + (k + 1) * size]
                up[1, y, :, :, at] = part.reshape(hx // 2, 2 * hz, c2)

    skip_arrived()
    loads[3].wait()
    total = conv(e3, o3, p3, g3, wus)
    acc[...] = total.reshape(hx, hy, hz, c1)

    main6()
    enlarge(range(1, cy + 1))
    loads[4].wait()

    @stage
    def _():
        pairs = []
        for ox in range(3):
            for k in range(3):
                lhs = up[ox, 1 : cy + 1, :, :, pl.ds(k * c2, c2)].reshape(cy * size, c2)
                pairs.append((lhs, wuu[ox * 9 + 3 + k]))
        halves(pairs, (thirds.at[0], thirds.at[1]))

    rim6()
    enlarge((0, cy + 1))

    @stage
    def _():
        for side, oy in enumerate((0, 2)):
            total = jnp.zeros(((cy + 1) * size, c1), F32)
            for ox in range(3):
                lhs = up[ox, side : side + cy + 1].reshape((cy + 1) * size, 3 * c2)
                rhs = wuu[(ox * 3 + oy) * 3 : (ox * 3 + oy) * 3 + 3].reshape(3 * c2, c1)
                total = total + jnp.dot(lhs, rhs, preferred_element_type=F32)
            ends[side] = total

    for y in range(hy):
        low, mid, high = (y + 1) // 2, (y + 2) // 2 - 1, (y + 3) // 2 - 1
        total = ends[0, low * size : (low + 1) * size] + ends[1, high * size : (high + 1) * size]
        total = total + thirds[0, mid * size : (mid + 1) * size] + thirds[1, mid * size : (mid + 1) * size]
        out[:, y] = (acc[:, y] + total.reshape(hx, hz, c1)).astype(BF16)

    for fn in late:
        fn()


def on_device(dims, volume, w_full, w_half, w_bottom_in, w_bottom_out, w_up):
    gxn, gyn = dims
    nx, ny, nz, c0 = volume.shape
    c1 = w_half.shape[4]
    c2, fo = w_bottom_out.shape[3:]
    hx, hy, hz = nx // 2, ny // 2, nz // 2
    cx, cy, cz = hx // 2, hy // 2, hz // 2
    ax = gxn * cx
    weights = [
        w_full.reshape(3, 3, 3 * c0, c0),
        w_half.reshape(27, c0, c1),
        w_bottom_in.reshape(27, c1, fo),
        w_bottom_out.reshape(27, c2, fo),
        w_up.reshape(27, c2 + c1, c1),
    ]
    vm = pltpu.VMEM
    dma = pltpu.SemaphoreType.DMA
    scratch = [vm(w.shape, BF16) for w in weights[1:4]]
    scratch += [vm((27, c1, c1), BF16), vm((27, c2, c1), BF16), dma((5,)), dma(()), dma(())]
    scratch += [vm((3, 4, 3 * c0, 2 * c0), BF16), vm((9 * c0, c0), BF16)]
    scratch += [
        vm((nx + 2, ny + 2, nz, c0), BF16), vm((nx, ny, 1, c0), F32), vm((nx + 2, ny + 2, 1, c0), F32),
        vm((nx + 2, ny + 2, c0), F32), vm((nx + 2, ny + 2, nz, 3 * c0), BF16), vm((hx, ny * nz, 2 * c0), F32),
        vm((nx * ny, c0), F32), vm((hy, nz, c0), F32),
        vm((hx + 2, hy + 2, hz, c0), BF16), vm((hx, hy, 1, c0), F32), vm((hx + 2, hy + 2, 1, c0), F32),
        vm((hx + 2, hy // 2 + 1, 2 * hz, 3 * c0), BF16), vm((hx + 2, hy // 2, 2 * hz, 3 * c0), BF16),
        vm((hx + 2, hy + 2, hz, c1), BF16), vm((hx, hy, 1, c1), F32), vm((hx + 2, hy + 2, 1, c1), F32),
        vm((hx + 2, hy // 2 + 1, 2 * hz, 3 * c1), BF16), vm((hx + 2, hy // 2, 2 * hz, 3 * c1), BF16),
        vm((hx, hy, hz, c1), F32),
        vm((cy + 1, cz * cx, c1), BF16), vm((gxn, cy + 1, cz * cx, c1), BF16), vm((gxn, 4, cz * cx, c1), BF16),
        vm((cy, cz + 2, ax, gxn * (cy + 1) * cz * cx), F32), vm((2, cz + 2, ax, gxn * 4 * cz * cx), F32),
        vm((3, cy + 2, cz // 2 + 1, 2 * ax, c1), BF16), vm((3, cy + 2, cz // 2, 2 * ax, c1), BF16),
        vm((cy, cz, ax, fo), BF16), vm((gxn, cy + 2, cz + 2, ax, fo), BF16),
        vm((3, cy + 2, cz // 2 + 1, 2 * ax, c2), BF16), vm((3, cy + 2, cz // 2, 2 * ax, c2), BF16),
        vm((gxn, cy, cz // 2, 2 * (cx + 2), fo), BF16), vm((gxn, cy + 2, cz // 2 + 2, 2 * (cx + 2), fo), BF16),
        vm((3, cy + 2, hx // 2, 2 * hz, 3 * c2), BF16),
        vm((2, hx * hy * hz, c1), F32), vm((2, cy * cz * ax, 3 * fo), F32), vm((2, cz * ax, fo), F32),
        vm((2, cy * hx * hz, c1), F32), vm((2, (cy + 1) * hx * hz, c1), F32),
    ]
    scratch += [dma((3,))] * 6 + [dma((4,))] * 6
    return pl.pallas_call(
        functools.partial(kernel, dims),
        out_shape=jax.ShapeDtypeStruct((hx, hy, hz, c1), BF16),
        in_specs=[pl.BlockSpec(memory_space=pltpu.HBM)] * 6,
        out_specs=pl.BlockSpec(memory_space=pltpu.VMEM),
        scratch_shapes=scratch,
        compiler_params=pltpu.CompilerParams(
            collective_id=0, has_side_effects=True, vmem_limit_bytes=52 * 1024 * 1024
        ),
    )(*[pltpu.with_memory_space_constraint(a, pltpu.HBM) for a in (volume, *weights)])


def solution(mesh):
    dims = (mesh.shape["gx"], mesh.shape["gy"])
    assert mesh.shape["gz"] == 2 and mesh.shape["gy"] % 2 == 0
    return jax.shard_map(
        functools.partial(on_device, dims),
        mesh=mesh,
        in_specs=(
            P("gx", "gy", "gz", None),
            P(),
            P(),
            P(None, None, None, None, "gx"),
            P(None, None, None, None, "gx"),
            P(),
        ),
        out_specs=P("gx", "gy", "gz", None),
        check_vma=False,
    )
```

```python
import functools

import jax
import jax.numpy as jnp
from jax import lax
from jax.experimental import pallas as pl
from jax.experimental.pallas import tpu as pltpu
from jax.sharding import PartitionSpec as P

F32 = jnp.float32
BF16 = jnp.bfloat16
STEPS = [(dx, dy) for dx in (-1, 0, 1) for dy in (-1, 0, 1)]


def span(d, n, pad):
    if d == 0:
        return pl.ds(pad, n), pl.ds(1, n)
    if d < 0:
        return pl.ds(pad, 1), pl.ds(n + 1, 1)
    return pl.ds(pad + n - 1, 1), pl.ds(0, 1)


def halves(pairs, refs):
    for i, ref in enumerate(refs):
        total = None
        for lhs, rhs in pairs[i::2]:
            part = jnp.dot(lhs, rhs, preferred_element_type=F32)
            total = part if total is None else total + part
        ref[...] = total


def kernel(
    dims,
    v_h, wf_h, wh_h, w1_h, w2_h, wu_h,
    out,
    wh, w1, w2, wus, wuu, wsem, vsem, fsem, wt, wz,
    p1, f1, g1, gs, e1, a1, rz, t1,
    p2, f2, g2, e2, o2,
    p3, f3, g3, e3, o3, acc,
    pk2, l2, m2, sel2, selm, pick2, pickm, q2, b2, pk3, l3, q3, b3, pk4, l4, up, sums, deeps, brims, thirds, ends,
    s1, r1, s2, r2, s3, r3, s4, r4, s5, r5, s6, r6,
):
    gxn, gyn = dims
    gx, gy, gz = lax.axis_index("gx"), lax.axis_index("gy"), lax.axis_index("gz")
    oz = 1 - gz

    nx, ny, nz, c0 = v_h.shape
    fetch = pltpu.make_async_copy(v_h, p1.at[1 : nx + 1, 1 : ny + 1], vsem)
    fetch.start()
    c2 = w2.shape[1]
    loads = [
        pltpu.make_async_copy(src, dst, wsem.at[i])
        for i, (src, dst) in enumerate((
            (wh_h, wh), (w1_h, w1), (w2_h, w2), (wu_h.at[:, c2:], wus), (wu_h.at[:, :c2], wuu),
        ))
    ]

    def on(cond, fn):
        if cond is True:
            fn()
        else:
            pl.when(cond)(fn)

    def exists(dx, dy):
        conds = []
        if dx < 0:
            conds.append(gx > 0)
        if dx > 0:
            conds.append(gx < gxn - 1)
        if dy < 0:
            conds.append(gy > 0)
        if dy > 0:
            conds.append(gy < gyn - 1)
        if not conds:
            return True
        return functools.reduce(jnp.logical_and, conds)

    for x in (0, nx + 1):
        p1[x] = jnp.zeros(p1.shape[1:], BF16)
    for y in (0, ny + 1):
        p1[1 : nx + 1, y] = jnp.zeros((nx, nz, c0), BF16)
    m2[...] = jnp.zeros_like(m2)
    for x in (0, nx + 1):
        g1[x] = jnp.zeros(g1.shape[1:], F32)
    for y in (0, ny + 1):
        g1[:, y] = jnp.zeros((nx + 2, 1, c0), F32)

    barrier = pltpu.get_barrier_semaphore()
    for s in range(gxn):
        there = lax.rem(gx + s, gxn)
        for dy in (-1, 0, 1):
            for z in (0, 1):
                if s == 0 and dy == 0 and z == 0:
                    continue

                def signal(there=there, dy=dy, z=z):
                    pl.semaphore_signal(
                        barrier, inc=1,
                        device_id={"gx": there, "gy": gy + dy, "gz": oz if z else gz},
                        device_id_type=pl.DeviceIdType.MESH,
                    )

                on(exists(0, dy), signal)
    k0 = 3 * c0
    for oy in range(3):
        for first, lane in ((0, 0), (1, c0)):
            dst = wt.at[oy, first : first + 3, :, lane : lane + c0]
            pltpu.make_async_copy(wf_h.at[:, oy], dst, fsem).start()
    lines = 1 + (gy > 0).astype(jnp.int32) + (gy < gyn - 1).astype(jnp.int32)

    def edge(block):
        size = block.shape[-2]
        return jnp.where(oz == 0, block[..., 0:1, :], block[..., size - 1 : size, :])

    for ref in (g2, g3):
        ref[...] = jnp.zeros(ref.shape, ref.dtype)
    for ref in (p2, p3):
        for x in (0, ref.shape[0] - 1):
            ref[x] = jnp.zeros(ref.shape[1:], BF16)
        for y in (0, ref.shape[1] - 1):
            ref[:, y] = jnp.zeros(ref.shape[:1] + ref.shape[2:], BF16)
    for x in (0, nx + 1):
        e1[x] = jnp.zeros(e1.shape[1:], BF16)
    for y in (0, ny + 1):
        e1[1 : nx + 1, y] = jnp.zeros((nx, nz, k0), BF16)
    for oy in range(3):
        wt[oy, 3, :, :c0] = jnp.zeros((k0, c0), BF16)
        wt[oy, 0, :, c0:] = jnp.zeros((k0, c0), BF16)
    fetch.wait()
    for load in loads:
        load.start()
    for x in range(nx):
        f1[x] = edge(p1[x + 1, 1 : ny + 1].astype(F32))
    pl.semaphore_wait(barrier, 2 * gxn * lines - 1)

    def send(src, dst, ss, rs, x, y, z):
        return pltpu.make_async_remote_copy(
            src_ref=src, dst_ref=dst, send_sem=ss, recv_sem=rs,
            device_id={"gx": x, "gy": y, "gz": z}, device_id_type=pl.DeviceIdType.MESH,
        )

    many_x = jnp.logical_and(gx > 0, gx < gxn - 1)
    many_y = jnp.logical_and(gy > 0, gy < gyn - 1)

    def by_y(fn):
        for b in (1, 2):
            pl.when(many_y if b == 2 else jnp.logical_not(many_y))(functools.partial(fn, b))

    def by_xy(fn):
        for a in (1, 2):
            for b in (1, 2):
                cx_ = many_x if a == 2 else jnp.logical_not(many_x)
                cy_ = many_y if b == 2 else jnp.logical_not(many_y)
                pl.when(jnp.logical_and(cx_, cy_))(functools.partial(fn, a, b))

    def drain(ref, sem):
        pltpu.make_async_copy(ref, ref, sem).wait()

    stage = pl.when(gx < gxn)
    short = jnp.minimum(gx, gxn - 1 - gx)
    farthest = []
    for i in range(gxn - 1, 0, -1):
        paired = gx + ((i + 1) // 2 if i % 2 else -(i // 2))
        rest = jnp.where(gx < gxn - 1 - gx, gx + (i - short), gx - (i - short))
        farthest.append(jnp.where(i <= 2 * short, paired, rest))

    late = []

    def neighbours(src, pad, face, rim, side, nx, ny, ss, rs):
        copies = []
        for dx, dy in STEPS:
            sx, tx = span(dx, nx, pad)
            sy, ty = span(dy, ny, pad)
            fx, _ = span(dx, nx, 0)
            fy, _ = span(dy, ny, 0)
            hops = abs(dx) + abs(dy)
            to = (gx + dx, gy + dy)
            copies.append((hops + 1, exists(dx, dy), send(face.at[fx, fy], side.at[tx, ty], ss.at[0], rs.at[0], *to, oz)))
            if hops:
                k = 1 if dx else 2
                copy = send(src.at[sx, sy], rim.at[tx, ty], ss.at[k], rs.at[k], *to, gz)
                copies.append((hops, exists(dx, dy), copy))
        for _, cond, copy in sorted(copies, key=lambda entry: -entry[0]):
            on(cond, copy.start)

        def finish(sems):
            def both(a, b):
                drain(side.at[0 : nx + a, 0 : ny + b], sems.at[0])
                drain(rim.at[0:a, 0 : ny + b], sems.at[1])
                drain(rim.at[0:nx, 0:b], sems.at[2])

            by_xy(both)

        late.append(lambda: finish(ss))
        return lambda: finish(rs)

    def shifted(block, fill):
        size = block.shape[-2]
        axis = block.ndim - 2
        rows = lax.broadcasted_iota(jnp.int32, block.shape, axis)
        below = jnp.where(rows == 0, 0.0, pltpu.roll(block, 1, axis))
        above = jnp.where(rows == size - 1, 0.0, pltpu.roll(block, size - 1, axis))
        if fill is not None:
            fill = jnp.broadcast_to(fill, block.shape)
            below = jnp.where(rows == jnp.where(gz == 1, 0, -1), fill, below)
            above = jnp.where(rows == jnp.where(gz == 0, size - 1, -1), fill, above)
        return below, above

    def rounded(x):
        return x.astype(BF16).astype(F32)

    arrived = neighbours(p1, 1, f1, p1, g1, nx, ny, s1, r1)

    def widen(at, block):
        block = block.astype(F32)
        below, above = shifted(block, None)
        for k, part in enumerate((below, block, above)):
            e1[at + (slice(None), pl.ds(k * c0, c0))] = part.astype(BF16)

    @pl.loop(1, nx + 1)
    def _(x):
        widen((x, pl.ds(1, ny)), p1[x, 1 : ny + 1])

    drain(wt.at[:, 0:3], fsem)

    group1 = 2 if nx % 4 == 0 else 1

    @pl.loop(0, nx // (2 * group1))
    def _(step):
        total = jnp.zeros((group1 * ny * nz, 2 * c0), F32)
        for oy in range(3):
            for half in range(2):
                lhs = []
                for i in range(2):
                    planes = [2 * (step * group1 + n) + 2 * half + i for n in range(group1)]
                    planes = [e1[x, oy : oy + ny].reshape(ny * nz, k0) for x in planes]
                    lhs.append(jnp.concatenate(planes, axis=0))
                rhs = wt[oy, 2 * half : 2 * half + 2].reshape(2 * k0, 2 * c0)
                total = total + jnp.dot(jnp.concatenate(lhs, axis=1), rhs, preferred_element_type=F32)
        for n in range(group1):
            a1[step * group1 + n] = total[n * ny * nz : (n + 1) * ny * nz]

    for ox in range(3):
        for oy in range(3):
            tap = wt[oy, ox, pl.ds(pl.multiple_of(2 * oz * c0, c0), c0), :c0]
            wz[(ox * 3 + oy) * c0 : (ox * 3 + oy + 1) * c0] = tap
    arrived()
    for x in range(nx + 2):
        for y in range(ny + 2):
            gs[x, y : y + 1] = g1[x, y]
    @stage
    def _():
        lhs = [gs[ox : ox + nx, oy : oy + ny].reshape(nx * ny, c0).astype(BF16) for ox in range(3) for oy in range(3)]
        rz[...] = jnp.dot(jnp.concatenate(lhs, axis=1), wz[...], preferred_element_type=F32)
        for x, ox, lane in ((0, 0, 0), (nx + 1, 2, c0)):
            widen((x, pl.ds(1, ny)), p1[x, 1 : ny + 1])
            lhs = [e1[x, oy : oy + ny].reshape(ny * nz, k0) for oy in range(3)]
            rhs = jnp.concatenate([wt[oy, ox, :, :c0] for oy in range(3)], axis=0)
            part = jnp.dot(jnp.concatenate(lhs, axis=1), rhs, preferred_element_type=F32)
            at = (0 if ox == 0 else nx // 2 - 1, slice(None), pl.ds(lane, c0))
            a1[at] = a1[at] + part
        for y, oy in ((0, 0), (ny + 1, 2)):
            widen((pl.ds(0, nx + 2), y), p1[:, y])
            lhs = [e1[ox : ox + nx, y].reshape(nx * nz, k0) for ox in range(3)]
            rhs = jnp.concatenate([wt[oy, ox, :, :c0] for ox in range(3)], axis=0)
            part = jnp.dot(jnp.concatenate(lhs, axis=1), rhs, preferred_element_type=F32).reshape(nx, nz, c0)
            for x in range(nx):
                at = (x // 2, pl.ds((0 if oy == 0 else ny - 1) * nz, nz), pl.ds(x % 2 * c0, c0))
                a1[at] = a1[at] + part[x]

    tile = 8
    last = lax.broadcasted_iota(jnp.int32, (tile, c0), 0) == (tile - 1) * oz
    for x in range(nx):
        for y in range(ny):
            at = (x // 2, pl.ds(pl.multiple_of(y * nz + (nz - tile) * oz, tile), tile), pl.ds(x % 2 * c0, c0))
            row = jnp.broadcast_to(rz[x * ny + y : x * ny + y + 1], (tile, c0))
            a1[at] = a1[at] + jnp.where(last, row, 0.0)

    hx, hy, hz = nx // 2, ny // 2, nz // 2

    @pl.loop(0, hx)
    def _(x):
        total = a1[x]
        both = jnp.maximum(jnp.maximum(total[:, :c0], total[:, c0:]), 0.0).reshape(hy, 2, nz, c0)
        t1[...] = jnp.max(both, axis=1)
        small = jnp.maximum(t1[:, pl.ds(0, hz, stride=2), :], t1[:, pl.ds(1, hz, stride=2), :])
        small = rounded(small)
        p2[x + 1, 1 : hy + 1] = small.astype(BF16)
        f2[x] = edge(small)

    arrived = neighbours(p2, 1, f2, p2, g2, hx, hy, s2, r2)
    for ref in (l3, l4):
        ref[...] = jnp.zeros(ref.shape, ref.dtype)
    arrived()
    rows = hx * hy * hz

    def pack(even, odd, at, block, lane):
        n, size, c = block.shape
        even[at, :, :, pl.ds(lane, c)] = block.reshape(n * size, c).astype(BF16).reshape(n // 2, 2 * size, c)
        block = block[1 : n - 1]
        odd[at, :, :, pl.ds(lane, c)] = block.reshape((n - 2) * size, c).astype(BF16).reshape(n // 2 - 1, 2 * size, c)

    def conv(even, odd, p, g, w):
        for x in range(hx + 2):
            block = p[x].astype(F32)
            c = block.shape[-1]
            below, above = shifted(block, g[x])
            for k, part in enumerate((below, block, above)):
                pack(even, odd, x, part, k * c)
        @stage
        def _():
            pairs = []
            for ox in range(3):
                for oy, (r, lo) in enumerate(((even, 0), (odd, 0), (even, 1))):
                    rhs = w[ox * 9 + oy * 3 : ox * 9 + oy * 3 + 3].reshape(3 * c, w.shape[2])
                    pairs.append((r[ox : ox + hx, lo : lo + hy // 2].reshape(rows, 3 * c), rhs))
            halves(pairs, (sums.at[0], sums.at[1]))

        return sums[0] + sums[1]

    loads[0].wait()
    c1 = wh.shape[2]
    total = conv(e2, o2, p2, g2, wh)
    skip = rounded(jnp.maximum(total, 0.0)).reshape(hx, hy, hz, c1)
    p3[1 : hx + 1, 1 : hy + 1] = skip.astype(BF16)

    cx, cy, cz = hx // 2, hy // 2, hz // 2
    ax = gxn * cx
    group = cz * cx
    m = jnp.max(skip.reshape(cx, 2, cy, 2, hz, c1), axis=(1, 3))
    m = m.reshape(cx * cy * hz, c1)
    m = jnp.maximum(m, pltpu.roll(m, m.shape[0] - 1, 0)).astype(BF16)

    blocks = []
    lane = lax.broadcasted_iota(jnp.int32, (group, cx * cy * hz), 1)
    sub = lax.broadcasted_iota(jnp.int32, (group, cx * cy * hz), 0)
    shift_x = cx.bit_length() - 1
    sub_x = sub & (cx - 1)
    sub_o = sub >> shift_x
    for y in range(cy):
        blocks.append(jnp.where(lane == (sub_x * cy + y) * hz + 2 * sub_o, 1.0, 0.0))
    blocks.append(jnp.where(lane == (sub_x * cy + sub_o) * hz + 2 * (cz - 1) * oz, 1.0, 0.0))
    pick = jnp.concatenate(blocks, axis=0).astype(BF16)
    packets = jnp.dot(pick, m, preferred_element_type=F32).reshape(cy + 1, group, c1).astype(BF16)
    pk2[...] = packets
    l2[gx, 0:cy] = packets[0:cy]

    def coarse_copy(k, dy, z):
        def make(src_gx, tgt_gx):
            if z == 0:
                src = {0: pl.ds(0, cy), -1: pl.ds(0, 1), 1: pl.ds(cy - 1, 1)}[dy]
            else:
                src = pl.ds(cy, 1)
            if dy == 0:
                dst = l2.at[src_gx, pl.ds(cy, 1) if z else pl.ds(0, cy)]
            else:
                dst = m2.at[src_gx, pl.ds(2 * z + (1 if dy < 0 else 0), 1)]
            return send(pk2.at[src], dst, s4.at[k], r4.at[k], tgt_gx, gy + dy, oz if z else gz)

        return make

    def deep_copy(pk, land, ss, rs):
        def choose(k, dy, z):
            def make(src_gx, tgt_gx):
                sy, ty = span(dy, cy, 0)
                sender = gz if src_gx is gx else (oz if z else gz)
                if z == 0:
                    src = pk.at[sy]
                    dst = land.at[src_gx, ty, pl.ds(1, cz)]
                else:
                    src = pk.at[sy, pl.ds((cz - 1) * (1 - sender), 1)]
                    dst = land.at[src_gx, ty, pl.ds((cz + 1) * sender, 1)]
                return send(src, dst, ss.at[k], rs.at[k], tgt_gx, gy + dy, oz if z else gz)

            return make

        return choose

    def narrow_copy(k, dy, z):
        def make(src_gx, tgt_gx):
            sy, ty = span(dy, cy, 0)
            sender = gz if src_gx is gx else (oz if z else gz)
            if z == 0:
                src = pk4.at[tgt_gx, sy]
                dst = l4.at[src_gx, ty, pl.ds(1, cz // 2)]
            else:
                src = pk4.at[tgt_gx, sy, pl.ds((cz // 2 - 1) * (1 - sender), 1)]
                dst = l4.at[src_gx, ty, pl.ds((cz // 2 + 1) * sender, 1)]
            return send(src, dst, s6.at[k], r6.at[k], tgt_gx, gy + dy, oz if z else gz)

        return make

    upper = lax.rem(gy, 2) == 1
    lower = lax.rem(gy, 2) == 0
    across = {-1: jnp.logical_and(lower, gy > 0), 1: jnp.logical_and(upper, gy < gyn - 1)}
    within = {-1: upper, 1: lower}

    def column_exchange(choose, main, rim, relay, carry, ss, rs):
        order = [(there, 0, z, 0) for z in (1, 0) for there in farthest]
        order += [(gx, 0, 1, 1)]
        for there, dy, z, k in order:
            choose(k, dy, z)(gx, there).start()
        for there in farthest + [gx]:
            for z in (1, 0):
                for dy in (-1, 1):
                    on(across[dy], choose(2, dy, z)(gx, there).start)

        def own(which):
            for k, ref in enumerate(main):
                drain(ref, which.at[k])

        def edges(which):
            for dy in (-1, 1):
                on(across[dy], lambda: drain(rim, which.at[2]))
            drain(relay, which.at[3])

        def arrive():
            own(rs)
            for dy in (-1, 1):
                for src, dst in carry(dy):
                    on(within[dy], send(src, dst, ss.at[3], rs.at[3], gx, gy + dy, gz).start)

        def finish():
            own(ss)
            edges(ss)

        late.append(finish)
        return arrive, lambda: edges(rs)

    def parts_of(land):
        wz = land.shape[2] - 2

        def carry(dy):
            rows = (cy, 0) if dy > 0 else (1, cy + 1)
            return [tuple(land.at[:, row] for row in rows)]

        main = (land.at[0 : gxn - 1, 0:cy, 0 : wz + 1], land.at[0, 0:cy, 0:1])
        return main, land.at[0:gxn, 0:1, 0 : wz + 1], land.at[:, 0], carry

    def carry_lines(dy):
        pairs = ((cy - 1, 0), (cy, 2)) if dy > 0 else ((0, 1), (cy, 3))
        return [(l2.at[:, line], m2.at[:, slot]) for line, slot in pairs]

    main4, rim4 = column_exchange(
        coarse_copy, (l2.at[0 : gxn - 1], l2.at[0, 0:1]), m2.at[:, 0:2], m2.at[:, 0:2], carry_lines, s4, r4
    )
    for x in range(hx):
        f3[x] = edge(p3[x + 1, 1 : hy + 1].astype(F32))

    def one_hot(ref, at, slots):
        width = gxn * slots * group
        lane = lax.broadcasted_iota(jnp.int32, (ax, width), 1)
        xs = lax.broadcasted_iota(jnp.int32, (ax, width), 0)
        base = lane - ((xs >> shift_x) * slots * group + (xs & (cx - 1)))
        ref[at] = jnp.where(base == slots_at, 1.0, 0.0)

    for y in range(-1, cy + 1):
        for z in range(-1, cz + 1):
            inside = 0 <= y < cy
            rim_slot = 0 if y < 0 else 1
            if 0 <= z < cz:
                slots_at = (y if inside else rim_slot) * group + z * cx
            else:
                line = y if inside else (cy - 1 if y < 0 else 0)
                mine = (gz == 1) if z < 0 else (gz == 0)
                slots_at = jnp.where(mine, (cy if inside else 2 + rim_slot) * group + line * cx, -(1 << 20))
            if inside:
                one_hot(sel2, (y, z + 1), cy + 1)
            else:
                one_hot(selm, (rim_slot, z + 1), 4)

    for wide, narrow in ((sel2, pick2), (selm, pickm)):
        narrow[...] = wide[...].reshape(narrow.shape).astype(BF16)

    def gathered(ref, land):
        width = ref.shape[-1]
        n = ref.shape[0] // ((cz + 2) * ax)
        select = ref[...]
        landed = land[...].astype(F32).reshape(width, c1).astype(BF16)
        return jnp.dot(select, landed, preferred_element_type=F32).reshape(n, cz + 2, ax, c1)

    deep = cy * cz * ax
    fo = w1.shape[2]

    windows = ((0, 0), (1, 0), (0, 1))

    def spread(even, odd, block, row):
        below, above = shifted(block, None)
        n, c = block.shape[0], block.shape[-1]
        for ox, part in enumerate((below, block, above)):
            whole = part.reshape(n * (cz + 2) * ax, c).astype(BF16)
            even[ox, row : row + n] = whole.reshape(n, cz // 2 + 1, 2 * ax, c)
            inner = part[:, 1 : cz + 1].reshape(n * cz * ax, c).astype(BF16)
            odd[ox, row : row + n] = inner.reshape(n, cz // 2, 2 * ax, c)

    def window(pair, ox, row, n):
        c = pair[0].shape[-1]
        lhs = [pair[i][ox, row : row + n, lo : lo + cz // 2].reshape(n * cz * ax, c) for i, lo in windows]
        return jnp.concatenate(lhs, axis=1)

    def bottom_own(pair, w):
        @stage
        def _():
            k = 3 * w.shape[1]
            pairs = []
            for ox in range(3):
                lhs = window(pair, ox, 1, cy)
                rhs = [w[ox * 9 + oy * 3 : ox * 9 + oy * 3 + 3].reshape(k, fo) for oy in range(3)]
                rhs = jnp.concatenate(rhs, axis=1)
                pairs += [(lhs[:, : k // 2], rhs[: k // 2]), (lhs[:, k // 2 :], rhs[k // 2 :])]
            halves(pairs, (deeps.at[0], deeps.at[1]))

    def bottom_rim(pair, w):
        k = 3 * w.shape[1]
        size = cz * ax
        @stage
        def _():
            for side, (row, oy) in enumerate(((0, 0), (cy + 1, 2))):
                total = jnp.zeros((size, fo), F32)
                for ox in range(3):
                    rhs = w[(ox * 3 + oy) * 3 : (ox * 3 + oy) * 3 + 3].reshape(k, fo)
                    total = total + jnp.dot(window(pair, ox, row, 1), rhs, preferred_element_type=F32)
                brims[side] = total

        def own(oy, y):
            at = (pl.ds(y * size, size), pl.ds(oy * fo, fo))
            return deeps[(0, *at)] + deeps[(1, *at)]

        lines = []
        for y in range(cy):
            before = own(0, y - 1) if y > 0 else brims[0]
            after = own(2, y + 1) if y < cy - 1 else brims[1]
            lines.append(own(1, y) + before + after)
        return jnp.maximum(jnp.concatenate(lines, axis=0), 0.0).reshape(cy, cz, ax, fo).astype(BF16)

    main4()
    spread(q2, b2, gathered(pick2, l2), 1)
    loads[1].wait()
    bottom_own((q2, b2), w1)
    rim4()
    block = gathered(pickm, m2)
    spread(q2, b2, block[0:1], 0)
    spread(q2, b2, block[1:2], cy + 1)
    first = bottom_rim((q2, b2), w1)
    pk3[...] = first
    l3[gx, 1 : cy + 1, 1 : cz + 1] = first
    main5, rim5 = column_exchange(deep_copy(pk3, l3, s5, r5), *parts_of(l3), s5, r5)

    skip_arrived = neighbours(p3, 1, f3, p3, g3, hx, hy, s3, r3)
    near = cx + 2
    wide = gxn * cz * near
    lane = lax.broadcasted_iota(jnp.int32, (wide, cz * ax), 1)
    row = lax.broadcasted_iota(jnp.int32, (wide, cz * ax), 0)
    shift_n = near.bit_length() - 1
    shift_z = cz.bit_length() - 1
    at = (row >> (shift_n + shift_z)) * cx + (row & (near - 1)) - 1
    at = jnp.where(jnp.logical_and(at >= 0, at < ax), at, -(cz + 1) * ax)
    share = jnp.where(lane == ((row >> shift_n) & (cz - 1)) * ax + at, 1.0, 0.0).astype(BF16)

    lane = lax.broadcasted_iota(jnp.int32, (hz, (cz + 4) * near), 1)
    zs = lax.broadcasted_iota(jnp.int32, (hz, (cz + 4) * near), 0)
    blocks = []
    for k in range(3):
        for x in range(-1, hx + 1):
            blocks.append(jnp.where(lane == (((zs + (k - 1)) >> 1) + 2) * near + (x >> 1) + 1, 1.0, 0.0))
    for k in range(3):
        blocks += blocks[k * (hx + 2) + 1 : (k + 1) * (hx + 2) - 1]
    pick = jnp.concatenate(blocks, axis=0).astype(BF16)

    def joined(row, n):
        return jnp.concatenate([l3[g, row : row + n].astype(F32) for g in range(gxn)], axis=-1)

    main5()
    spread(q3, b3, joined(1, cy), 1)
    loads[2].wait()
    bottom_own((q3, b3), w2)
    rim5()
    spread(q3, b3, joined(0, 1), 0)
    spread(q3, b3, joined(cy + 1, 1), cy + 1)
    second = bottom_rim((q3, b3), w2)
    for y in range(cy):
        line = second[y].astype(F32).reshape(cz * ax, fo).astype(BF16)
        line = jnp.dot(share, line, preferred_element_type=F32)
        pk4[:, y] = line.reshape(gxn, cz // 2, 2 * near, fo).astype(BF16)
    l4[gx, 1 : cy + 1, 1 : cz // 2 + 1] = pk4[gx]
    main6, rim6 = column_exchange(narrow_copy, *parts_of(l4), s6, r6)
    size = hx * hz

    def enlarge(ys):
        fields = [l4[g, y].astype(F32).reshape((cz + 4) * near, fo) for y in ys for g in range(gxn)]
        fields = jnp.concatenate(fields, axis=-1).astype(BF16)
        fields = jnp.dot(pick, fields, preferred_element_type=F32).astype(BF16)
        for i, y in enumerate(ys):
            field = fields[:, i * c2 : (i + 1) * c2]
            for k in range(3):
                at = pl.ds(k * c2, c2)
                part = field[k * (size + 2 * hz) : (k + 1) * (size + 2 * hz)]
                up[0, y, :, :, at] = part[:size].reshape(hx // 2, 2 * hz, c2)
                up[2, y, :, :, at] = part[2 * hz :].reshape(hx // 2, 2 * hz, c2)
                part = field[3 * (size + 2 * hz) + k * size : 3 * (size + 2 * hz) + (k + 1) * size]
                up[1, y, :, :, at] = part.reshape(hx // 2, 2 * hz, c2)

    skip_arrived()
    loads[3].wait()
    total = conv(e3, o3, p3, g3, wus)
    acc[...] = total.reshape(hx, hy, hz, c1)

    main6()
    enlarge(range(1, cy + 1))
    loads[4].wait()

    @stage
    def _():
        pairs = []
        for ox in range(3):
            for k in range(3):
                lhs = up[ox, 1 : cy + 1, :, :, pl.ds(k * c2, c2)].reshape(cy * size, c2)
                pairs.append((lhs, wuu[ox * 9 + 3 + k]))
        halves(pairs, (thirds.at[0], thirds.at[1]))

    rim6()
    enlarge((0, cy + 1))

    @stage
    def _():
        for side, oy in enumerate((0, 2)):
            total = jnp.zeros(((cy + 1) * size, c1), F32)
            for ox in range(3):
                lhs = up[ox, side : side + cy + 1].reshape((cy + 1) * size, 3 * c2)
                rhs = wuu[(ox * 3 + oy) * 3 : (ox * 3 + oy) * 3 + 3].reshape(3 * c2, c1)
                total = total + jnp.dot(lhs, rhs, preferred_element_type=F32)
            ends[side] = total

    for y in range(hy):
        low, mid, high = (y + 1) // 2, (y + 2) // 2 - 1, (y + 3) // 2 - 1
        total = ends[0, low * size : (low + 1) * size] + ends[1, high * size : (high + 1) * size]
        total = total + thirds[0, mid * size : (mid + 1) * size] + thirds[1, mid * size : (mid + 1) * size]
        out[:, y] = (acc[:, y] + total.reshape(hx, hz, c1)).astype(BF16)

    for fn in late:
        fn()


def on_device(dims, volume, w_full, w_half, w_bottom_in, w_bottom_out, w_up):
    gxn, gyn = dims
    nx, ny, nz, c0 = volume.shape
    c1 = w_half.shape[4]
    c2, fo = w_bottom_out.shape[3:]
    hx, hy, hz = nx // 2, ny // 2, nz // 2
    cx, cy, cz = hx // 2, hy // 2, hz // 2
    ax = gxn * cx
    weights = [
        w_full.reshape(3, 3, 3 * c0, c0),
        w_half.reshape(27, c0, c1),
        w_bottom_in.reshape(27, c1, fo),
        w_bottom_out.reshape(27, c2, fo),
        w_up.reshape(27, c2 + c1, c1),
    ]
    vm = pltpu.VMEM
    dma = pltpu.SemaphoreType.DMA
    scratch = [vm(w.shape, BF16) for w in weights[1:4]]
    scratch += [vm((27, c1, c1), BF16), vm((27, c2, c1), BF16), dma((5,)), dma(()), dma(())]
    scratch += [vm((3, 4, 3 * c0, 2 * c0), BF16), vm((9 * c0, c0), BF16)]
    scratch += [
        vm((nx + 2, ny + 2, nz, c0), BF16), vm((nx, ny, 1, c0), F32), vm((nx + 2, ny + 2, 1, c0), F32),
        vm((nx + 2, ny + 2, c0), F32), vm((nx + 2, ny + 2, nz, 3 * c0), BF16), vm((hx, ny * nz, 2 * c0), F32),
        vm((nx * ny, c0), F32), vm((hy, nz, c0), F32),
        vm((hx + 2, hy + 2, hz, c0), BF16), vm((hx, hy, 1, c0), F32), vm((hx + 2, hy + 2, 1, c0), F32),
        vm((hx + 2, hy // 2 + 1, 2 * hz, 3 * c0), BF16), vm((hx + 2, hy // 2, 2 * hz, 3 * c0), BF16),
        vm((hx + 2, hy + 2, hz, c1), BF16), vm((hx, hy, 1, c1), F32), vm((hx + 2, hy + 2, 1, c1), F32),
        vm((hx + 2, hy // 2 + 1, 2 * hz, 3 * c1), BF16), vm((hx + 2, hy // 2, 2 * hz, 3 * c1), BF16),
        vm((hx, hy, hz, c1), F32),
        vm((cy + 1, cz * cx, c1), BF16), vm((gxn, cy + 1, cz * cx, c1), BF16), vm((gxn, 4, cz * cx, c1), BF16),
        vm((cy, cz + 2, ax, gxn * (cy + 1) * cz * cx), F32), vm((2, cz + 2, ax, gxn * 4 * cz * cx), F32),
        vm((cy * (cz + 2) * ax, gxn * (cy + 1) * cz * cx), BF16), vm((2 * (cz + 2) * ax, gxn * 4 * cz * cx), BF16),
        vm((3, cy + 2, cz // 2 + 1, 2 * ax, c1), BF16), vm((3, cy + 2, cz // 2, 2 * ax, c1), BF16),
        vm((cy, cz, ax, fo), BF16), vm((gxn, cy + 2, cz + 2, ax, fo), BF16),
        vm((3, cy + 2, cz // 2 + 1, 2 * ax, c2), BF16), vm((3, cy + 2, cz // 2, 2 * ax, c2), BF16),
        vm((gxn, cy, cz // 2, 2 * (cx + 2), fo), BF16), vm((gxn, cy + 2, cz // 2 + 2, 2 * (cx + 2), fo), BF16),
        vm((3, cy + 2, hx // 2, 2 * hz, 3 * c2), BF16),
        vm((2, hx * hy * hz, c1), F32), vm((2, cy * cz * ax, 3 * fo), F32), vm((2, cz * ax, fo), F32),
        vm((2, cy * hx * hz, c1), F32), vm((2, (cy + 1) * hx * hz, c1), F32),
    ]
    scratch += [dma((3,))] * 6 + [dma((4,))] * 6
    return pl.pallas_call(
        functools.partial(kernel, dims),
        out_shape=jax.ShapeDtypeStruct((hx, hy, hz, c1), BF16),
        in_specs=[pl.BlockSpec(memory_space=pltpu.HBM)] * 6,
        out_specs=pl.BlockSpec(memory_space=pltpu.VMEM),
        scratch_shapes=scratch,
        compiler_params=pltpu.CompilerParams(
            collective_id=0, has_side_effects=True, vmem_limit_bytes=52 * 1024 * 1024
        ),
    )(*[pltpu.with_memory_space_constraint(a, pltpu.HBM) for a in (volume, *weights)])


def solution(mesh):
    dims = (mesh.shape["gx"], mesh.shape["gy"])
    assert mesh.shape["gz"] == 2 and mesh.shape["gy"] % 2 == 0
    return jax.shard_map(
        functools.partial(on_device, dims),
        mesh=mesh,
        in_specs=(
            P("gx", "gy", "gz", None),
            P(),
            P(),
            P(None, None, None, None, "gx"),
            P(None, None, None, None, "gx"),
            P(),
        ),
        out_specs=P("gx", "gy", "gz", None),
        check_vma=False,
    )
```
